32 devices in a mesh: pod: 1 (over z), d: 32 (over y, x, core).
Axes of the slice: x: 4, y: 4, z: 1, core: 2. Of those that a mesh axis runs over, the one named last changes fastest.
The devices are a block of a 4x4x8 slice.
Arguments:
- x: bfloat16 [32, 2048, 2048], P(('pod', 'd'))
- prompt_len: int32 [32], P(('pod', 'd'))
- ln_scale: float32 [2048], P('d')
- w_in: bfloat16 [2048, 18944], P('d')
- w_out: bfloat16 [10240, 2048], P(None, 'd')
Outputs:
- output 1: bfloat16 [32, 2048, 2048], P(('pod', 'd'))
- output 2: bfloat16 [32, 2048, 256], P(('pod', 'd'))
- output 3: bfloat16 [32, 2048, 256], P(('pod', 'd'))
All inputs are finite; a program needn't handle non-finite values.
Results may differ from the reference program's by a relative error of at most 0.00408039.
Values are sent between devices in bfloat16 or wider.
A program may use at most 768 MiB of HBM per device.

```python
import math
import jax
import jax.numpy as jnp
from jax import lax

E = 2048
F = 8192
HEADS = 8
HEAD = 256
T = 2048
BATCH = 32

COLS_IN = 2 * F + HEADS * HEAD + 2 * HEAD
ROWS_OUT = F + HEADS * HEAD
EPS = 1e-6
ROPE_BASE = 10000.0


def setup_inputs(seed: int = 0, part: int = 0) -> dict:
    shared_key = jax.random.key(seed)
    part_key = jax.random.fold_in(jax.random.key(seed + 1), part)
    key_x, key_len, key_full = jax.random.split(part_key, 3)
    key_ln, key_in, key_out = jax.random.split(shared_key, 3)
    x = jax.random.normal(key_x, (BATCH, T, E), jnp.float32).astype(jnp.bfloat16)
    drawn_len = jax.random.randint(key_len, (BATCH,), 1, T + 1, dtype=jnp.int32)
    full_slot = jax.random.randint(key_full, (), 0, BATCH, dtype=jnp.int32)
    prompt_len = jnp.where(jnp.arange(BATCH) == full_slot, T, drawn_len).astype(jnp.int32)
    ln_scale = 1.0 + 0.25 * jax.random.normal(key_ln, (E,), jnp.float32)
    q_gain = math.sqrt(0.5 * math.log(T))
    col_gain = jnp.concatenate([
        jnp.ones((2 * F,), jnp.float32),
        jnp.full((HEADS * HEAD,), q_gain, jnp.float32),
        jnp.ones((2 * HEAD,), jnp.float32)])
    w_in = (jax.random.normal(key_in, (E, COLS_IN), jnp.float32) * (E ** -0.5) * col_gain).astype(jnp.bfloat16)
    row_gain = jnp.concatenate([
        jnp.full((F,), F ** -0.5, jnp.float32),
        jnp.full((HEADS * HEAD,), (HEADS * HEAD) ** -0.5, jnp.float32)])
    w_out = (jax.random.normal(key_out, (ROWS_OUT, E), jnp.float32) * row_gain[:, None]).astype(jnp.bfloat16)
    return {"x": x, "prompt_len": prompt_len, "ln_scale": ln_scale, "w_in": w_in, "w_out": w_out}


def rope_tables():
    half_dim = HEAD // 2
    inv_freq = ROPE_BASE ** (-2.0 * jnp.arange(half_dim, dtype=jnp.float32) / HEAD)
    angles = jnp.arange(T, dtype=jnp.float32)[:, None] * inv_freq[None, :]
    return jnp.cos(angles), jnp.sin(angles)


def apply_rope(rope_in, cos_b, sin_b):
    half_dim = rope_in.shape[-1] // 2
    lower_half = rope_in[..., :half_dim]
    upper_half = rope_in[..., half_dim:]
    return jnp.concatenate([lower_half * cos_b - upper_half * sin_b, upper_half * cos_b + lower_half * sin_b], axis=-1)


def reference(x, prompt_len, ln_scale, w_in, w_out):
    cos_t, sin_t = rope_tables()
    positions = jnp.arange(T)
    causal = positions[None, :] <= positions[:, None]
    q_start = 2 * F
    k_start = q_start + HEADS * HEAD
    v_start = k_start + HEAD

    def one_sequence(seq_args):
        x_seq, seq_len = seq_args
        x_float = x_seq.astype(jnp.float32)
        centered = x_float - jnp.mean(x_float, axis=-1, keepdims=True)
        var_val = jnp.mean(centered * centered, axis=-1, keepdims=True)
        h_norm = (centered * lax.rsqrt(var_val + EPS) * ln_scale).astype(jnp.bfloat16)
        projected = jnp.dot(h_norm, w_in, preferred_element_type=jnp.float32)
        gated = (jax.nn.silu(projected[:, :F]) * projected[:, F:q_start]).astype(jnp.bfloat16)
        q_rot = apply_rope(projected[:, q_start:k_start].reshape(T, HEADS, HEAD), cos_t[:, None, :], sin_t[:, None, :]).astype(jnp.bfloat16)
        k_rot = apply_rope(projected[:, k_start:v_start], cos_t, sin_t).astype(jnp.bfloat16)
        v_val = projected[:, v_start:].astype(jnp.bfloat16)
        scores = jnp.einsum("thd,sd->hts", q_rot.astype(jnp.float32), k_rot.astype(jnp.float32)) * (1.0 / math.sqrt(HEAD))
        allowed = causal & (positions[None, :] < seq_len)
        probs_bf = jax.nn.softmax(jnp.where(allowed[None, :, :], scores, -1e30), axis=-1).astype(jnp.bfloat16)
        attn_out = jnp.einsum("hts,sd->thd", probs_bf.astype(jnp.float32), v_val.astype(jnp.float32)).astype(jnp.bfloat16).reshape(T, HEADS * HEAD)
        mixed_rows = jnp.concatenate([gated, attn_out], axis=-1)
        out_sum = jnp.dot(mixed_rows, w_out, preferred_element_type=jnp.float32)
        return (x_float + out_sum).astype(jnp.bfloat16), k_rot, v_val

    y_out, k_cache, v_cache = lax.map(one_sequence, (x, prompt_len))
    return y_out, k_cache, v_cache
```

```python
import functools
import math

import jax
import jax.numpy as jnp
import numpy as np
from jax import lax
from jax.experimental import pallas as pl
from jax.experimental.pallas import tpu as pltpu
from jax.sharding import PartitionSpec as P

EPS = 1e-6
ROPE_BASE = 10000.0
MASKED = -1e30
MESH = pl.DeviceIdType.MESH
HBM = pltpu.HBM
VMEM_LIMIT = 67043328

CHUNK = 384
LAG = (0, 2, 4, 6, 8, 10)


def dims(mesh, x, w_in, w_out):
    devices = mesh.shape["d"]
    cores = 2
    side = math.isqrt(devices // cores)
    model = x.shape[2]
    ffn = 4 * model
    attn = w_out.shape[0] - ffn
    head = (w_in.shape[1] - 2 * ffn - attn) // 2
    return dict(D=devices, CORES=cores, SIDE=side, T=x.shape[1], E=model, F=ffn, H=attn // head, HD=head,
                R=model // devices, COLS=w_in.shape[1] + w_out.shape[0], FC=head)


def rope_tables(seq_len, head_dim):
    half = head_dim // 2
    inv_freq = np.float32(ROPE_BASE) ** (np.float32(-2.0) * np.arange(half, dtype=np.float32) / np.float32(head_dim))
    return inv_freq


def place():
    return lax.axis_index("d")


def order_copies(d, win_ref, wot_ref, stage_ref, sem):
    F, H, HD, FC = d["F"], d["H"], d["HD"], d["FC"]
    qs = 2 * F
    ks = qs + H * HD
    pltpu.make_async_copy(win_ref.at[:, pl.ds(ks, 2 * HD)], stage_ref.at[:, pl.ds(0, 2 * HD)], sem).start()

    @pl.loop(0, H)
    def _(h):
        at = pl.multiple_of(2 * HD + h * 2 * HD, HD)
        pltpu.make_async_copy(win_ref.at[:, pl.ds(pl.multiple_of(qs + h * HD, HD), HD)],
                              stage_ref.at[:, pl.ds(at, HD)], sem).start()
        pltpu.make_async_copy(wot_ref.at[:, pl.ds(pl.multiple_of(F + h * HD, HD), HD)],
                              stage_ref.at[:, pl.ds(at + HD, HD)], sem).start()

    base = 2 * HD + H * 2 * HD

    @pl.loop(0, F // FC)
    def _(j):
        at = pl.multiple_of(base + j * 3 * FC, FC)
        pltpu.make_async_copy(win_ref.at[:, pl.ds(pl.multiple_of(j * FC, FC), FC)],
                              stage_ref.at[:, pl.ds(at, FC)], sem).start()
        pltpu.make_async_copy(win_ref.at[:, pl.ds(pl.multiple_of(F + j * FC, FC), FC)],
                              stage_ref.at[:, pl.ds(at + FC, FC)], sem).start()
        pltpu.make_async_copy(wot_ref.at[:, pl.ds(pl.multiple_of(j * FC, FC), FC)],
                              stage_ref.at[:, pl.ds(at + 2 * FC, FC)], sem).start()


class Comm:
    def __init__(self, d, stage_ref, w_ref, send_sem, recv_sem):
        self.d = d
        self.stage, self.w, self.send, self.recv = stage_ref, w_ref, send_sem, recv_sem
        self.groups = d["COLS"] // CHUNK
        side, cores = d["SIDE"], d["CORES"]
        me = place()
        self.me = me
        self.core = lax.rem(me, cores)
        self.x = lax.rem(lax.div(me, cores), side)
        self.y = lax.div(me, cores * side)

    def dev(self, y, x, core):
        d = self.d
        return {"d": (y * d["SIDE"] + x) * d["CORES"] + core}

    def wrap(self, v):
        side = self.d["SIDE"]
        return lax.rem(v + side, side)

    def put(self, src, dst, stage, g, device):
        return pltpu.make_async_remote_copy(src_ref=src, dst_ref=dst, send_sem=self.send.at[stage],
                                            recv_sem=self.recv.at[stage, g], device_id=device, device_id_type=MESH)

    def landed(self, ref, stage, g):
        pltpu.make_async_copy(ref, ref, self.recv.at[stage, g]).wait()

    def stage_fn(self, stage, g):
        w, x, y, c = self.w, self.x, self.y, self.core
        half = self.d["R"] // 2
        cols = pl.ds(pl.multiple_of(g * CHUNK, 128), CHUNK)
        ra, rb = pl.ds(0, half), pl.ds(half, half)
        turn = 1 - 2 * lax.rem(g, 2)
        if stage == 0:
            for s in (1, -1):
                self.put(self.stage.at[ra, cols], w.at[y, x, c, ra, cols], 0, g,
                         self.dev(y, self.wrap(x + s), c)).start()
                self.put(self.stage.at[rb, cols], w.at[y, x, c, rb, cols], 0, g,
                         self.dev(self.wrap(y + s), x, c)).start()
        elif stage == 1:
            self.landed(w.at[0, 0:2, :, ra, cols], 0, g)
            xs, ys = self.wrap(x - turn), self.wrap(y + turn)
            a = w.at[y, xs, c, ra, cols]
            self.put(a, a, 1, g, self.dev(y, self.wrap(x + turn), c)).start()
            b = w.at[ys, x, c, rb, cols]
            self.put(b, b, 1, g, self.dev(self.wrap(y - turn), x, c)).start()
        elif stage == 2:
            self.landed(w.at[0, 0, :, ra, cols], 1, g)
            a = w.at[y, :, c, ra, cols]
            b = w.at[:, x, c, rb, cols]
            for s in (1, -1):
                self.put(a, a, 2, g, self.dev(self.wrap(y + s), x, c)).start()
                self.put(b, b, 2, g, self.dev(y, self.wrap(x + s), c)).start()
        elif stage == 3:
            self.landed(w.at[0:2, :, :, ra, cols], 2, g)
            ys, xs = self.wrap(y - turn), self.wrap(x + turn)
            a = w.at[ys, :, c, ra, cols]
            self.put(a, a, 3, g, self.dev(self.wrap(y + turn), x, c)).start()
            b = w.at[:, xs, c, rb, cols]
            self.put(b, b, 3, g, self.dev(y, self.wrap(x - turn), c)).start()
        elif stage == 4:
            self.landed(w.at[0, :, :, ra, cols], 3, g)
            a = w.at[:, :, c, :, cols]
            self.put(a, a, 4, g, self.dev(y, x, 1 - c)).start()
        else:
            self.landed(w.at[:, :, 0, :, cols], 4, g)

    def point(self, p):
        for stage in range(6):
            g = p - LAG[stage]
            if isinstance(g, int):
                if 0 <= g < self.groups:
                    self.stage_fn(stage, g)
            else:
                @pl.when(jnp.logical_and(g >= 0, g < self.groups))
                def _(stage=stage, g=g):
                    self.stage_fn(stage, g)

    def drain(self):
        side, w = self.d["SIDE"], self.w
        for stage, ref in ((0, w.at[0, 0]), (1, w.at[0, 0, 0]), (2, w.at[0]), (3, w.at[0, 0:side // 2]),
                           (4, w.at[0:side // 2])):
            pltpu.make_async_copy(ref, ref, self.send.at[stage]).wait()


def meet(d):
    barrier = pltpu.get_barrier_semaphore()
    me = place()

    @pl.loop(1, d["D"])
    def _(i):
        pl.semaphore_signal(barrier, inc=1, device_id={"d": lax.rem(me + i, d["D"])}, device_id_type=MESH)

    pl.semaphore_wait(barrier, d["D"] - 1)


def spread_scale(d, ln_ref, ln_all, ln_send, ln_recv):
    me = place()

    @pl.loop(1, d["D"])
    def _(i):
        pltpu.make_async_remote_copy(src_ref=ln_ref, dst_ref=ln_all.at[me], send_sem=ln_send, recv_sem=ln_recv,
                                     device_id={"d": lax.rem(me + i, d["D"])}, device_id_type=MESH).start()

    ln_all[me] = ln_ref[...]


def spread_scale_wait(d, ln_all, ln_send, ln_recv):
    rest = ln_all.at[pl.ds(0, d["D"] - 1)]
    pltpu.make_async_copy(rest, rest, ln_recv).wait()
    pltpu.make_async_copy(rest, rest, ln_send).wait()


def scale_row(d, ln_all, row_ref):
    lane = lax.broadcasted_iota(jnp.int32, (1, 128), 1)
    per = 128 // d["R"]
    for i in range(d["E"] // 128):
        part = ln_all[per * i][0:1, :]
        for k in range(1, per):
            part = jnp.where(lane < k * d["R"], part, ln_all[per * i + k][0:1, :])
        row_ref[0:1, i * 128:(i + 1) * 128] = part


def gather_kernel(d, ln_ref, win_ref, wot_ref, w_ref, lnout_ref, stage_ref, ln_all, local_sem, ln_send, ln_recv,
                  send_sem, recv_sem):
    order_copies(d, win_ref, wot_ref, stage_ref, local_sem.at[0])
    comm = Comm(d, stage_ref, w_ref, send_sem, recv_sem)
    own = pltpu.make_async_copy(stage_ref, w_ref.at[comm.y, comm.x, comm.core], local_sem.at[1])
    meet(d)
    spread_scale(d, ln_ref, ln_all, ln_send, ln_recv)
    pltpu.make_async_copy(stage_ref, stage_ref, local_sem.at[0]).wait()
    own.start()
    spread_scale_wait(d, ln_all, ln_send, ln_recv)
    comm.point(0)
    comm.point(1)
    own.wait()

    @pl.loop(2, comm.groups + LAG[5])
    def _(p):
        comm.point(p)

    comm.drain()
    scale_row(d, ln_all, lnout_ref)


def gather(d, mesh, ln, w_in, wot):
    groups = d["COLS"] // CHUNK
    ln_tile = jnp.broadcast_to(jnp.tile(ln, 128 // d["R"])[None], (8, 128))
    w_shape = (d["SIDE"], d["SIDE"], d["CORES"], d["R"], d["COLS"])
    return pl.pallas_call(
        functools.partial(gather_kernel, d),
        out_shape=(jax.ShapeDtypeStruct(w_shape, jnp.bfloat16), jax.ShapeDtypeStruct((1, d["E"]), jnp.float32)),
        in_specs=[pl.BlockSpec(memory_space=pltpu.VMEM), pl.BlockSpec(memory_space=HBM), pl.BlockSpec(memory_space=HBM)],
        out_specs=(pl.BlockSpec(memory_space=HBM), pl.BlockSpec(memory_space=pltpu.VMEM)),
        scratch_shapes=[
            pltpu.VMEM((d["R"], d["COLS"]), jnp.bfloat16),
            pltpu.VMEM((d["D"], 8, 128), jnp.float32),
            pltpu.SemaphoreType.DMA((2,)),
            pltpu.SemaphoreType.DMA,
            pltpu.SemaphoreType.DMA,
            pltpu.SemaphoreType.DMA((5,)),
            pltpu.SemaphoreType.DMA((5, groups)),
        ],
        compiler_params=pltpu.CompilerParams(collective_id=0, has_side_effects=True, vmem_limit_bytes=VMEM_LIMIT),
        name="gather",
    )(ln_tile, w_in, wot)


def nn(a, b):
    return lax.dot_general(a, b, (((1,), (0,)), ((), ())), preferred_element_type=jnp.float32)


def nt(a, b):
    return lax.dot_general(a, b, (((1,), (1,)), ((), ())), preferred_element_type=jnp.float32)


def rope(u, cos, sin):
    half = u.shape[1] // 2
    u1, u2 = u[:, :half], u[:, half:]
    return jnp.concatenate([u1 * cos - u2 * sin, u2 * cos + u1 * sin], axis=1)


class Layer:
    XB = 128
    MB = 512
    QB = 256

    def __init__(self, d, r):
        self.d, self.r = d, r

    def x_copy(self, i, slot):
        rows = pl.ds(pl.multiple_of(i * self.XB, self.XB), self.XB)
        return pltpu.make_async_copy(self.r.x.at[0, rows, :], self.r.xbuf.at[slot], self.r.xsem.at[slot])

    def unit(self, col, buf, sem):
        return pltpu.make_async_copy(self.r.w.at[:, :, :, :, pl.ds(pl.multiple_of(col, 128), self.d["FC"])], buf, sem)

    def wval(self, buf):
        return buf[...].reshape(self.d["E"], self.d["FC"])

    def norm(self):
        d, r = self.d, self.r
        n = d["T"] // self.XB
        self.x_copy(0, 0).start()

        @pl.loop(0, n)
        def _(i):
            slot = lax.rem(i, 2)

            @pl.when(i + 1 < n)
            def _():
                self.x_copy(i + 1, 1 - slot).start()

            self.x_copy(i, slot).wait()
            rows = pl.ds(pl.multiple_of(i * self.XB, self.XB), self.XB)
            xf = r.xbuf[slot].astype(jnp.float32)
            centered = xf - jnp.mean(xf, axis=-1, keepdims=True)
            var = jnp.mean(centered * centered, axis=-1, keepdims=True)
            r.h[rows, :] = (centered * lax.rsqrt(var + EPS) * r.ln[...]).astype(jnp.bfloat16)
            r.yacc[rows, :] = xf

    def tables(self):
        d, r = self.d, self.r
        lo = r.rc.shape[0] - d["T"] // self.QB
        cl, sl = r.rc[0:self.QB, :], r.rs[0:self.QB, :]
        for b in range(d["T"] // self.QB):
            cb, sb = r.rc[self.QB + b:self.QB + b + 1, :], r.rs[self.QB + b:self.QB + b + 1, :]
            rows = slice(b * self.QB, (b + 1) * self.QB)
            r.cos[rows, :] = cl * cb - sl * sb
            r.sin[rows, :] = sl * cb + cl * sb

    def bias(self):
        r, d = self.r, self.d
        col = lax.broadcasted_iota(jnp.int32, (8, d["T"]), 1)
        r.bias[...] = jnp.where(col < r.plen[0], 0.0, MASKED)

    def keys(self, kbuf, vbuf):
        r, d = self.r, self.d
        for m in range(d["T"] // self.MB):
            rows = slice(m * self.MB, (m + 1) * self.MB)
            hb = r.h[rows, :]
            r.k[rows, :] = rope(nn(hb, self.wval(kbuf)), r.cos[rows, :], r.sin[rows, :]).astype(jnp.bfloat16)
            r.v[rows, :] = nn(hb, self.wval(vbuf)).astype(jnp.bfloat16)

    def query(self, qbuf):
        r, d = self.r, self.d
        scale = 1.0 / math.sqrt(d["HD"])
        for m in range(d["T"] // self.MB):
            rows = slice(m * self.MB, (m + 1) * self.MB)
            q = rope(nn(r.h[rows, :], self.wval(qbuf)), r.cos[rows, :], r.sin[rows, :]).astype(jnp.bfloat16)
            r.q[rows, :] = q * jnp.bfloat16(scale)

    def attend(self):
        r, d = self.r, self.d
        qb = self.QB
        row = lax.broadcasted_iota(jnp.int32, (qb, qb), 0)
        col = lax.broadcasted_iota(jnp.int32, (qb, qb), 1)
        for b in range(d["T"] // qb):
            n = (b + 1) * qb
            rows = slice(b * qb, n)
            s = nt(r.q[rows, :], r.k[0:n, :]) + r.bias[0:1, 0:n]
            last = jnp.where(col <= row, s[:, n - qb:], MASKED)
            s = last if b == 0 else jnp.concatenate([s[:, :n - qb], last], axis=1)
            e = jnp.exp(s - jnp.max(s, axis=-1, keepdims=True))
            p = (e * (1.0 / jnp.sum(e, axis=-1, keepdims=True))).astype(jnp.bfloat16)
            r.o[rows, :] = nn(p, r.v[0:n, :]).astype(jnp.bfloat16)

    def add_out(self, a_ref, obuf, tile):
        r, d = self.r, self.d
        fc = d["FC"]
        per = fc // d["R"]
        cols = slice(tile * fc, (tile + 1) * fc)
        w = self.wval(obuf)[cols, :]
        r.yacc[:, cols] += nt(a_ref[...], w)

    def gated(self, m, gbuf, ubuf, a_ref):
        r = self.r
        rows = slice(m * self.MB, (m + 1) * self.MB)
        hb = r.h[rows, :]
        g = nn(hb, self.wval(gbuf))
        u = nn(hb, self.wval(ubuf))
        hg = g * 0.5
        a_ref[rows, :] = ((hg + hg * jnp.tanh(hg)) * u).astype(jnp.bfloat16)

    def finish(self):
        d, r = self.d, self.r
        n = d["T"] // self.XB

        def out(i, slot):
            rows = pl.ds(pl.multiple_of(i * self.XB, self.XB), self.XB)
            return pltpu.make_async_copy(r.xbuf.at[slot], r.y.at[0, rows, :], r.xsem.at[slot])

        @pl.loop(0, n)
        def _(i):
            slot = lax.rem(i, 2)

            @pl.when(i >= 2)
            def _():
                out(i - 2, slot).wait()

            rows = pl.ds(pl.multiple_of(i * self.XB, self.XB), self.XB)
            r.xbuf[slot] = r.yacc[rows, :].astype(jnp.bfloat16)
            out(i, slot).start()

        out(n - 2, n % 2).wait()
        out(n - 1, 1 - n % 2).wait()


class Refs:
    pass


LAYER_NAMES = ("x", "plen", "ln", "rc", "rs", "w", "y", "kc", "vc", "h", "yacc", "xbuf", "cos", "sin", "bias", "k", "v", "q", "o", "a",
               "wbuf", "obuf", "xsem", "wsem", "osem", "csem")


def layer_scratch(d):
    T, E, HD, FC = d["T"], d["E"], d["HD"], d["FC"]
    unit = (d["SIDE"], d["SIDE"], d["CORES"], d["R"], FC)
    return [
        pltpu.VMEM((T, E), jnp.bfloat16),
        pltpu.VMEM((T, E), jnp.float32),
        pltpu.VMEM((2, Layer.XB, E), jnp.bfloat16),
        pltpu.VMEM((T, HD // 2), jnp.float32),
        pltpu.VMEM((T, HD // 2), jnp.float32),
        pltpu.VMEM((8, T), jnp.float32),
        pltpu.VMEM((T, HD), jnp.bfloat16),
        pltpu.VMEM((T, HD), jnp.bfloat16),
        pltpu.VMEM((T, HD), jnp.bfloat16),
        pltpu.VMEM((T, HD), jnp.bfloat16),
        pltpu.VMEM((2, T, FC), jnp.bfloat16),
        pltpu.VMEM((2, 2) + unit, jnp.bfloat16),
        pltpu.VMEM((3,) + unit, jnp.bfloat16),
        pltpu.SemaphoreType.DMA((2,)),
        pltpu.SemaphoreType.DMA((2, 2)),
        pltpu.SemaphoreType.DMA((3,)),
        pltpu.SemaphoreType.DMA((2,)),
    ]


def layer_kernel(d, *refs):
    r = Refs()
    for name, ref in zip(LAYER_NAMES, refs, strict=True):
        setattr(r, name, ref)
    L = Layer(d, r)
    HD, FC, H = d["HD"], d["FC"], d["H"]
    J = d["F"] // FC
    tiles = d["E"] // FC
    mbs = d["T"] // L.MB
    base = 2 * HD + H * 2 * HD

    def fetch_kv():
        return [L.unit(0, r.wbuf.at[0, 0], r.wsem.at[0, 0]), L.unit(HD, r.wbuf.at[0, 1], r.wsem.at[0, 1])]

    def fetch_head(h):
        col = 2 * HD + h * 2 * HD
        return [L.unit(col, r.wbuf.at[1, lax.rem(h, 2)], r.wsem.at[1, lax.rem(h, 2)]),
                L.unit(col + HD, r.obuf.at[lax.rem(h, 2)], r.osem.at[lax.rem(h, 2)])]

    def fetch_mlp(j):
        col = base + j * 3 * FC
        s = lax.rem(j, 2)
        o = lax.rem(j, 3)
        return [L.unit(col, r.wbuf.at[s, 0], r.wsem.at[s, 0]), L.unit(col + FC, r.wbuf.at[s, 1], r.wsem.at[s, 1]),
                L.unit(col + 2 * FC, r.obuf.at[o], r.osem.at[o])]

    def start(copies):
        for c in copies:
            c.start()

    def wait(copies):
        for c in copies:
            c.wait()

    start(fetch_kv())
    start(fetch_head(0))
    L.norm()
    L.tables()
    L.bias()
    wait(fetch_kv())
    L.keys(r.wbuf.at[0, 0], r.wbuf.at[0, 1])
    pltpu.make_async_copy(r.k, r.kc.at[0], r.csem.at[0]).start()
    pltpu.make_async_copy(r.v, r.vc.at[0], r.csem.at[1]).start()

    @pl.loop(0, H)
    def _(h):
        @pl.when(h + 1 < H)
        def _():
            start(fetch_head(h + 1))

        wait(fetch_head(h))
        L.query(r.wbuf.at[1, lax.rem(h, 2)])
        L.attend()
        for t in range(tiles):
            L.add_out(r.o, r.obuf.at[lax.rem(h, 2)], t)

    start(fetch_mlp(0))
    start(fetch_mlp(1))

    wait(fetch_mlp(0))
    for m in range(mbs):
        L.gated(m, r.wbuf.at[0, 0], r.wbuf.at[0, 1], r.a.at[0])

    @pl.loop(1, J)
    def _(j):
        @pl.when(j + 1 < J)
        def _():
            start(fetch_mlp(j + 1))

        wait(fetch_mlp(j))
        s = lax.rem(j, 2)
        prev = r.obuf.at[lax.rem(j - 1, 3)]
        per = tiles // mbs
        for m in range(mbs):
            L.gated(m, r.wbuf.at[s, 0], r.wbuf.at[s, 1], r.a.at[s])
            for t in range(m * per, (m + 1) * per):
                L.add_out(r.a.at[1 - s], prev, t)

    for t in range(tiles):
        L.add_out(r.a.at[(J - 1) % 2], r.obuf.at[(J - 1) % 3], t)
    L.finish()
    pltpu.make_async_copy(r.k, r.kc.at[0], r.csem.at[0]).wait()
    pltpu.make_async_copy(r.v, r.vc.at[0], r.csem.at[1]).wait()


def layer(d, x, prompt_len, ln_row, w):
    T, E, HD = d["T"], d["E"], d["HD"]
    half = HD // 2
    inv_freq = np.float64(ROPE_BASE) ** (-2.0 * np.arange(half) / HD)
    steps = np.concatenate([np.arange(Layer.QB), np.arange(T // Layer.QB) * Layer.QB])
    angles = steps[:, None] * inv_freq[None, :]
    rc = jnp.asarray(np.cos(angles), jnp.float32)
    rs = jnp.asarray(np.sin(angles), jnp.float32)
    hbm, vmem = pl.BlockSpec(memory_space=HBM), pl.BlockSpec(memory_space=pltpu.VMEM)
    flops = 2 * T * E * d["COLS"] + 2 * T * T * HD * d["H"]
    return pl.pallas_call(
        functools.partial(layer_kernel, d),
        out_shape=(jax.ShapeDtypeStruct(x.shape, jnp.bfloat16),
                   jax.ShapeDtypeStruct((1, T, HD), jnp.bfloat16), jax.ShapeDtypeStruct((1, T, HD), jnp.bfloat16)),
        in_specs=[hbm, pl.BlockSpec(memory_space=pltpu.SMEM), vmem, vmem, vmem, hbm],
        out_specs=(hbm, hbm, hbm),
        scratch_shapes=layer_scratch(d),
        compiler_params=pltpu.CompilerParams(vmem_limit_bytes=VMEM_LIMIT),
        cost_estimate=pl.CostEstimate(flops=flops, bytes_accessed=4 * T * E + 2 * E * d["COLS"], transcendentals=0),
        name="layer",
    )(x, prompt_len, ln_row, rc, rs, w)


def solution(mesh):
    batch_spec = P(("pod", "d"))

    def local_layer(x, prompt_len, ln_shard, w_in_shard, w_out_shard):
        d = dims(mesh, x, w_in_shard, w_out_shard)
        w, ln_row = gather(d, mesh, ln_shard, w_in_shard, w_out_shard.T)
        return layer(d, x, prompt_len, ln_row, w)

    return jax.shard_map(local_layer, mesh=mesh,
                         in_specs=(batch_spec, batch_spec, P("d"), P("d", None), P(None, "d")),
                         out_specs=(batch_spec, batch_spec, batch_spec), check_vma=False)
```

```python
import functools
import math

import jax
import jax.numpy as jnp
import numpy as np
from jax import lax
from jax.experimental import pallas as pl
from jax.experimental.pallas import tpu as pltpu
from jax.sharding import PartitionSpec as P

EPS = 1e-6
ROPE_BASE = 10000.0
MASKED = -1e30
MESH = pl.DeviceIdType.MESH
HBM = pltpu.HBM
VMEM_LIMIT = 67043328

CHUNK = 768
LAG = (0, 1, 2, 4, 6, 7)
HEAD_POINTS = 10


def dims(mesh, x, w_in, w_out):
    devices = mesh.shape["d"]
    cores = 2
    side = math.isqrt(devices // cores)
    model = x.shape[2]
    ffn = 4 * model
    attn = w_out.shape[0] - ffn
    head = (w_in.shape[1] - 2 * ffn - attn) // 2
    return dict(D=devices, CORES=cores, SIDE=side, T=x.shape[1], E=model, F=ffn, H=attn // head, HD=head,
                R=model // devices, COLS=w_in.shape[1] + w_out.shape[0], FC=head)


def place():
    return lax.axis_index("d")


def order_copies(d, win_ref, wot_ref, stage_ref, sem):
    F, H, HD, FC = d["F"], d["H"], d["HD"], d["FC"]
    qs = 2 * F
    ks = qs + H * HD
    pltpu.make_async_copy(win_ref.at[:, pl.ds(ks, 2 * HD)], stage_ref.at[:, pl.ds(0, 2 * HD)], sem).start()

    @pl.loop(0, H)
    def _(h):
        at = pl.multiple_of(2 * HD + h * 2 * HD, HD)
        pltpu.make_async_copy(win_ref.at[:, pl.ds(pl.multiple_of(qs + h * HD, HD), HD)],
                              stage_ref.at[:, pl.ds(at, HD)], sem).start()
        pltpu.make_async_copy(wot_ref.at[:, pl.ds(pl.multiple_of(F + h * HD, HD), HD)],
                              stage_ref.at[:, pl.ds(at + HD, HD)], sem).start()

    base = 2 * HD + H * 2 * HD

    @pl.loop(0, F // FC)
    def _(j):
        at = pl.multiple_of(base + j * 3 * FC, FC)
        pltpu.make_async_copy(win_ref.at[:, pl.ds(pl.multiple_of(j * FC, FC), FC)],
                              stage_ref.at[:, pl.ds(at, FC)], sem).start()
        pltpu.make_async_copy(win_ref.at[:, pl.ds(pl.multiple_of(F + j * FC, FC), FC)],
                              stage_ref.at[:, pl.ds(at + FC, FC)], sem).start()
        pltpu.make_async_copy(wot_ref.at[:, pl.ds(pl.multiple_of(j * FC, FC), FC)],
                              stage_ref.at[:, pl.ds(at + 2 * FC, FC)], sem).start()


class Comm:
    def __init__(self, d, stage_ref, w_ref, send_sem, recv_sem):
        self.d = d
        self.stage, self.w, self.send, self.recv = stage_ref, w_ref, send_sem, recv_sem
        self.groups = d["COLS"] // CHUNK
        side, cores = d["SIDE"], d["CORES"]
        me = place()
        self.me = me
        self.core = lax.rem(me, cores)
        self.x = lax.rem(lax.div(me, cores), side)
        self.y = lax.div(me, cores * side)

    def dev(self, y, x, core):
        d = self.d
        return {"d": (y * d["SIDE"] + x) * d["CORES"] + core}

    def wrap(self, v):
        side = self.d["SIDE"]
        return lax.rem(v + side, side)

    def put(self, src, dst, stage, g, device):
        return pltpu.make_async_remote_copy(src_ref=src, dst_ref=dst, send_sem=self.send.at[stage],
                                            recv_sem=self.recv.at[stage, g], device_id=device, device_id_type=MESH)

    def landed(self, ref, stage, g):
        pltpu.make_async_copy(ref, ref, self.recv.at[stage, g]).wait()

    def stage_fn(self, stage, g):
        w, x, y, c = self.w, self.x, self.y, self.core
        half = self.d["R"] // 2
        cols = pl.ds(pl.multiple_of(g * CHUNK, 128), CHUNK)
        ra, rb = pl.ds(0, half), pl.ds(half, half)
        turn = 1 - 2 * lax.rem(g, 2)
        if stage == 0:
            for s in (1, -1):
                self.put(self.stage.at[ra, cols], w.at[y, x, c, ra, cols], 0, g,
                         self.dev(y, self.wrap(x + s), c)).start()
                self.put(self.stage.at[rb, cols], w.at[y, x, c, rb, cols], 0, g,
                         self.dev(self.wrap(y + s), x, c)).start()
        elif stage == 1:
            self.landed(w.at[0, 0:2, :, ra, cols], 0, g)
            xs, ys = self.wrap(x - turn), self.wrap(y + turn)
            a = w.at[y, xs, c, ra, cols]
            self.put(a, a, 1, g, self.dev(y, self.wrap(x + turn), c)).start()
            b = w.at[ys, x, c, rb, cols]
            self.put(b, b, 1, g, self.dev(self.wrap(y - turn), x, c)).start()
        elif stage == 2:
            self.landed(w.at[0, 0, :, ra, cols], 1, g)
            a = w.at[y, :, c, ra, cols]
            b = w.at[:, x, c, rb, cols]
            for s in (1, -1):
                self.put(a, a, 2, g, self.dev(self.wrap(y + s), x, c)).start()
                self.put(b, b, 2, g, self.dev(y, self.wrap(x + s), c)).start()
        elif stage == 3:
            self.landed(w.at[0:2, :, :, ra, cols], 2, g)
            ys, xs = self.wrap(y - turn), self.wrap(x + turn)
            a = w.at[ys, :, c, ra, cols]
            self.put(a, a, 3, g, self.dev(self.wrap(y + turn), x, c)).start()
            b = w.at[:, xs, c, rb, cols]
            self.put(b, b, 3, g, self.dev(y, self.wrap(x - turn), c)).start()
        elif stage == 4:
            self.landed(w.at[0, :, :, ra, cols], 3, g)
            a = w.at[:, :, c, :, cols]
            self.put(a, a, 4, g, self.dev(y, x, 1 - c)).start()
        else:
            self.landed(w.at[:, :, 0, :, cols], 4, g)

    def point(self, p):
        for stage in range(6):
            g = p - LAG[stage]
            if isinstance(g, int):
                if 0 <= g < self.groups:
                    self.stage_fn(stage, g)
            else:
                @pl.when(jnp.logical_and(g >= 0, g < self.groups))
                def _(stage=stage, g=g):
                    self.stage_fn(stage, g)

    def drain(self):
        side, w = self.d["SIDE"], self.w
        for stage, ref in ((0, w.at[0, 0]), (1, w.at[0, 0, 0]), (2, w.at[0]), (3, w.at[0, 0:side // 2]),
                           (4, w.at[0:side // 2])):
            pltpu.make_async_copy(ref, ref, self.send.at[stage]).wait()


def meet(d):
    barrier = pltpu.get_barrier_semaphore()
    me = place()

    @pl.loop(1, d["D"])
    def _(i):
        pl.semaphore_signal(barrier, inc=1, device_id={"d": lax.rem(me + i, d["D"])}, device_id_type=MESH)

    pl.semaphore_wait(barrier, d["D"] - 1)


def spread_scale(d, ln_ref, ln_all, ln_send, ln_recv):
    me = place()

    @pl.loop(1, d["D"])
    def _(i):
        pltpu.make_async_remote_copy(src_ref=ln_ref, dst_ref=ln_all.at[me], send_sem=ln_send, recv_sem=ln_recv,
                                     device_id={"d": lax.rem(me + i, d["D"])}, device_id_type=MESH).start()

    ln_all[me] = ln_ref[...]


def spread_scale_wait(d, ln_all, ln_send, ln_recv):
    rest = ln_all.at[pl.ds(0, d["D"] - 1)]
    pltpu.make_async_copy(rest, rest, ln_recv).wait()
    pltpu.make_async_copy(rest, rest, ln_send).wait()


def scale_row(d, ln_all, row_ref):
    lane = lax.broadcasted_iota(jnp.int32, (1, 128), 1)
    per = 128 // d["R"]
    for i in range(d["E"] // 128):
        part = ln_all[per * i][0:1, :]
        for k in range(1, per):
            part = jnp.where(lane < k * d["R"], part, ln_all[per * i + k][0:1, :])
        row_ref[0:1, i * 128:(i + 1) * 128] = part


def nn(a, b):
    return lax.dot_general(a, b, (((1,), (0,)), ((), ())), preferred_element_type=jnp.float32)


def nt(a, b):
    return lax.dot_general(a, b, (((1,), (1,)), ((), ())), preferred_element_type=jnp.float32)


def rope(u, cos, sin):
    half = u.shape[1] // 2
    u1, u2 = u[:, :half], u[:, half:]
    return jnp.concatenate([u1 * cos - u2 * sin, u2 * cos + u1 * sin], axis=1)


class Layer:
    XB = 128
    MB = 512
    QB = 256

    def __init__(self, d, r):
        self.d, self.r = d, r

    def x_copy(self, i):
        rows = pl.ds(pl.multiple_of(i * self.XB, self.XB), self.XB)
        return pltpu.make_async_copy(self.r.x.at[0, rows, :], self.r.h.at[rows, :], self.r.xsem.at[i])

    def y_copy(self, m):
        rows = pl.ds(m * self.MB, self.MB)
        return pltpu.make_async_copy(self.r.h.at[rows, :], self.r.y.at[0, rows, :], self.r.xsem.at[m])

    def unit(self, col, buf, sem):
        return pltpu.make_async_copy(self.r.w.at[:, :, :, :, pl.ds(pl.multiple_of(col, 128), self.d["FC"])], buf, sem)

    def wval(self, buf):
        return buf[...].reshape(self.d["E"], self.d["FC"])

    def norm(self, i):
        r = self.r
        self.x_copy(i).wait()
        rows = pl.ds(pl.multiple_of(i * self.XB, self.XB), self.XB)
        xf = r.h[rows, :].astype(jnp.float32)
        centered = xf - jnp.mean(xf, axis=-1, keepdims=True)
        var = jnp.mean(centered * centered, axis=-1, keepdims=True)
        r.h[rows, :] = (centered * lax.rsqrt(var + EPS) * r.ln[...]).astype(jnp.bfloat16)
        r.yacc[rows, :] = xf

    def tables(self):
        d, r = self.d, self.r
        lo = r.rc.shape[0] - d["T"] // self.QB
        cl, sl = r.rc[0:self.QB, :], r.rs[0:self.QB, :]
        for b in range(d["T"] // self.QB):
            cb, sb = r.rc[self.QB + b:self.QB + b + 1, :], r.rs[self.QB + b:self.QB + b + 1, :]
            rows = slice(b * self.QB, (b + 1) * self.QB)
            r.cos[rows, :] = cl * cb - sl * sb
            r.sin[rows, :] = sl * cb + cl * sb

    def bias(self):
        r, d = self.r, self.d
        col = lax.broadcasted_iota(jnp.int32, (8, d["T"]), 1)
        r.bias[...] = jnp.where(col < r.plen[0], 0.0, MASKED)

    def keys(self, kbuf, vbuf):
        r, d = self.r, self.d
        for m in range(d["T"] // self.MB):
            rows = slice(m * self.MB, (m + 1) * self.MB)
            hb = r.h[rows, :]
            r.k[rows, :] = rope(nn(hb, self.wval(kbuf)), r.cos[rows, :], r.sin[rows, :]).astype(jnp.bfloat16)
            r.v[rows, :] = nn(hb, self.wval(vbuf)).astype(jnp.bfloat16)

    def query(self, qbuf):
        r, d = self.r, self.d
        scale = 1.0 / math.sqrt(d["HD"])
        for m in range(d["T"] // self.MB):
            rows = slice(m * self.MB, (m + 1) * self.MB)
            q = rope(nn(r.h[rows, :], self.wval(qbuf)), r.cos[rows, :], r.sin[rows, :]).astype(jnp.bfloat16)
            r.q[rows, :] = q * jnp.bfloat16(scale)

    def attend(self):
        r, d = self.r, self.d
        qb = self.QB
        row = lax.broadcasted_iota(jnp.int32, (qb, qb), 0)
        col = lax.broadcasted_iota(jnp.int32, (qb, qb), 1)
        for b in range(d["T"] // qb):
            n = (b + 1) * qb
            rows = slice(b * qb, n)
            s = nt(r.q[rows, :], r.k[0:n, :]) + r.bias[0:1, 0:n]
            last = jnp.where(col <= row, s[:, n - qb:], MASKED)
            s = last if b == 0 else jnp.concatenate([s[:, :n - qb], last], axis=1)
            e = jnp.exp(s - jnp.max(s, axis=-1, keepdims=True))
            p = (e * (1.0 / jnp.sum(e, axis=-1, keepdims=True))).astype(jnp.bfloat16)
            r.o[rows, :] = nn(p, r.v[0:n, :]).astype(jnp.bfloat16)

    def add_out(self, a_ref, obuf, tile):
        r, d = self.r, self.d
        fc = d["FC"]
        per = fc // d["R"]
        cols = slice(tile * fc, (tile + 1) * fc)
        w = self.wval(obuf)[cols, :]
        r.yacc[:, cols] += nt(a_ref[...], w)

    def gated(self, m, gbuf, ubuf, a_ref):
        r = self.r
        rows = slice(m * self.MB, (m + 1) * self.MB)
        hb = r.h[rows, :]
        g = nn(hb, self.wval(gbuf))
        u = nn(hb, self.wval(ubuf))
        hg = g * 0.5
        a_ref[rows, :] = ((hg + hg * jnp.tanh(hg)) * u).astype(jnp.bfloat16)

    def finish(self, a_ref, obuf):
        d, r = self.d, self.r
        fc = d["FC"]
        for m in range(d["T"] // self.MB):
            rows = slice(m * self.MB, (m + 1) * self.MB)
            for t in range(d["E"] // fc):
                cols = slice(t * fc, (t + 1) * fc)
                total = r.yacc[rows, cols] + nt(a_ref[rows, :], self.wval(obuf)[cols, :])
                r.h[rows, cols] = total.astype(jnp.bfloat16)
            self.y_copy(m).start()
        for m in range(d["T"] // self.MB):
            self.y_copy(m).wait()


class Refs:
    pass


NAMES = ("ln_tile", "win", "wot", "x", "plen", "rc", "rs",
         "y", "kc", "vc", "w",
         "stage", "ln_all", "ln", "h", "yacc", "cos", "sin", "bias", "k", "v", "q", "o", "a", "wbuf", "obuf",
         "local_sem", "ln_send", "ln_recv", "send_sem", "recv_sem", "xsem", "wsem", "osem", "csem")


def scratch(d):
    T, E, HD, FC = d["T"], d["E"], d["HD"], d["FC"]
    unit = (d["SIDE"], d["SIDE"], d["CORES"], d["R"], FC)
    bf16, f32, dma = jnp.bfloat16, jnp.float32, pltpu.SemaphoreType.DMA
    return [
        pltpu.VMEM((d["R"], d["COLS"]), bf16),
        pltpu.VMEM((d["D"], 8, 128), f32),
        pltpu.VMEM((1, E), f32),
        pltpu.VMEM((T, E), bf16),
        pltpu.VMEM((T, E), f32),
        pltpu.VMEM((T, HD // 2), f32),
        pltpu.VMEM((T, HD // 2), f32),
        pltpu.VMEM((8, T), f32),
        pltpu.VMEM((T, HD), bf16),
        pltpu.VMEM((T, HD), bf16),
        pltpu.VMEM((T, HD), bf16),
        pltpu.VMEM((T, HD), bf16),
        pltpu.VMEM((2, T, FC), bf16),
        pltpu.VMEM((2, 2) + unit, bf16),
        pltpu.VMEM((3,) + unit, bf16),
        dma((2,)), dma, dma, dma((5,)), dma((5, d["COLS"] // CHUNK)),
        dma((T // Layer.XB,)), dma((2, 2)), dma((3,)), dma((2,)),
    ]


def kernel(d, *refs):
    r = Refs()
    for name, ref in zip(NAMES, refs, strict=True):
        setattr(r, name, ref)
    L = Layer(d, r)
    HD, FC, H = d["HD"], d["FC"], d["H"]
    J = d["F"] // FC
    tiles = d["E"] // FC
    mbs = d["T"] // L.MB
    xbs = d["T"] // L.XB
    base = 2 * HD + H * 2 * HD

    def fetch_kv():
        return [L.unit(0, r.wbuf.at[0, 0], r.wsem.at[0, 0]), L.unit(HD, r.wbuf.at[0, 1], r.wsem.at[0, 1])]

    def fetch_head(h):
        col = 2 * HD + h * 2 * HD
        s = lax.rem(h, 2)
        return [L.unit(col, r.wbuf.at[1, s], r.wsem.at[1, s]), L.unit(col + HD, r.obuf.at[s], r.osem.at[s])]

    def fetch_mlp(j):
        col = base + j * 3 * FC
        s = lax.rem(j, 2)
        o = lax.rem(j + H, 3)
        return [L.unit(col, r.wbuf.at[s, 0], r.wsem.at[s, 0]), L.unit(col + FC, r.wbuf.at[s, 1], r.wsem.at[s, 1]),
                L.unit(col + 2 * FC, r.obuf.at[o], r.osem.at[o])]

    def start(copies):
        for c in copies:
            c.start()

    def wait(copies):
        for c in copies:
            c.wait()

    groups = d["COLS"] // CHUNK
    total = groups + LAG[5]
    first = LAG[5] + 2
    over_mlp = max(total - first - HEAD_POINTS, 0)

    def head_points(h):
        return h * HEAD_POINTS // H

    def mlp_points(j):
        return j * over_mlp // (J - 1)

    def ready(points):
        return (points - LAG[5]) * CHUNK

    assert ready(first) >= 2 * HD + 2 * HD
    for h in range(H):
        assert ready(first + head_points(h + 1)) >= min(2 * HD + (h + 2) * 2 * HD, base)
    assert ready(first + HEAD_POINTS) >= base + 3 * FC
    for j in range(J - 1):
        assert ready(first + HEAD_POINTS + mlp_points(j + 1)) >= base + (j + 2) * 3 * FC, j

    order_copies(d, r.win, r.wot, r.stage, r.local_sem.at[0])
    for i in range(xbs):
        L.x_copy(i).start()
    comm = Comm(d, r.stage, r.w, r.send_sem, r.recv_sem)
    own = pltpu.make_async_copy(r.stage, r.w.at[comm.y, comm.x, comm.core], r.local_sem.at[1])
    meet(d)
    spread_scale(d, r.ln_tile, r.ln_all, r.ln_send, r.ln_recv)
    pltpu.make_async_copy(r.stage, r.stage, r.local_sem.at[0]).wait()
    own.start()
    for p in range(LAG[2]):
        comm.point(p)
    own.wait()
    L.tables()
    L.bias()
    spread_scale_wait(d, r.ln_all, r.ln_send, r.ln_recv)
    scale_row(d, r.ln_all, r.ln)
    per = -(-xbs // (first - 1 - LAG[2]))

    @pl.loop(LAG[2], first)
    def _(p):
        comm.point(p)

        @pl.loop(0, per)
        def _(k):
            i = (p - LAG[2]) * per + k

            @pl.when(i < xbs)
            def _():
                L.norm(i)

        @pl.when(p == first - 2)
        def _():
            start(fetch_kv())

    start(fetch_head(0))
    wait(fetch_kv())
    L.keys(r.wbuf.at[0, 0], r.wbuf.at[0, 1])
    pltpu.make_async_copy(r.k, r.kc.at[0], r.csem.at[0]).start()
    pltpu.make_async_copy(r.v, r.vc.at[0], r.csem.at[1]).start()

    @pl.loop(0, H)
    def _(h):
        lo, hi = lax.div(h * HEAD_POINTS, H), lax.div((h + 1) * HEAD_POINTS, H)

        @pl.loop(first + lo, first + hi)
        def _(p):
            comm.point(p)

        @pl.when(h + 1 < H)
        def _():
            start(fetch_head(h + 1))

        @pl.when(h + 1 == H)
        def _():
            start(fetch_mlp(0))

        wait(fetch_head(h))
        L.query(r.wbuf.at[1, lax.rem(h, 2)])
        L.attend()
        for t in range(tiles):
            L.add_out(r.o, r.obuf.at[lax.rem(h, 2)], t)

    wait(fetch_mlp(0))

    def mlp_point(j):
        lo, hi = lax.div(j * over_mlp, J - 1), lax.div((j + 1) * over_mlp, J - 1)

        @pl.loop(first + HEAD_POINTS + lo, first + HEAD_POINTS + hi)
        def _(p):
            comm.point(p)

    mlp_point(0)
    start(fetch_mlp(1))
    for m in range(mbs):
        L.gated(m, r.wbuf.at[0, 0], r.wbuf.at[0, 1], r.a.at[0])

    @pl.loop(1, J)
    def _(j):
        @pl.when(j + 1 < J)
        def _():
            mlp_point(j)
            start(fetch_mlp(j + 1))

        wait(fetch_mlp(j))
        s = lax.rem(j, 2)
        prev = r.obuf.at[lax.rem(j - 1 + H, 3)]
        per = tiles // mbs
        for m in range(mbs):
            L.gated(m, r.wbuf.at[s, 0], r.wbuf.at[s, 1], r.a.at[s])
            for t in range(m * per, (m + 1) * per):
                L.add_out(r.a.at[1 - s], prev, t)

    L.finish(r.a.at[(J - 1) % 2], r.obuf.at[(J - 1 + H) % 3])
    pltpu.make_async_copy(r.k, r.kc.at[0], r.csem.at[0]).wait()
    pltpu.make_async_copy(r.v, r.vc.at[0], r.csem.at[1]).wait()
    comm.drain()


def layer(d, x, prompt_len, ln, w_in, wot):
    T, E, HD = d["T"], d["E"], d["HD"]
    half = HD // 2
    inv_freq = np.float64(ROPE_BASE) ** (-2.0 * np.arange(half) / HD)
    steps = np.concatenate([np.arange(Layer.QB), np.arange(T // Layer.QB) * Layer.QB])
    angles = steps[:, None] * inv_freq[None, :]
    rc = jnp.asarray(np.cos(angles), jnp.float32)
    rs = jnp.asarray(np.sin(angles), jnp.float32)
    ln_tile = jnp.broadcast_to(jnp.tile(ln, 128 // d["R"])[None], (8, 128))
    w_shape = (d["SIDE"], d["SIDE"], d["CORES"], d["R"], d["COLS"])
    hbm, vmem = pl.BlockSpec(memory_space=HBM), pl.BlockSpec(memory_space=pltpu.VMEM)
    flops = 2 * T * E * d["COLS"] + 2 * T * T * HD * d["H"]
    cache = jax.ShapeDtypeStruct((1, T, HD), jnp.bfloat16)
    y, kc, vc, _ = pl.pallas_call(
        functools.partial(kernel, d),
        out_shape=(jax.ShapeDtypeStruct(x.shape, jnp.bfloat16), cache, cache,
                   jax.ShapeDtypeStruct(w_shape, jnp.bfloat16)),
        in_specs=[vmem, hbm, hbm, hbm, pl.BlockSpec(memory_space=pltpu.SMEM), vmem, vmem],
        out_specs=(hbm, hbm, hbm, hbm),
        scratch_shapes=scratch(d),
        compiler_params=pltpu.CompilerParams(collective_id=0, has_side_effects=True, vmem_limit_bytes=VMEM_LIMIT),
        cost_estimate=pl.CostEstimate(flops=flops, bytes_accessed=4 * T * E + 2 * E * d["COLS"], transcendentals=0),
        name="layer",
    )(ln_tile, w_in, wot, x, prompt_len, rc, rs)
    return y, kc, vc


def solution(mesh):
    batch_spec = P(("pod", "d"))

    def local_layer(x, prompt_len, ln_shard, w_in_shard, w_out_shard):
        d = dims(mesh, x, w_in_shard, w_out_shard)
        return layer(d, x, prompt_len, ln_shard, w_in_shard, w_out_shard.T)

    return jax.shard_map(local_layer, mesh=mesh,
                         in_specs=(batch_spec, batch_spec, P("d"), P("d", None), P(None, "d")),
                         out_specs=(batch_spec, batch_spec, batch_spec), check_vma=False)
```

```python
import functools
import math

import jax
import jax.numpy as jnp
import numpy as np
from jax import lax
from jax.experimental import pallas as pl
from jax.experimental.pallas import tpu as pltpu
from jax.sharding import PartitionSpec as P

EPS = 1e-6
ROPE_BASE = 10000.0
MASKED = -1e30
MESH = pl.DeviceIdType.MESH
HBM = pltpu.HBM
VMEM_LIMIT = 67043328

CHUNK = 768
LAG = (0, 2, 4, 6, 8, 9)
HEAD_POINTS = 8


def dims(mesh, x, w_in, w_out):
    devices = mesh.shape["d"]
    cores = 2
    side = math.isqrt(devices // cores)
    model = x.shape[2]
    ffn = 4 * model
    attn = w_out.shape[0] - ffn
    head = (w_in.shape[1] - 2 * ffn - attn) // 2
    return dict(D=devices, CORES=cores, SIDE=side, T=x.shape[1], E=model, F=ffn, H=attn // head, HD=head,
                R=model // devices, COLS=w_in.shape[1] + w_out.shape[0], FC=head)


def place():
    return lax.axis_index("d")


def order_copies(d, win_ref, wot_ref, stage_ref, sem):
    F, H, HD, FC = d["F"], d["H"], d["HD"], d["FC"]
    qs = 2 * F
    ks = qs + H * HD
    pltpu.make_async_copy(win_ref.at[:, pl.ds(ks, 2 * HD)], stage_ref.at[:, pl.ds(0, 2 * HD)], sem).start()

    @pl.loop(0, H)
    def _(h):
        at = pl.multiple_of(2 * HD + h * 2 * HD, HD)
        pltpu.make_async_copy(win_ref.at[:, pl.ds(pl.multiple_of(qs + h * HD, HD), HD)],
                              stage_ref.at[:, pl.ds(at, HD)], sem).start()
        pltpu.make_async_copy(wot_ref.at[:, pl.ds(pl.multiple_of(F + h * HD, HD), HD)],
                              stage_ref.at[:, pl.ds(at + HD, HD)], sem).start()

    base = 2 * HD + H * 2 * HD

    @pl.loop(0, F // FC)
    def _(j):
        at = pl.multiple_of(base + j * 3 * FC, FC)
        pltpu.make_async_copy(win_ref.at[:, pl.ds(pl.multiple_of(j * FC, FC), FC)],
                              stage_ref.at[:, pl.ds(at, FC)], sem).start()
        pltpu.make_async_copy(win_ref.at[:, pl.ds(pl.multiple_of(F + j * FC, FC), FC)],
                              stage_ref.at[:, pl.ds(at + FC, FC)], sem).start()
        pltpu.make_async_copy(wot_ref.at[:, pl.ds(pl.multiple_of(j * FC, FC), FC)],
                              stage_ref.at[:, pl.ds(at + 2 * FC, FC)], sem).start()


class Comm:
    def __init__(self, d, stage_ref, w_ref, send_sem, recv_sem):
        self.d = d
        self.stage, self.w, self.send, self.recv = stage_ref, w_ref, send_sem, recv_sem
        self.groups = d["COLS"] // CHUNK
        side, cores = d["SIDE"], d["CORES"]
        me = place()
        self.me = me
        self.core = lax.rem(me, cores)
        self.x = lax.rem(lax.div(me, cores), side)
        self.y = lax.div(me, cores * side)

    def dev(self, y, x, core):
        d = self.d
        return {"d": (y * d["SIDE"] + x) * d["CORES"] + core}

    def wrap(self, v):
        side = self.d["SIDE"]
        return lax.rem(v + side, side)

    def put(self, src, dst, stage, g, device):
        return pltpu.make_async_remote_copy(src_ref=src, dst_ref=dst, send_sem=self.send.at[stage],
                                            recv_sem=self.recv.at[stage, g], device_id=device, device_id_type=MESH)

    def landed(self, ref, stage, g):
        pltpu.make_async_copy(ref, ref, self.recv.at[stage, g]).wait()

    def stage_fn(self, stage, g):
        w, x, y, c = self.w, self.x, self.y, self.core
        half = self.d["R"] // 2
        cols = pl.ds(pl.multiple_of(g * CHUNK, 128), CHUNK)
        ra, rb = pl.ds(0, half), pl.ds(half, half)
        turn = 1 - 2 * lax.rem(g, 2)
        if stage == 0:
            for s in (1, -1):
                self.put(self.stage.at[ra, cols], w.at[y, x, c, ra, cols], 0, g,
                         self.dev(y, self.wrap(x + s), c)).start()
                self.put(self.stage.at[rb, cols], w.at[y, x, c, rb, cols], 0, g,
                         self.dev(self.wrap(y + s), x, c)).start()
        elif stage == 1:
            self.landed(w.at[0, 0:2, :, ra, cols], 0, g)
            xs, ys = self.wrap(x - turn), self.wrap(y + turn)
            a = w.at[y, xs, c, ra, cols]
            self.put(a, a, 1, g, self.dev(y, self.wrap(x + turn), c)).start()
            b = w.at[ys, x, c, rb, cols]
            self.put(b, b, 1, g, self.dev(self.wrap(y - turn), x, c)).start()
        elif stage == 2:
            self.landed(w.at[0, 0, :, ra, cols], 1, g)
            a = w.at[y, :, c, ra, cols]
            b = w.at[:, x, c, rb, cols]
            for s in (1, -1):
                self.put(a, a, 2, g, self.dev(self.wrap(y + s), x, c)).start()
                self.put(b, b, 2, g, self.dev(y, self.wrap(x + s), c)).start()
        elif stage == 3:
            self.landed(w.at[0:2, :, :, ra, cols], 2, g)
            ys, xs = self.wrap(y - turn), self.wrap(x + turn)
            a = w.at[ys, :, c, ra, cols]
            self.put(a, a, 3, g, self.dev(self.wrap(y + turn), x, c)).start()
            b = w.at[:, xs, c, rb, cols]
            self.put(b, b, 3, g, self.dev(y, self.wrap(x - turn), c)).start()
        elif stage == 4:
            self.landed(w.at[0, :, :, ra, cols], 3, g)
            a = w.at[:, :, c, :, cols]
            self.put(a, a, 4, g, self.dev(y, x, 1 - c)).start()
        else:
            self.landed(w.at[:, :, 0, :, cols], 4, g)

    def point(self, p):
        for stage in (4, 3, 2, 1, 0, 5):
            g = p - LAG[stage]
            if isinstance(g, int):
                if 0 <= g < self.groups:
                    self.stage_fn(stage, g)
            else:
                @pl.when(jnp.logical_and(g >= 0, g < self.groups))
                def _(stage=stage, g=g):
                    self.stage_fn(stage, g)

    def drain(self):
        side, w = self.d["SIDE"], self.w
        for stage, ref in ((0, w.at[0, 0]), (1, w.at[0, 0, 0]), (2, w.at[0]), (3, w.at[0, 0:side // 2]),
                           (4, w.at[0:side // 2])):
            pltpu.make_async_copy(ref, ref, self.send.at[stage]).wait()


def meet(d):
    barrier = pltpu.get_barrier_semaphore()
    me = place()

    @pl.loop(1, d["D"])
    def _(i):
        pl.semaphore_signal(barrier, inc=1, device_id={"d": lax.rem(me + i, d["D"])}, device_id_type=MESH)

    pl.semaphore_wait(barrier, d["D"] - 1)


def spread_scale(d, ln_ref, ln_all, ln_send, ln_recv):
    me = place()

    @pl.loop(1, d["D"])
    def _(i):
        pltpu.make_async_remote_copy(src_ref=ln_ref, dst_ref=ln_all.at[me], send_sem=ln_send, recv_sem=ln_recv,
                                     device_id={"d": lax.rem(me + i, d["D"])}, device_id_type=MESH).start()

    ln_all[me] = ln_ref[...]


def spread_scale_wait(d, ln_all, ln_send, ln_recv):
    rest = ln_all.at[pl.ds(0, d["D"] - 1)]
    pltpu.make_async_copy(rest, rest, ln_recv).wait()
    pltpu.make_async_copy(rest, rest, ln_send).wait()


def scale_row(d, ln_all, row_ref):
    lane = lax.broadcasted_iota(jnp.int32, (1, 128), 1)
    per = 128 // d["R"]
    for i in range(d["E"] // 128):
        part = ln_all[per * i][0:1, :]
        for k in range(1, per):
            part = jnp.where(lane < k * d["R"], part, ln_all[per * i + k][0:1, :])
        row_ref[0:1, i * 128:(i + 1) * 128] = part


def nn(a, b):
    return lax.dot_general(a, b, (((1,), (0,)), ((), ())), preferred_element_type=jnp.float32)


def nt(a, b):
    return lax.dot_general(a, b, (((1,), (1,)), ((), ())), preferred_element_type=jnp.float32)


def rope(u, cos, sin):
    half = u.shape[1] // 2
    u1, u2 = u[:, :half], u[:, half:]
    return jnp.concatenate([u1 * cos - u2 * sin, u2 * cos + u1 * sin], axis=1)


class Layer:
    XB = 128
    MB = 512
    QB = 256

    def __init__(self, d, r):
        self.d, self.r = d, r

    def x_copy(self, i):
        rows = pl.ds(pl.multiple_of(i * self.XB, self.XB), self.XB)
        return pltpu.make_async_copy(self.r.x.at[0, rows, :], self.r.h.at[rows, :], self.r.xsem.at[i])

    def y_copy(self, m):
        rows = pl.ds(m * self.MB, self.MB)
        return pltpu.make_async_copy(self.r.h.at[rows, :], self.r.y.at[0, rows, :], self.r.xsem.at[m])

    def unit(self, col, buf, sem):
        return pltpu.make_async_copy(self.r.w.at[:, :, :, :, pl.ds(pl.multiple_of(col, 128), self.d["FC"])], buf, sem)

    def wval(self, buf):
        return buf[...].reshape(self.d["E"], self.d["FC"])

    def norm(self, i):
        r = self.r
        self.x_copy(i).wait()
        rows = pl.ds(pl.multiple_of(i * self.XB, self.XB), self.XB)
        xf = r.h[rows, :].astype(jnp.float32)
        centered = xf - jnp.mean(xf, axis=-1, keepdims=True)
        var = jnp.mean(centered * centered, axis=-1, keepdims=True)
        r.h[rows, :] = (centered * lax.rsqrt(var + EPS) * r.ln[...]).astype(jnp.bfloat16)
        r.yacc[rows, :] = xf

    def tables(self):
        d, r = self.d, self.r
        lo = r.rc.shape[0] - d["T"] // self.QB
        cl, sl = r.rc[0:self.QB, :], r.rs[0:self.QB, :]
        for b in range(d["T"] // self.QB):
            cb, sb = r.rc[self.QB + b:self.QB + b + 1, :], r.rs[self.QB + b:self.QB + b + 1, :]
            rows = slice(b * self.QB, (b + 1) * self.QB)
            r.cos[rows, :] = cl * cb - sl * sb
            r.sin[rows, :] = sl * cb + cl * sb

    def bias(self):
        r, d = self.r, self.d
        col = lax.broadcasted_iota(jnp.int32, (8, d["T"]), 1)
        r.bias[...] = jnp.where(col < r.plen[0], 0.0, MASKED)

    def keys(self, kbuf, vbuf):
        r, d = self.r, self.d
        for m in range(d["T"] // self.MB):
            rows = slice(m * self.MB, (m + 1) * self.MB)
            hb = r.h[rows, :]
            kf = rope(nn(hb, self.wval(kbuf)), r.cos[rows, :], r.sin[rows, :])
            r.k[rows, :] = kf.astype(jnp.bfloat16)
            r.kt[:, rows] = kf.T.astype(jnp.bfloat16)
            r.v[rows, :] = nn(hb, self.wval(vbuf)).astype(jnp.bfloat16)

    def query(self, m, qbuf, q_ref):
        r = self.r
        rows = slice(m * self.MB, (m + 1) * self.MB)
        q_ref[rows, :] = rope(nn(r.h[rows, :], self.wval(qbuf)), r.cos[rows, :], r.sin[rows, :]).astype(jnp.bfloat16)

    def scores(self, b, q_ref, z_ref):
        d, r = self.d, self.r
        qb, half = self.QB, self.QB // 2
        unit = math.log2(math.e) / math.sqrt(d["HD"])
        q = q_ref[b * qb:(b + 1) * qb, :]
        top = [None, None]
        for c in range(b + 1):
            cols = slice(c * qb, (c + 1) * qb)
            s = nn(q, r.kt[:, cols])
            for i in range(2):
                part = slice(i * half, (i + 1) * half)
                z = s[part, :] * unit + r.bias[0:1, cols]
                if c == b:
                    row = lax.broadcasted_iota(jnp.int32, (half, qb), 0) + i * half
                    col = lax.broadcasted_iota(jnp.int32, (half, qb), 1)
                    z = jnp.where(col <= row, z, MASKED)
                z_ref[part, cols] = z
                for k in range(qb // 128):
                    zk = z[:, k * 128:(k + 1) * 128]
                    top[i] = zk if top[i] is None else jnp.maximum(top[i], zk)
        return [jnp.max(t, axis=-1, keepdims=True) for t in top]

    def softmax(self, b, z_ref, p_ref, top):
        qb, half = self.QB, self.QB // 2
        for i in range(2):
            part = slice(i * half, (i + 1) * half)
            total = None
            for c in range(b + 1):
                cols = slice(c * qb, (c + 1) * qb)
                e = jnp.exp2(z_ref[part, cols] - top[i])
                z_ref[part, cols] = e
                for k in range(qb // 128):
                    ek = e[:, k * 128:(k + 1) * 128]
                    total = ek if total is None else total + ek
            inv = 1.0 / jnp.sum(total, axis=-1, keepdims=True)
            for c in range(b + 1):
                cols = slice(c * qb, (c + 1) * qb)
                p_ref[part, cols] = (z_ref[part, cols] * inv).astype(jnp.bfloat16)

    def values(self, b, p_ref, o_ref):
        r, qb = self.r, self.QB
        n = (b + 1) * qb
        o_ref[b * qb:n, :] = nn(p_ref[:, 0:n], r.v[0:n, :]).astype(jnp.bfloat16)

    def head(self, q_ref, o_ref, q_next, qbuf_next, o_prev, obuf_prev):
        d, r = self.d, self.r
        nb = d["T"] // self.QB
        mbs, tiles = d["T"] // self.MB, d["E"] // d["FC"]
        work = [functools.partial(self.add_out, o_prev, obuf_prev, t) for t in range(tiles)]
        per = tiles // mbs
        steps = []
        for m in range(mbs):
            steps += [work[m * per:(m + 1) * per], [functools.partial(self.query, m, qbuf_next, q_next)]]
        last = None
        for n, b in enumerate(reversed(range(nb))):
            z_ref, p_ref = r.z.at[n % 2], r.p.at[n % 2]
            top = self.scores(b, q_ref, z_ref)
            for f in steps[n]:
                f()
            self.softmax(b, z_ref, p_ref, top)
            if last is not None:
                self.values(*last)
            last = (b, p_ref, o_ref)
        self.values(*last)

    def add_out(self, a_ref, obuf, tile):
        r, d = self.r, self.d
        fc = d["FC"]
        per = fc // d["R"]
        cols = slice(tile * fc, (tile + 1) * fc)
        w = self.wval(obuf)[cols, :]
        r.yacc[:, cols] += nt(a_ref[...], w)

    def gated(self, m, gbuf, ubuf, a_ref):
        r = self.r
        rows = slice(m * self.MB, (m + 1) * self.MB)
        hb = r.h[rows, :]
        g = nn(hb, self.wval(gbuf))
        u = nn(hb, self.wval(ubuf))
        hg = g * 0.5
        a_ref[rows, :] = ((hg + hg * jnp.tanh(hg)) * u).astype(jnp.bfloat16)

    def finish(self, a_ref, obuf):
        d, r = self.d, self.r
        fc = d["FC"]
        for m in range(d["T"] // self.MB):
            rows = slice(m * self.MB, (m + 1) * self.MB)
            for t in range(d["E"] // fc):
                cols = slice(t * fc, (t + 1) * fc)
                total = r.yacc[rows, cols] + nt(a_ref[rows, :], self.wval(obuf)[cols, :])
                r.h[rows, cols] = total.astype(jnp.bfloat16)
            self.y_copy(m).start()
        for m in range(d["T"] // self.MB):
            self.y_copy(m).wait()


class Refs:
    pass


NAMES = ("ln_tile", "win", "wot", "x", "plen", "rc", "rs",
         "y", "kc", "vc", "w",
         "stage", "ln_all", "ln", "h", "yacc", "cos", "sin", "bias", "k", "kt", "v", "q", "o", "z", "p", "a", "wbuf", "obuf",
         "local_sem", "ln_send", "ln_recv", "send_sem", "recv_sem", "xsem", "wsem", "osem", "csem")


def scratch(d):
    T, E, HD, FC = d["T"], d["E"], d["HD"], d["FC"]
    unit = (d["SIDE"], d["SIDE"], d["CORES"], d["R"], FC)
    bf16, f32, dma = jnp.bfloat16, jnp.float32, pltpu.SemaphoreType.DMA
    return [
        pltpu.VMEM((d["R"], d["COLS"]), bf16),
        pltpu.VMEM((d["D"], 8, 128), f32),
        pltpu.VMEM((1, E), f32),
        pltpu.VMEM((T, E), bf16),
        pltpu.VMEM((T, E), f32),
        pltpu.VMEM((T, HD // 2), f32),
        pltpu.VMEM((T, HD // 2), f32),
        pltpu.VMEM((8, T), f32),
        pltpu.VMEM((T, HD), bf16),
        pltpu.VMEM((HD, T), bf16),
        pltpu.VMEM((T, HD), bf16),
        pltpu.VMEM((2, T, HD), bf16),
        pltpu.VMEM((2, T, HD), bf16),
        pltpu.VMEM((2, Layer.QB, T), f32),
        pltpu.VMEM((2, Layer.QB, T), bf16),
        pltpu.VMEM((2, T, FC), bf16),
        pltpu.VMEM((2, 2) + unit, bf16),
        pltpu.VMEM((3,) + unit, bf16),
        dma((2,)), dma, dma, dma((5,)), dma((5, d["COLS"] // CHUNK)),
        dma((T // Layer.XB,)), dma((2, 2)), dma((3,)), dma((2,)),
    ]


def kernel(d, *refs):
    r = Refs()
    for name, ref in zip(NAMES, refs, strict=True):
        setattr(r, name, ref)
    L = Layer(d, r)
    HD, FC, H = d["HD"], d["FC"], d["H"]
    J = d["F"] // FC
    tiles = d["E"] // FC
    mbs = d["T"] // L.MB
    xbs = d["T"] // L.XB
    base = 2 * HD + H * 2 * HD

    def fetch_kv():
        return [L.unit(0, r.wbuf.at[0, 0], r.wsem.at[0, 0]), L.unit(HD, r.wbuf.at[0, 1], r.wsem.at[0, 1])]

    def fetch_q(h):
        s = lax.rem(h, 2)
        return [L.unit(2 * HD + h * 2 * HD, r.wbuf.at[1, s], r.wsem.at[1, s])]

    def fetch_o(h):
        s = lax.rem(h, 3)
        return [L.unit(2 * HD + h * 2 * HD + HD, r.obuf.at[s], r.osem.at[s])]

    def fetch_mlp(j):
        col = base + j * 3 * FC
        s = lax.rem(j, 2)
        o = lax.rem(j + H, 3)
        return [L.unit(col, r.wbuf.at[s, 0], r.wsem.at[s, 0]), L.unit(col + FC, r.wbuf.at[s, 1], r.wsem.at[s, 1]),
                L.unit(col + 2 * FC, r.obuf.at[o], r.osem.at[o])]

    def start(copies):
        for c in copies:
            c.start()

    def wait(copies):
        for c in copies:
            c.wait()

    groups = d["COLS"] // CHUNK
    total = groups + LAG[5]
    first = LAG[5] + 2
    over_mlp = max(total - first - HEAD_POINTS, 0)

    def head_points(h):
        return h * HEAD_POINTS // H

    def mlp_points(j):
        return j * over_mlp // (J - 1)

    def ready(points):
        return (points - LAG[5]) * CHUNK

    assert ready(first) >= 2 * HD + 2 * HD
    assert ready(first) >= 2 * HD + 3 * HD
    for h in range(H):
        assert ready(first + head_points(h + 1)) >= min(2 * HD + (h + 2) * 2 * HD + HD, base)
    assert ready(first + HEAD_POINTS) >= base + 3 * FC
    for j in range(J - 1):
        assert ready(first + HEAD_POINTS + mlp_points(j + 1)) >= base + (j + 2) * 3 * FC, j

    order_copies(d, r.win, r.wot, r.stage, r.local_sem.at[0])
    for i in range(xbs):
        L.x_copy(i).start()
    comm = Comm(d, r.stage, r.w, r.send_sem, r.recv_sem)
    own = pltpu.make_async_copy(r.stage, r.w.at[comm.y, comm.x, comm.core], r.local_sem.at[1])
    meet(d)
    spread_scale(d, r.ln_tile, r.ln_all, r.ln_send, r.ln_recv)
    pltpu.make_async_copy(r.stage, r.stage, r.local_sem.at[0]).wait()
    own.start()
    for p in range(LAG[2]):
        comm.point(p)
    own.wait()
    L.tables()
    L.bias()
    spread_scale_wait(d, r.ln_all, r.ln_send, r.ln_recv)
    scale_row(d, r.ln_all, r.ln)
    per = -(-xbs // (first - 1 - LAG[2]))

    @pl.loop(LAG[2], first)
    def _(p):
        with jax.named_scope("point_start"):
            comm.point(p)

        @pl.loop(0, per)
        def _(k):
            i = (p - LAG[2]) * per + k

            @pl.when(i < xbs)
            def _():
                L.norm(i)

        @pl.when(p == first - 2)
        def _():
            start(fetch_kv())

    start(fetch_q(0))
    with jax.named_scope("wait_kv"):
        wait(fetch_kv())
    L.keys(r.wbuf.at[0, 0], r.wbuf.at[0, 1])
    pltpu.make_async_copy(r.k, r.kc.at[0], r.csem.at[0]).start()
    pltpu.make_async_copy(r.v, r.vc.at[0], r.csem.at[1]).start()
    start(fetch_q(1))
    start(fetch_o(0))
    wait(fetch_q(0))
    for m in range(mbs):
        L.query(m, r.wbuf.at[1, 0], r.q.at[0])
    r.o[1] = jnp.zeros((d["T"], HD), jnp.bfloat16)
    r.obuf[2] = jnp.zeros(r.obuf.shape[1:], jnp.bfloat16)

    @pl.loop(0, H)
    def _(h):
        lo, hi = lax.div(h * HEAD_POINTS, H), lax.div((h + 1) * HEAD_POINTS, H)

        @pl.loop(first + lo, first + hi)
        def _(p):
            with jax.named_scope("point_head"):
                comm.point(p)

        @pl.when(h + 1 < H)
        def _():
            wait(fetch_q(h + 1))
            start(fetch_o(h + 1))

        @pl.when(h + 2 < H)
        def _():
            start(fetch_q(h + 2))

        @pl.when(h > 0)
        def _():
            wait(fetch_o(h - 1))

        @pl.when(h + 1 == H)
        def _():
            start(fetch_mlp(0))

        s = lax.rem(h, 2)
        with jax.named_scope("head"):
            L.head(r.q.at[s], r.o.at[s], r.q.at[1 - s], r.wbuf.at[1, 1 - s], r.o.at[1 - s], r.obuf.at[lax.rem(h + 2, 3)])

    wait(fetch_o(H - 1))
    wait(fetch_mlp(0))

    def mlp_point(j):
        lo, hi = lax.div(j * over_mlp, J - 1), lax.div((j + 1) * over_mlp, J - 1)

        @pl.loop(first + HEAD_POINTS + lo, first + HEAD_POINTS + hi)
        def _(p):
            with jax.named_scope("point_mlp"):
                comm.point(p)

    mlp_point(0)
    start(fetch_mlp(1))
    per = tiles // mbs
    for m in range(mbs):
        L.gated(m, r.wbuf.at[0, 0], r.wbuf.at[0, 1], r.a.at[0])
        for t in range(m * per, (m + 1) * per):
            L.add_out(r.o.at[(H - 1) % 2], r.obuf.at[(H - 1) % 3], t)

    @pl.loop(1, J)
    def _(j):
        @pl.when(j + 1 < J)
        def _():
            mlp_point(j)
            start(fetch_mlp(j + 1))

        with jax.named_scope("wait_mlp"):
            wait(fetch_mlp(j))
        s = lax.rem(j, 2)
        prev = r.obuf.at[lax.rem(j - 1 + H, 3)]
        per = tiles // mbs
        with jax.named_scope("mlp"):
            for m in range(mbs):
                L.gated(m, r.wbuf.at[s, 0], r.wbuf.at[s, 1], r.a.at[s])
                for t in range(m * per, (m + 1) * per):
                    L.add_out(r.a.at[1 - s], prev, t)

    with jax.named_scope("finish"):
        L.finish(r.a.at[(J - 1) % 2], r.obuf.at[(J - 1 + H) % 3])
    pltpu.make_async_copy(r.k, r.kc.at[0], r.csem.at[0]).wait()
    pltpu.make_async_copy(r.v, r.vc.at[0], r.csem.at[1]).wait()
    comm.drain()


def layer(d, x, prompt_len, ln, w_in, wot):
    T, E, HD = d["T"], d["E"], d["HD"]
    half = HD // 2
    inv_freq = np.float64(ROPE_BASE) ** (-2.0 * np.arange(half) / HD)
    steps = np.concatenate([np.arange(Layer.QB), np.arange(T // Layer.QB) * Layer.QB])
    angles = steps[:, None] * inv_freq[None, :]
    rc = jnp.asarray(np.cos(angles), jnp.float32)
    rs = jnp.asarray(np.sin(angles), jnp.float32)
    ln_tile = jnp.broadcast_to(jnp.tile(ln, 128 // d["R"])[None], (8, 128))
    w_shape = (d["SIDE"], d["SIDE"], d["CORES"], d["R"], d["COLS"])
    hbm, vmem = pl.BlockSpec(memory_space=HBM), pl.BlockSpec(memory_space=pltpu.VMEM)
    flops = 2 * T * E * d["COLS"] + 2 * T * T * HD * d["H"]
    cache = jax.ShapeDtypeStruct((1, T, HD), jnp.bfloat16)
    y, kc, vc, _ = pl.pallas_call(
        functools.partial(kernel, d),
        out_shape=(jax.ShapeDtypeStruct(x.shape, jnp.bfloat16), cache, cache,
                   jax.ShapeDtypeStruct(w_shape, jnp.bfloat16)),
        in_specs=[vmem, hbm, hbm, hbm, pl.BlockSpec(memory_space=pltpu.SMEM), vmem, vmem],
        out_specs=(hbm, hbm, hbm, hbm),
        scratch_shapes=scratch(d),
        compiler_params=pltpu.CompilerParams(collective_id=0, has_side_effects=True, vmem_limit_bytes=VMEM_LIMIT),
        cost_estimate=pl.CostEstimate(flops=flops, bytes_accessed=4 * T * E + 2 * E * d["COLS"], transcendentals=0),
        name="layer",
    )(ln_tile, w_in, wot, x, prompt_len, rc, rs)
    return y, kc, vc


def solution(mesh):
    batch_spec = P(("pod", "d"))

    def local_layer(x, prompt_len, ln_shard, w_in_shard, w_out_shard):
        d = dims(mesh, x, w_in_shard, w_out_shard)
        return layer(d, x, prompt_len, ln_shard, w_in_shard, w_out_shard.T)

    return jax.shard_map(local_layer, mesh=mesh,
                         in_specs=(batch_spec, batch_spec, P("d"), P("d", None), P(None, "d")),
                         out_specs=(batch_spec, batch_spec, batch_spec), check_vma=False)
```

```python
import functools
import math

import jax
import jax.numpy as jnp
import numpy as np
from jax import lax
from jax.experimental import pallas as pl
from jax.experimental.pallas import tpu as pltpu
from jax.sharding import PartitionSpec as P

EPS = 1e-6
ROPE_BASE = 10000.0
MASKED = -1e30
MESH = pl.DeviceIdType.MESH
HBM = pltpu.HBM
VMEM_LIMIT = 67043328

SMALL, SMALL_WIDTH, WIDTH = 20, 384, 768
LAG = (0, 2, 4, 6, 8, 9)
FIRST = 12
NORM, KEYS, QUERY = 6, 7, 8
OPENING = (
    (0, 0), (0, 1), (0, 2), (0, 3), (0, 4), (0, 5), (0, 6), (1, 0), (1, 1), (0, 7), (1, 2), (1, 3), (0, 8), (1, 4),
    (NORM, 2), (1, 5), (NORM, 1), (1, 6), (NORM, 1), (2, 0), (2, 1), (NORM, 11), (1, 7), (NORM, 1), (1, 8), (0, 9),
    (3, 0), (2, 2), (3, 1), (2, 3), (4, 0), (1, 9), (0, 10), (3, 2), (2, 4), (4, 1), (5, 0), (3, 3), (2, 5), (5, 1),
    (KEYS, 1), (4, 2), (KEYS, 1), (1, 10), (4, 3), (KEYS, 1), (3, 4), (2, 6), (KEYS, 1), (5, 2), (3, 5), (2, 7),
    (QUERY, 2), (5, 3), (QUERY, 2), (0, 11))


def dims(mesh, x, w_in, w_out):
    devices = mesh.shape["d"]
    cores = 2
    side = math.isqrt(devices // cores)
    model = x.shape[2]
    ffn = 4 * model
    attn = w_out.shape[0] - ffn
    head = (w_in.shape[1] - 2 * ffn - attn) // 2
    return dict(D=devices, CORES=cores, SIDE=side, T=x.shape[1], E=model, F=ffn, H=attn // head, HD=head,
                R=model // devices, COLS=w_in.shape[1] + w_out.shape[0], FC=head)


def place():
    return lax.axis_index("d")


def order_copies(d, win_ref, wot_ref, stage_ref, sem):
    F, H, HD, FC = d["F"], d["H"], d["HD"], d["FC"]
    qs = 2 * F
    ks = qs + H * HD
    pltpu.make_async_copy(win_ref.at[:, pl.ds(ks, 2 * HD)], stage_ref.at[:, pl.ds(0, 2 * HD)], sem).start()

    @pl.loop(0, H)
    def _(h):
        at = pl.multiple_of(2 * HD + h * 2 * HD, HD)
        pltpu.make_async_copy(win_ref.at[:, pl.ds(pl.multiple_of(qs + h * HD, HD), HD)],
                              stage_ref.at[:, pl.ds(at, HD)], sem).start()
        pltpu.make_async_copy(wot_ref.at[:, pl.ds(pl.multiple_of(F + h * HD, HD), HD)],
                              stage_ref.at[:, pl.ds(at + HD, HD)], sem).start()

    base = 2 * HD + H * 2 * HD

    @pl.loop(0, F // FC)
    def _(j):
        at = pl.multiple_of(base + j * 3 * FC, FC)
        pltpu.make_async_copy(win_ref.at[:, pl.ds(pl.multiple_of(j * FC, FC), FC)],
                              stage_ref.at[:, pl.ds(at, FC)], sem).start()
        pltpu.make_async_copy(win_ref.at[:, pl.ds(pl.multiple_of(F + j * FC, FC), FC)],
                              stage_ref.at[:, pl.ds(at + FC, FC)], sem).start()
        pltpu.make_async_copy(wot_ref.at[:, pl.ds(pl.multiple_of(j * FC, FC), FC)],
                              stage_ref.at[:, pl.ds(at + 2 * FC, FC)], sem).start()


class Comm:
    def __init__(self, d, stage_ref, w_ref, send_sem, recv_sem):
        self.d = d
        self.stage, self.w, self.send, self.recv = stage_ref, w_ref, send_sem, recv_sem
        self.groups = SMALL + (d["COLS"] - SMALL * SMALL_WIDTH) // WIDTH
        self.done = [sum(1 for op in OPENING if op[0] == k) for k in range(6)]
        side, cores = d["SIDE"], d["CORES"]
        me = place()
        self.core = lax.rem(me, cores)
        self.x = lax.rem(lax.div(me, cores), side)
        self.y = lax.div(me, cores * side)

    @staticmethod
    def end(groups):
        return min(groups, SMALL) * SMALL_WIDTH + max(groups - SMALL, 0) * WIDTH

    def dev(self, y, x, core):
        d = self.d
        return {"d": (y * d["SIDE"] + x) * d["CORES"] + core}

    def wrap(self, v):
        side = self.d["SIDE"]
        return lax.rem(v + side, side)

    def put(self, src, dst, stage, g, device):
        return pltpu.make_async_remote_copy(src_ref=src, dst_ref=dst, send_sem=self.send.at[stage],
                                            recv_sem=self.recv.at[stage, g], device_id=device, device_id_type=MESH)

    def landed(self, ref, stage, g):
        pltpu.make_async_copy(ref, ref, self.recv.at[stage, g]).wait()

    def stage_fn(self, stage, g, small):
        w, x, y, c = self.w, self.x, self.y, self.core
        half = self.d["R"] // 2
        if small:
            cols = pl.ds(pl.multiple_of(g * SMALL_WIDTH, 128), SMALL_WIDTH)
        else:
            cols = pl.ds(pl.multiple_of(SMALL * SMALL_WIDTH + (g - SMALL) * WIDTH, 128), WIDTH)
        ra, rb = pl.ds(0, half), pl.ds(half, half)
        turn = 1 - 2 * lax.rem(g, 2)
        if stage == 0:
            for s in (1, -1):
                self.put(self.stage.at[ra, cols], w.at[y, x, c, ra, cols], 0, g,
                         self.dev(y, self.wrap(x + s), c)).start()
                self.put(self.stage.at[rb, cols], w.at[y, x, c, rb, cols], 0, g,
                         self.dev(self.wrap(y + s), x, c)).start()
        elif stage == 1:
            self.landed(w.at[0, 0:2, :, ra, cols], 0, g)
            xs, ys = self.wrap(x - turn), self.wrap(y + turn)
            a = w.at[y, xs, c, ra, cols]
            self.put(a, a, 1, g, self.dev(y, self.wrap(x + turn), c)).start()
            b = w.at[ys, x, c, rb, cols]
            self.put(b, b, 1, g, self.dev(self.wrap(y - turn), x, c)).start()
        elif stage == 2:
            self.landed(w.at[0, 0, :, ra, cols], 1, g)
            a = w.at[y, :, c, ra, cols]
            b = w.at[:, x, c, rb, cols]
            for s in (1, -1):
                self.put(a, a, 2, g, self.dev(self.wrap(y + s), x, c)).start()
                self.put(b, b, 2, g, self.dev(y, self.wrap(x + s), c)).start()
        elif stage == 3:
            self.landed(w.at[0:2, :, :, ra, cols], 2, g)
            ys, xs = self.wrap(y - turn), self.wrap(x + turn)
            a = w.at[ys, :, c, ra, cols]
            self.put(a, a, 3, g, self.dev(self.wrap(y + turn), x, c)).start()
            b = w.at[:, xs, c, rb, cols]
            self.put(b, b, 3, g, self.dev(y, self.wrap(x - turn), c)).start()
        elif stage == 4:
            self.landed(w.at[0, :, :, ra, cols], 3, g)
            a = w.at[:, :, c, :, cols]
            self.put(a, a, 4, g, self.dev(y, x, 1 - c)).start()
        else:
            self.landed(w.at[:, :, 0, :, cols], 4, g)

    def point(self, p, lo, hi):
        for stage in (4, 3, 2, 1, 0, 5):
            g = p - LAG[stage]
            for small, start, stop in ((True, 0, SMALL), (False, SMALL, self.groups)):
                start = max(start, self.done[stage])
                if hi - 1 - LAG[stage] < start or lo - LAG[stage] >= stop:
                    continue

                @pl.when(jnp.logical_and(g >= start, g < stop))
                def _(stage=stage, g=g, small=small):
                    self.stage_fn(stage, g, small)

    def drain(self):
        side, w = self.d["SIDE"], self.w
        for stage, ref in ((0, w.at[0, 0]), (1, w.at[0, 0, 0]), (2, w.at[0]), (3, w.at[0, 0:side // 2]),
                           (4, w.at[0:side // 2])):
            pltpu.make_async_copy(ref, ref, self.send.at[stage]).wait()


def arrive(d):
    barrier = pltpu.get_barrier_semaphore()
    me = place()

    @pl.loop(1, d["D"])
    def _(i):
        pl.semaphore_signal(barrier, inc=1, device_id={"d": lax.rem(me + i, d["D"])}, device_id_type=MESH)


def meet(d):
    pl.semaphore_wait(pltpu.get_barrier_semaphore(), d["D"] - 1)


def spread_scale(d, ln_ref, ln_all, ln_send, ln_recv):
    me = place()

    @pl.loop(1, d["D"])
    def _(i):
        pltpu.make_async_remote_copy(src_ref=ln_ref, dst_ref=ln_all.at[me], send_sem=ln_send, recv_sem=ln_recv,
                                     device_id={"d": lax.rem(me + i, d["D"])}, device_id_type=MESH).start()

    ln_all[me] = ln_ref[...]


def spread_scale_wait(d, ln_all, ln_send, ln_recv):
    rest = ln_all.at[pl.ds(0, d["D"] - 1)]
    pltpu.make_async_copy(rest, rest, ln_recv).wait()
    pltpu.make_async_copy(rest, rest, ln_send).wait()


def scale_row(d, ln_all, row_ref):
    lane = lax.broadcasted_iota(jnp.int32, (1, 128), 1)
    per = 128 // d["R"]
    for i in range(d["E"] // 128):
        part = ln_all[per * i][0:1, :]
        for k in range(1, per):
            part = jnp.where(lane < k * d["R"], part, ln_all[per * i + k][0:1, :])
        row_ref[0:1, i * 128:(i + 1) * 128] = part


def nn(a, b):
    return lax.dot_general(a, b, (((1,), (0,)), ((), ())), preferred_element_type=jnp.float32)


def nt(a, b):
    return lax.dot_general(a, b, (((1,), (1,)), ((), ())), preferred_element_type=jnp.float32)


def rope(u, cos, sin):
    half = u.shape[1] // 2
    u1, u2 = u[:, :half], u[:, half:]
    return jnp.concatenate([u1 * cos - u2 * sin, u2 * cos + u1 * sin], axis=1)


class Layer:
    XB = 128
    MB = 512
    QB = 256

    def __init__(self, d, r):
        self.d, self.r = d, r

    def x_copy(self, i):
        rows = pl.ds(pl.multiple_of(i * self.XB, self.XB), self.XB)
        return pltpu.make_async_copy(self.r.x.at[0, rows, :], self.r.h.at[rows, :], self.r.xsem.at[i])

    def y_copy(self, m):
        rows = pl.ds(m * self.MB, self.MB)
        return pltpu.make_async_copy(self.r.h.at[rows, :], self.r.y.at[0, rows, :], self.r.xsem.at[m])

    def unit(self, col, buf, sem):
        return pltpu.make_async_copy(self.r.w.at[:, :, :, :, pl.ds(pl.multiple_of(col, 128), self.d["FC"])], buf, sem)

    def wval(self, buf):
        return buf[...].reshape(self.d["E"], self.d["FC"])

    def norm(self, i):
        r = self.r
        self.x_copy(i).wait()
        rows = pl.ds(pl.multiple_of(i * self.XB, self.XB), self.XB)
        xf = r.h[rows, :].astype(jnp.float32)
        centered = xf - jnp.mean(xf, axis=-1, keepdims=True)
        var = jnp.mean(centered * centered, axis=-1, keepdims=True)
        r.h[rows, :] = (centered * lax.rsqrt(var + EPS) * r.ln[...]).astype(jnp.bfloat16)
        r.yacc[rows, :] = xf

    def tables(self):
        d, r = self.d, self.r
        lo = r.rc.shape[0] - d["T"] // self.QB
        cl, sl = r.rc[0:self.QB, :], r.rs[0:self.QB, :]
        for b in range(d["T"] // self.QB):
            cb, sb = r.rc[self.QB + b:self.QB + b + 1, :], r.rs[self.QB + b:self.QB + b + 1, :]
            rows = slice(b * self.QB, (b + 1) * self.QB)
            r.cos[rows, :] = cl * cb - sl * sb
            r.sin[rows, :] = sl * cb + cl * sb

    def bias(self):
        r, d = self.r, self.d
        col = lax.broadcasted_iota(jnp.int32, (8, d["T"]), 1)
        r.bias[...] = jnp.where(col < r.plen[0], 0.0, MASKED)

    def keys(self, m, kbuf, vbuf):
        r = self.r
        rows = slice(m * self.MB, (m + 1) * self.MB)
        hb = r.h[rows, :]
        kf = rope(nn(hb, self.wval(kbuf)), r.cos[rows, :], r.sin[rows, :])
        r.k[rows, :] = kf.astype(jnp.bfloat16)
        r.kt[:, rows] = kf.T.astype(jnp.bfloat16)
        r.v[rows, :] = nn(hb, self.wval(vbuf)).astype(jnp.bfloat16)

    def query(self, m, qbuf, q_ref):
        r = self.r
        rows = slice(m * self.MB, (m + 1) * self.MB)
        q_ref[rows, :] = rope(nn(r.h[rows, :], self.wval(qbuf)), r.cos[rows, :], r.sin[rows, :]).astype(jnp.bfloat16)

    def scores(self, b, q_ref, z_ref):
        d, r = self.d, self.r
        qb, half = self.QB, self.QB // 2
        unit = math.log2(math.e) / math.sqrt(d["HD"])
        q = q_ref[b * qb:(b + 1) * qb, :]
        top = [None, None]
        for c in range(b + 1):
            cols = slice(c * qb, (c + 1) * qb)
            s = nn(q, r.kt[:, cols])
            for i in range(2):
                part = slice(i * half, (i + 1) * half)
                z = s[part, :] * unit + r.bias[0:1, cols]
                if c == b:
                    row = lax.broadcasted_iota(jnp.int32, (half, qb), 0) + i * half
                    col = lax.broadcasted_iota(jnp.int32, (half, qb), 1)
                    z = jnp.where(col <= row, z, MASKED)
                z_ref[part, cols] = z
                for k in range(qb // 128):
                    zk = z[:, k * 128:(k + 1) * 128]
                    top[i] = zk if top[i] is None else jnp.maximum(top[i], zk)
        return [jnp.max(t, axis=-1, keepdims=True) for t in top]

    def softmax(self, b, z_ref, p_ref, top):
        qb, half = self.QB, self.QB // 2
        for i in range(2):
            part = slice(i * half, (i + 1) * half)
            total = None
            for c in range(b + 1):
                cols = slice(c * qb, (c + 1) * qb)
                e = jnp.exp2(z_ref[part, cols] - top[i])
                z_ref[part, cols] = e
                for k in range(qb // 128):
                    ek = e[:, k * 128:(k + 1) * 128]
                    total = ek if total is None else total + ek
            inv = 1.0 / jnp.sum(total, axis=-1, keepdims=True)
            for c in range(b + 1):
                cols = slice(c * qb, (c + 1) * qb)
                p_ref[part, cols] = (z_ref[part, cols] * inv).astype(jnp.bfloat16)

    def values(self, b, p_ref, o_ref):
        r, qb = self.r, self.QB
        n = (b + 1) * qb
        o_ref[b * qb:n, :] = nn(p_ref[:, 0:n], r.v[0:n, :]).astype(jnp.bfloat16)

    def head(self, q_ref, o_ref, q_next, qbuf_next, o_prev, obuf_prev, midway):
        d, r = self.d, self.r
        nb = d["T"] // self.QB
        mbs, tiles = d["T"] // self.MB, d["E"] // d["FC"]
        work = [functools.partial(self.add_out, o_prev, obuf_prev, t) for t in range(tiles)]
        per = tiles // mbs
        steps = []
        for m in range(mbs):
            steps += [work[m * per:(m + 1) * per], [functools.partial(self.query, m, qbuf_next, q_next)]]
        last = None
        for n, b in enumerate(reversed(range(nb))):
            if n == nb // 2:
                midway()
            z_ref, p_ref = r.z.at[n % 2], r.p.at[n % 2]
            top = self.scores(b, q_ref, z_ref)
            for f in steps[n]:
                f()
            self.softmax(b, z_ref, p_ref, top)
            if last is not None:
                self.values(*last)
            last = (b, p_ref, o_ref)
        self.values(*last)

    def add_out(self, a_ref, obuf, tile):
        r, d = self.r, self.d
        fc = d["FC"]
        per = fc // d["R"]
        cols = slice(tile * fc, (tile + 1) * fc)
        w = self.wval(obuf)[cols, :]
        r.yacc[:, cols] += nt(a_ref[...], w)

    def gated(self, m, gbuf, ubuf, a_ref):
        r = self.r
        rows = slice(m * self.MB, (m + 1) * self.MB)
        hb = r.h[rows, :]
        g = nn(hb, self.wval(gbuf))
        u = nn(hb, self.wval(ubuf))
        hg = g * 0.5
        a_ref[rows, :] = ((hg + hg * jnp.tanh(hg)) * u).astype(jnp.bfloat16)

    def finish(self, a_ref, obuf):
        d, r = self.d, self.r
        fc = d["FC"]
        for m in range(d["T"] // self.MB):
            rows = slice(m * self.MB, (m + 1) * self.MB)
            for t in range(d["E"] // fc):
                cols = slice(t * fc, (t + 1) * fc)
                total = r.yacc[rows, cols] + nt(a_ref[rows, :], self.wval(obuf)[cols, :])
                r.h[rows, cols] = total.astype(jnp.bfloat16)
            self.y_copy(m).start()
        for m in range(d["T"] // self.MB):
            self.y_copy(m).wait()


class Refs:
    pass


NAMES = ("ln_tile", "win", "wot", "x", "plen", "rc", "rs",
         "y", "kc", "vc", "w",
         "stage", "ln_all", "ln", "h", "yacc", "cos", "sin", "bias", "k", "kt", "v", "q", "o", "z", "p", "a", "wbuf", "obuf",
         "local_sem", "ln_send", "ln_recv", "send_sem", "recv_sem", "xsem", "wsem", "osem", "csem")


def scratch(d):
    T, E, HD, FC = d["T"], d["E"], d["HD"], d["FC"]
    unit = (d["SIDE"], d["SIDE"], d["CORES"], d["R"], FC)
    bf16, f32, dma = jnp.bfloat16, jnp.float32, pltpu.SemaphoreType.DMA
    return [
        pltpu.VMEM((d["R"], d["COLS"]), bf16),
        pltpu.VMEM((d["D"], 8, 128), f32),
        pltpu.VMEM((1, E), f32),
        pltpu.VMEM((T, E), bf16),
        pltpu.VMEM((T, E), f32),
        pltpu.VMEM((T, HD // 2), f32),
        pltpu.VMEM((T, HD // 2), f32),
        pltpu.VMEM((8, T), f32),
        pltpu.VMEM((T, HD), bf16),
        pltpu.VMEM((HD, T), bf16),
        pltpu.VMEM((T, HD), bf16),
        pltpu.VMEM((2, T, HD), bf16),
        pltpu.VMEM((2, T, HD), bf16),
        pltpu.VMEM((2, Layer.QB, T), f32),
        pltpu.VMEM((2, Layer.QB, T), bf16),
        pltpu.VMEM((2, T, FC), bf16),
        pltpu.VMEM((2, 2) + unit, bf16),
        pltpu.VMEM((3,) + unit, bf16),
        dma((2,)), dma, dma, dma((5,)), dma((5, SMALL + (d["COLS"] - SMALL * SMALL_WIDTH) // WIDTH)),
        dma((T // Layer.XB,)), dma((2, 2)), dma((3,)), dma((2,)),
    ]


def kernel(d, *refs):
    r = Refs()
    for name, ref in zip(NAMES, refs, strict=True):
        setattr(r, name, ref)
    L = Layer(d, r)
    HD, FC, H = d["HD"], d["FC"], d["H"]
    J = d["F"] // FC
    tiles = d["E"] // FC
    mbs = d["T"] // L.MB
    xbs = d["T"] // L.XB
    base = 2 * HD + H * 2 * HD

    def fetch_kv():
        return [L.unit(0, r.wbuf.at[0, 0], r.wsem.at[0, 0]), L.unit(HD, r.wbuf.at[0, 1], r.wsem.at[0, 1])]

    def fetch_q(h):
        s = lax.rem(h, 2)
        return [L.unit(2 * HD + h * 2 * HD, r.wbuf.at[1, s], r.wsem.at[1, s])]

    def fetch_o(h):
        s = lax.rem(h, 3)
        return [L.unit(2 * HD + h * 2 * HD + HD, r.obuf.at[s], r.osem.at[s])]

    def fetch_mlp(j):
        col = base + j * 3 * FC
        s = lax.rem(j, 2)
        o = lax.rem(j + H, 3)
        return [L.unit(col, r.wbuf.at[s, 0], r.wsem.at[s, 0]), L.unit(col + FC, r.wbuf.at[s, 1], r.wsem.at[s, 1]),
                L.unit(col + 2 * FC, r.obuf.at[o], r.osem.at[o])]

    def start(copies):
        for c in copies:
            c.start()

    def wait(copies):
        for c in copies:
            c.wait()

    comm = Comm(d, r.stage, r.w, r.send_sem, r.recv_sem)
    after_heads = FIRST + 2 * H
    last = comm.groups + LAG[5]
    over_mlp = last - after_heads

    def ready(points):
        return comm.end(max(points - LAG[5], comm.done[5]))

    for k in range(6):
        assert comm.done[k] >= min(FIRST - LAG[k], comm.groups)
    assert ready(FIRST) >= 2 * HD + 3 * HD
    for h in range(1, H):
        assert ready(FIRST + 2 * h + 1) >= min(2 * HD + (h + 2) * 2 * HD + HD, base)
    assert ready(FIRST + 2 * H - 1) >= base + 3 * FC
    for j in range(J - 1):
        assert ready(after_heads + (j + 1) * over_mlp // (J - 1)) >= base + (j + 2) * 3 * FC

    arrive(d)
    order_copies(d, r.win, r.wot, r.stage, r.local_sem.at[0])
    for i in range(xbs):
        L.x_copy(i).start()
    own = pltpu.make_async_copy(r.stage, r.w.at[comm.y, comm.x, comm.core], r.local_sem.at[1])
    pltpu.make_async_copy(r.stage, r.stage, r.local_sem.at[0]).wait()
    own.start()
    meet(d)
    normed = keyed = queried = 0
    for n, (what, g) in enumerate(OPENING):
        if what <= 5:
            if (what, g) == (2, 0):
                own.wait()
            comm.stage_fn(what, g, g < SMALL)
            if n == 0:
                spread_scale(d, r.ln_tile, r.ln_all, r.ln_send, r.ln_recv)
            if what == 5 and comm.end(g) < 3 * HD <= comm.end(g + 1):
                start(fetch_kv())
                start(fetch_q(0))
            if what == 5 and comm.end(g) < 5 * HD <= comm.end(g + 1):
                start(fetch_q(1))
                start(fetch_o(0))
        elif what == NORM:
            if normed == 0:
                L.tables()
                L.bias()
                spread_scale_wait(d, r.ln_all, r.ln_send, r.ln_recv)
                scale_row(d, r.ln_all, r.ln)
            many = min(g, xbs - normed)
            if many > 0:
                @pl.loop(normed, normed + many)
                def _(i):
                    L.norm(i)
            normed += many
        elif what == KEYS:
            if keyed == 0:
                assert normed == xbs
                wait(fetch_kv())
            if keyed < mbs:
                L.keys(keyed, r.wbuf.at[0, 0], r.wbuf.at[0, 1])
            keyed += 1
            if keyed == mbs:
                pltpu.make_async_copy(r.k, r.kc.at[0], r.csem.at[0]).start()
                pltpu.make_async_copy(r.v, r.vc.at[0], r.csem.at[1]).start()
        else:
            if queried == 0:
                wait(fetch_q(0))
            for m in range(queried, min(queried + g, mbs)):
                L.query(m, r.wbuf.at[1, 0], r.q.at[0])
            queried += g
    r.o[1] = jnp.zeros((d["T"], HD), jnp.bfloat16)
    r.obuf[2] = jnp.zeros(r.obuf.shape[1:], jnp.bfloat16)

    @pl.loop(0, H)
    def _(h):
        with jax.named_scope("point_head"):
            comm.point(FIRST + 2 * h, FIRST, after_heads)

        @pl.when(h == 1)
        def _():
            start(fetch_o(h))
            start(fetch_q(h + 1))

        @pl.when(jnp.logical_and(h > 0, h + 1 < H))
        def _():
            start(fetch_o(h + 1))

        @pl.when(jnp.logical_and(h > 0, h + 2 < H))
        def _():
            start(fetch_q(h + 2))

        @pl.when(h + 1 < H)
        def _():
            wait(fetch_q(h + 1))

        @pl.when(h > 0)
        def _():
            wait(fetch_o(h - 1))

        @pl.when(h + 1 == H)
        def _():
            start(fetch_mlp(0))

        s = lax.rem(h, 2)

        def midway():
            with jax.named_scope("point_mid"):
                comm.point(FIRST + 2 * h + 1, FIRST, after_heads)

        with jax.named_scope("head"):
            L.head(r.q.at[s], r.o.at[s], r.q.at[1 - s], r.wbuf.at[1, 1 - s], r.o.at[1 - s], r.obuf.at[lax.rem(h + 2, 3)], midway)

    wait(fetch_o(H - 1))
    wait(fetch_mlp(0))

    def mlp_point(j, lo, hi):
        @pl.loop(after_heads + lax.div(j * over_mlp, J - 1), after_heads + lax.div((j + 1) * over_mlp, J - 1))
        def _(p):
            with jax.named_scope("point_mlp"):
                comm.point(p, lo, hi)

    opening = after_heads + -(-over_mlp // (J - 1))
    mlp_point(0, after_heads, opening)
    start(fetch_mlp(1))
    per = tiles // mbs
    for m in range(mbs):
        L.gated(m, r.wbuf.at[0, 0], r.wbuf.at[0, 1], r.a.at[0])
        for t in range(m * per, (m + 1) * per):
            L.add_out(r.o.at[(H - 1) % 2], r.obuf.at[(H - 1) % 3], t)

    @pl.loop(1, J)
    def _(j):
        @pl.when(j + 1 < J)
        def _():
            mlp_point(j, after_heads + over_mlp // (J - 1), last)
            start(fetch_mlp(j + 1))

        with jax.named_scope("wait_mlp"):
            wait(fetch_mlp(j))
        s = lax.rem(j, 2)
        prev = r.obuf.at[lax.rem(j - 1 + H, 3)]
        with jax.named_scope("mlp"):
            for m in range(mbs):
                L.gated(m, r.wbuf.at[s, 0], r.wbuf.at[s, 1], r.a.at[s])
                for t in range(m * per, (m + 1) * per):
                    L.add_out(r.a.at[1 - s], prev, t)

    with jax.named_scope("finish"):
        L.finish(r.a.at[(J - 1) % 2], r.obuf.at[(J - 1 + H) % 3])
    pltpu.make_async_copy(r.k, r.kc.at[0], r.csem.at[0]).wait()
    pltpu.make_async_copy(r.v, r.vc.at[0], r.csem.at[1]).wait()
    comm.drain()


def layer(d, x, prompt_len, ln, w_in, wot):
    T, E, HD = d["T"], d["E"], d["HD"]
    half = HD // 2
    inv_freq = np.float64(ROPE_BASE) ** (-2.0 * np.arange(half) / HD)
    steps = np.concatenate([np.arange(Layer.QB), np.arange(T // Layer.QB) * Layer.QB])
    angles = steps[:, None] * inv_freq[None, :]
    rc = jnp.asarray(np.cos(angles), jnp.float32)
    rs = jnp.asarray(np.sin(angles), jnp.float32)
    ln_tile = jnp.broadcast_to(jnp.tile(ln, 128 // d["R"])[None], (8, 128))
    w_shape = (d["SIDE"], d["SIDE"], d["CORES"], d["R"], d["COLS"])
    hbm, vmem = pl.BlockSpec(memory_space=HBM), pl.BlockSpec(memory_space=pltpu.VMEM)
    flops = 2 * T * E * d["COLS"] + 2 * T * T * HD * d["H"]
    cache = jax.ShapeDtypeStruct((1, T, HD), jnp.bfloat16)
    y, kc, vc, _ = pl.pallas_call(
        functools.partial(kernel, d),
        out_shape=(jax.ShapeDtypeStruct(x.shape, jnp.bfloat16), cache, cache,
                   jax.ShapeDtypeStruct(w_shape, jnp.bfloat16)),
        in_specs=[vmem, hbm, hbm, hbm, pl.BlockSpec(memory_space=pltpu.SMEM), vmem, vmem],
        out_specs=(hbm, hbm, hbm, hbm),
        scratch_shapes=scratch(d),
        compiler_params=pltpu.CompilerParams(collective_id=0, has_side_effects=True, vmem_limit_bytes=VMEM_LIMIT),
        cost_estimate=pl.CostEstimate(flops=flops, bytes_accessed=4 * T * E + 2 * E * d["COLS"], transcendentals=0),
        name="layer",
    )(ln_tile, w_in, wot, x, prompt_len, rc, rs)
    return hand_on(y, kc, vc)


def hand_on_kernel(parts, *refs):
    n = len(parts)
    src, dst, buf, sem_in, sem_out = refs[:n], refs[n:2 * n], refs[2 * n:3 * n], refs[3 * n], refs[3 * n + 1]
    moves = []
    for i, blocks in enumerate(parts):
        rows = src[i].shape[1] // blocks
        for k in range(blocks):
            at = pl.ds(k * rows, rows)
            moves.append((src[i].at[0, at, :], buf[i].at[at, :], dst[i].at[0, at, :]))
    for k, (a, b, _) in enumerate(moves):
        pltpu.make_async_copy(a, b, sem_in.at[k]).start()
    for k, (a, b, c) in enumerate(moves):
        pltpu.make_async_copy(a, b, sem_in.at[k]).wait()
        pltpu.make_async_copy(b, c, sem_out.at[k]).start()
    for k, (_, b, c) in enumerate(moves):
        pltpu.make_async_copy(b, c, sem_out.at[k]).wait()


def hand_on(y, kc, vc):
    arrays, parts = (y, kc, vc), (8, 1, 1)
    hbm = pl.BlockSpec(memory_space=HBM)
    return pl.pallas_call(
        functools.partial(hand_on_kernel, parts),
        out_shape=tuple(jax.ShapeDtypeStruct(a.shape, a.dtype) for a in arrays),
        in_specs=[hbm] * 3,
        out_specs=(hbm,) * 3,
        scratch_shapes=[pltpu.VMEM(a.shape[1:], a.dtype) for a in arrays]
        + [pltpu.SemaphoreType.DMA((sum(parts),)), pltpu.SemaphoreType.DMA((sum(parts),))],
        compiler_params=pltpu.CompilerParams(vmem_limit_bytes=VMEM_LIMIT),
        name="hand_on",
    )(*arrays)


def solution(mesh):
    batch_spec = P(("pod", "d"))

    def local_layer(x, prompt_len, ln_shard, w_in_shard, w_out_shard):
        d = dims(mesh, x, w_in_shard, w_out_shard)
        return layer(d, x, prompt_len, ln_shard, w_in_shard, w_out_shard.T)

    return jax.shard_map(local_layer, mesh=mesh,
                         in_specs=(batch_spec, batch_spec, P("d"), P("d", None), P(None, "d")),
                         out_specs=(batch_spec, batch_spec, batch_spec), check_vma=False)
```

```python
import functools
import math

import jax
import jax.numpy as jnp
import numpy as np
from jax import lax
from jax.experimental import pallas as pl
from jax.experimental.pallas import tpu as pltpu
from jax.sharding import PartitionSpec as P

EPS = 1e-6
ROPE_BASE = 10000.0
MASKED = -1e30
MESH = pl.DeviceIdType.MESH
HBM = pltpu.HBM
VMEM_LIMIT = 67043328

SMALL, SMALL_WIDTH, WIDTH = 20, 384, 768
LAG = (0, 2, 4, 6, 8, 9)
FIRST = 12
KEYS, QUERY, NORM = 6, 7, 8
OPENING = (0, 0, 0, 0, 0, 0, 0, 1, 1, 0, 1, 1, 0, 1, NORM + 2, 1, NORM + 1, 1, NORM + 1, 2, 2, NORM + 11, 1, NORM + 1, 1, 0,
           3, 2, 3, 2, 4, 1, 0, 3, 2, 4, 5, 3, 2, 5, KEYS, 4, KEYS, 1, 4, KEYS, 3, 2, KEYS, 5, 3, 2,
           QUERY, QUERY, 5, QUERY, QUERY, 0)


def dims(mesh, x, w_in, w_out):
    devices = mesh.shape["d"]
    cores = 2
    side = math.isqrt(devices // cores)
    model = x.shape[2]
    ffn = 4 * model
    attn = w_out.shape[0] - ffn
    head = (w_in.shape[1] - 2 * ffn - attn) // 2
    return dict(D=devices, CORES=cores, SIDE=side, T=x.shape[1], E=model, F=ffn, H=attn // head, HD=head,
                R=model // devices, COLS=w_in.shape[1] + w_out.shape[0], FC=head)


def place():
    return lax.axis_index("d")


def order_copies(d, win_ref, wot_ref, stage_ref, sem, part):
    F, H, HD, FC = d["F"], d["H"], d["HD"], d["FC"]
    qs = 2 * F
    ks = qs + H * HD
    base = 2 * HD + H * 2 * HD

    def move(src_ref, col, at, width, which):
        pltpu.make_async_copy(src_ref.at[:, pl.ds(pl.multiple_of(col, HD), width)],
                              stage_ref.at[:, pl.ds(pl.multiple_of(at, HD), width)], sem.at[which]).start()

    if part == 0:
        move(win_ref, ks, 0, 2 * HD, 0)

        @pl.loop(0, H)
        def _(h):
            move(win_ref, qs + h * HD, 2 * HD + h * 2 * HD, HD, 0)
            move(wot_ref, F + h * HD, 3 * HD + h * 2 * HD, HD, 0)

        return

    @pl.loop(0, F // FC)
    def _(j):
        at = base + j * 3 * FC
        move(win_ref, j * FC, at, FC, 1)
        move(win_ref, F + j * FC, at + FC, FC, 1)
        move(wot_ref, j * FC, at + 2 * FC, FC, 1)


class Comm:
    def __init__(self, d, stage_ref, w_ref, send_sem, recv_sem):
        self.d = d
        self.stage, self.w, self.send, self.recv = stage_ref, w_ref, send_sem, recv_sem
        self.groups = SMALL + (d["COLS"] - SMALL * SMALL_WIDTH) // WIDTH
        self.done = [OPENING.count(k) for k in range(6)]
        side, cores = d["SIDE"], d["CORES"]
        me = place()
        self.core = lax.rem(me, cores)
        self.x = lax.rem(lax.div(me, cores), side)
        self.y = lax.div(me, cores * side)

    @staticmethod
    def end(groups):
        return min(groups, SMALL) * SMALL_WIDTH + max(groups - SMALL, 0) * WIDTH

    def dev(self, y, x, core):
        d = self.d
        return {"d": (y * d["SIDE"] + x) * d["CORES"] + core}

    def wrap(self, v):
        side = self.d["SIDE"]
        return lax.rem(v + side, side)

    def put(self, src, dst, stage, g, device):
        return pltpu.make_async_remote_copy(src_ref=src, dst_ref=dst, send_sem=self.send.at[stage],
                                            recv_sem=self.recv.at[stage, g], device_id=device, device_id_type=MESH)

    def landed(self, ref, stage, g):
        pltpu.make_async_copy(ref, ref, self.recv.at[stage, g]).wait()

    def stage_fn(self, stage, g, small):
        w, x, y, c = self.w, self.x, self.y, self.core
        half = self.d["R"] // 2
        if small:
            cols = pl.ds(pl.multiple_of(g * SMALL_WIDTH, 128), SMALL_WIDTH)
        else:
            cols = pl.ds(pl.multiple_of(SMALL * SMALL_WIDTH + (g - SMALL) * WIDTH, 128), WIDTH)
        ra, rb = pl.ds(0, half), pl.ds(half, half)
        turn = 1 - 2 * lax.rem(g, 2)
        if stage == 0:
            for s in (1, -1):
                self.put(self.stage.at[ra, cols], w.at[y, x, c, ra, cols], 0, g,
                         self.dev(y, self.wrap(x + s), c)).start()
                self.put(self.stage.at[rb, cols], w.at[y, x, c, rb, cols], 0, g,
                         self.dev(self.wrap(y + s), x, c)).start()
        elif stage == 1:
            self.landed(w.at[0, 0:2, :, ra, cols], 0, g)
            xs, ys = self.wrap(x - turn), self.wrap(y + turn)
            a = w.at[y, xs, c, ra, cols]
            self.put(a, a, 1, g, self.dev(y, self.wrap(x + turn), c)).start()
            b = w.at[ys, x, c, rb, cols]
            self.put(b, b, 1, g, self.dev(self.wrap(y - turn), x, c)).start()
        elif stage == 2:
            self.landed(w.at[0, 0, :, ra, cols], 1, g)
            a = w.at[y, :, c, ra, cols]
            b = w.at[:, x, c, rb, cols]
            for s in (1, -1):
                self.put(a, a, 2, g, self.dev(self.wrap(y + s), x, c)).start()
                self.put(b, b, 2, g, self.dev(y, self.wrap(x + s), c)).start()
        elif stage == 3:
            self.landed(w.at[0:2, :, :, ra, cols], 2, g)
            ys, xs = self.wrap(y - turn), self.wrap(x + turn)
            a = w.at[ys, :, c, ra, cols]
            self.put(a, a, 3, g, self.dev(self.wrap(y + turn), x, c)).start()
            b = w.at[:, xs, c, rb, cols]
            self.put(b, b, 3, g, self.dev(y, self.wrap(x - turn), c)).start()
        elif stage == 4:
            self.landed(w.at[0, :, :, ra, cols], 3, g)
            a = w.at[:, :, c, :, cols]
            self.put(a, a, 4, g, self.dev(y, x, 1 - c)).start()
        else:
            self.landed(w.at[:, :, 0, :, cols], 4, g)

    def point(self, p, lo, hi):
        for stage in (4, 3, 2, 1, 0, 5):
            g = p - LAG[stage]
            for small, start, stop in ((True, 0, SMALL), (False, SMALL, self.groups)):
                start = max(start, self.done[stage])
                if hi - 1 - LAG[stage] < start or lo - LAG[stage] >= stop:
                    continue

                @pl.when(jnp.logical_and(g >= start, g < stop))
                def _(stage=stage, g=g, small=small):
                    self.stage_fn(stage, g, small)

    def drain(self):
        side, w = self.d["SIDE"], self.w
        for stage, ref in ((0, w.at[0, 0]), (1, w.at[0, 0, 0]), (2, w.at[0]), (3, w.at[0, 0:side // 2]),
                           (4, w.at[0:side // 2])):
            pltpu.make_async_copy(ref, ref, self.send.at[stage]).wait()


def arrive(d):
    barrier = pltpu.get_barrier_semaphore()
    me = place()

    @pl.loop(1, d["D"])
    def _(i):
        pl.semaphore_signal(barrier, inc=1, device_id={"d": lax.rem(me + i, d["D"])}, device_id_type=MESH)


def meet(d):
    pl.semaphore_wait(pltpu.get_barrier_semaphore(), d["D"] - 1)


def spread_scale(d, ln_ref, ln_all, ln_send, ln_recv):
    me = place()

    @pl.loop(1, d["D"])
    def _(i):
        pltpu.make_async_remote_copy(src_ref=ln_ref, dst_ref=ln_all.at[me], send_sem=ln_send, recv_sem=ln_recv,
                                     device_id={"d": lax.rem(me + i, d["D"])}, device_id_type=MESH).start()

    ln_all[me] = ln_ref[...]


def spread_scale_wait(d, ln_all, ln_send, ln_recv):
    rest = ln_all.at[pl.ds(0, d["D"] - 1)]
    pltpu.make_async_copy(rest, rest, ln_recv).wait()
    pltpu.make_async_copy(rest, rest, ln_send).wait()


def scale_row(d, ln_all, row_ref):
    per = 128 // d["R"]
    for i in range(d["E"] // 128):
        row_ref[0:1, i * 128:(i + 1) * 128] = jnp.concatenate([ln_all[per * i + k] for k in range(per)], axis=1)


def nn(a, b):
    return lax.dot_general(a, b, (((1,), (0,)), ((), ())), preferred_element_type=jnp.float32)


def nt(a, b):
    return lax.dot_general(a, b, (((1,), (1,)), ((), ())), preferred_element_type=jnp.float32)


def rope(u, cos, sin):
    half = u.shape[1] // 2
    u1, u2 = u[:, :half], u[:, half:]
    return jnp.concatenate([u1 * cos - u2 * sin, u2 * cos + u1 * sin], axis=1)


class Layer:
    XB = 128
    MB = 512
    QB = 256

    def __init__(self, d, r):
        self.d, self.r = d, r

    def x_copy(self, i):
        rows = pl.ds(pl.multiple_of(i * self.XB, self.XB), self.XB)
        return pltpu.make_async_copy(self.r.x.at[0, rows, :], self.r.h.at[rows, :], self.r.xsem.at[i])

    def y_copy(self, t):
        cols = pl.ds(t * self.d["FC"], self.d["FC"])
        return pltpu.make_async_copy(self.r.h.at[:, cols], self.r.y.at[0, :, cols], self.r.xsem.at[t])

    def unit(self, col, buf, sem):
        return pltpu.make_async_copy(self.r.w.at[:, :, :, :, pl.ds(pl.multiple_of(col, 128), self.d["FC"])], buf, sem)

    def wval(self, buf):
        return buf[...].reshape(self.d["E"], self.d["FC"])

    def norm(self, i):
        r = self.r
        self.x_copy(i).wait()
        rows = pl.ds(pl.multiple_of(i * self.XB, self.XB), self.XB)
        xf = r.h[rows, :].astype(jnp.float32)
        centered = xf - jnp.mean(xf, axis=-1, keepdims=True)
        var = jnp.mean(centered * centered, axis=-1, keepdims=True)
        r.h[rows, :] = (centered * lax.rsqrt(var + EPS) * r.ln[...]).astype(jnp.bfloat16)
        r.yacc[rows, :] = xf

    def tables(self):
        d, r = self.d, self.r
        lo = r.rc.shape[0] - d["T"] // self.QB
        cl, sl = r.rc[0:self.QB, :], r.rs[0:self.QB, :]
        for b in range(d["T"] // self.QB):
            cb, sb = r.rc[self.QB + b:self.QB + b + 1, :], r.rs[self.QB + b:self.QB + b + 1, :]
            rows = slice(b * self.QB, (b + 1) * self.QB)
            r.cos[rows, :] = cl * cb - sl * sb
            r.sin[rows, :] = sl * cb + cl * sb

    def bias(self):
        r, d = self.r, self.d
        col = lax.broadcasted_iota(jnp.int32, (8, d["T"]), 1)
        r.bias[...] = jnp.where(col < r.plen[0], 0.0, MASKED)

    def keys(self, m, kbuf, vbuf):
        r = self.r
        rows = slice(m * self.MB, (m + 1) * self.MB)
        hb = r.h[rows, :]
        kf = rope(nn(hb, self.wval(kbuf)), r.cos[rows, :], r.sin[rows, :])
        r.k[rows, :] = kf.astype(jnp.bfloat16)
        r.kt[:, rows] = kf.T.astype(jnp.bfloat16)
        r.v[rows, :] = nn(hb, self.wval(vbuf)).astype(jnp.bfloat16)

    def query(self, m, qbuf, q_ref):
        r = self.r
        rows = slice(m * self.MB, (m + 1) * self.MB)
        q_ref[rows, :] = rope(nn(r.h[rows, :], self.wval(qbuf)), r.cos[rows, :], r.sin[rows, :]).astype(jnp.bfloat16)

    def scores(self, b, q_ref, z_ref):
        d, r = self.d, self.r
        qb, half = self.QB, self.QB // 2
        unit = math.log2(math.e) / math.sqrt(d["HD"])
        q = q_ref[b * qb:(b + 1) * qb, :]
        top = [None, None]
        for c in range(b + 1):
            cols = slice(c * qb, (c + 1) * qb)
            s = nn(q, r.kt[:, cols])
            for i in range(2):
                part = slice(i * half, (i + 1) * half)
                z = s[part, :] * unit + r.bias[0:1, cols]
                if c == b:
                    row = lax.broadcasted_iota(jnp.int32, (half, qb), 0) + i * half
                    col = lax.broadcasted_iota(jnp.int32, (half, qb), 1)
                    z = jnp.where(col <= row, z, MASKED)
                z_ref[part, cols] = z
                for k in range(qb // 128):
                    zk = z[:, k * 128:(k + 1) * 128]
                    top[i] = zk if top[i] is None else jnp.maximum(top[i], zk)
        return [jnp.max(t, axis=-1, keepdims=True) for t in top]

    def softmax(self, b, z_ref, p_ref, top):
        qb, half = self.QB, self.QB // 2
        for i in range(2):
            part = slice(i * half, (i + 1) * half)
            total = None
            for c in range(b + 1):
                cols = slice(c * qb, (c + 1) * qb)
                e = jnp.exp2(z_ref[part, cols] - top[i])
                z_ref[part, cols] = e
                for k in range(qb // 128):
                    ek = e[:, k * 128:(k + 1) * 128]
                    total = ek if total is None else total + ek
            inv = 1.0 / jnp.sum(total, axis=-1, keepdims=True)
            for c in range(b + 1):
                cols = slice(c * qb, (c + 1) * qb)
                p_ref[part, cols] = (z_ref[part, cols] * inv).astype(jnp.bfloat16)

    def values(self, b, p_ref, o_ref):
        r, qb = self.r, self.QB
        n = (b + 1) * qb
        o_ref[b * qb:n, :] = nn(p_ref[:, 0:n], r.v[0:n, :]).astype(jnp.bfloat16)

    def head(self, q_ref, o_ref, q_next, qbuf_next, o_prev, obuf_prev, midway):
        d, r = self.d, self.r
        nb = d["T"] // self.QB
        mbs, tiles = d["T"] // self.MB, d["E"] // d["FC"]
        work = [functools.partial(self.add_out, o_prev, obuf_prev, t) for t in range(tiles)]
        per = tiles // mbs
        steps = []
        for m in range(mbs):
            steps += [work[m * per:(m + 1) * per], [functools.partial(self.query, m, qbuf_next, q_next)]]
        last = None
        for n, b in enumerate(reversed(range(nb))):
            if n == nb // 2:
                midway()
            z_ref, p_ref = r.z.at[n % 2], r.p.at[n % 2]
            top = self.scores(b, q_ref, z_ref)
            for f in steps[n]:
                f()
            self.softmax(b, z_ref, p_ref, top)
            if last is not None:
                self.values(*last)
            last = (b, p_ref, o_ref)
        self.values(*last)

    def add_out(self, a_ref, obuf, tile):
        r, d = self.r, self.d
        fc = d["FC"]
        per = fc // d["R"]
        cols = slice(tile * fc, (tile + 1) * fc)
        w = self.wval(obuf)[cols, :]
        r.yacc[:, cols] += nt(a_ref[...], w)

    def gated(self, m, gbuf, ubuf, a_ref):
        r = self.r
        rows = slice(m * self.MB, (m + 1) * self.MB)
        hb = r.h[rows, :]
        g = nn(hb, self.wval(gbuf))
        u = nn(hb, self.wval(ubuf))
        hg = g * 0.5
        a_ref[rows, :] = ((hg + hg * jnp.tanh(hg)) * u).astype(jnp.bfloat16)

    def finish(self, a_ref, obuf):
        d, r = self.d, self.r
        fc = d["FC"]
        for t in range(d["E"] // fc):
            cols = slice(t * fc, (t + 1) * fc)
            total = r.yacc[:, cols] + nt(a_ref[...], self.wval(obuf)[cols, :])
            r.h[:, cols] = total.astype(jnp.bfloat16)
            self.y_copy(t).start()
        for t in range(d["E"] // fc):
            self.y_copy(t).wait()


class Refs:
    pass


NAMES = ("ln_own", "win", "wot", "x", "plen", "rc", "rs",
         "y", "kc", "vc", "w",
         "stage", "ln_all", "ln", "h", "yacc", "cos", "sin", "bias", "k", "kt", "v", "q", "z", "p", "a", "wbuf", "obuf",
         "local_sem", "ln_send", "ln_recv", "send_sem", "recv_sem", "xsem", "wsem", "osem", "csem")


def scratch(d):
    T, E, HD, FC = d["T"], d["E"], d["HD"], d["FC"]
    unit = (d["SIDE"], d["SIDE"], d["CORES"], d["R"], FC)
    bf16, f32, dma = jnp.bfloat16, jnp.float32, pltpu.SemaphoreType.DMA
    return [
        pltpu.VMEM((d["R"], d["COLS"]), bf16),
        pltpu.VMEM((d["D"], 1, d["R"]), f32),
        pltpu.VMEM((1, E), f32),
        pltpu.VMEM((T, E), bf16),
        pltpu.VMEM((T, E), f32),
        pltpu.VMEM((T, HD // 2), f32),
        pltpu.VMEM((T, HD // 2), f32),
        pltpu.VMEM((8, T), f32),
        pltpu.VMEM((T, HD), bf16),
        pltpu.VMEM((HD, T), bf16),
        pltpu.VMEM((T, HD), bf16),
        pltpu.VMEM((2, T, HD), bf16),
        pltpu.VMEM((2, Layer.QB, T), f32),
        pltpu.VMEM((2, Layer.QB, T), bf16),
        pltpu.VMEM((2, T, FC), bf16),
        pltpu.VMEM((2, 2) + unit, bf16),
        pltpu.VMEM((3,) + unit, bf16),
        dma((4,)), dma, dma, dma((5,)), dma((5, SMALL + (d["COLS"] - SMALL * SMALL_WIDTH) // WIDTH)),
        dma((max(T // Layer.XB, E // FC),)), dma((2, 2)), dma((3,)), dma((2,)),
    ]


def kernel(d, *refs):
    r = Refs()
    for name, ref in zip(NAMES, refs, strict=True):
        setattr(r, name, ref)
    L = Layer(d, r)
    HD, FC, H = d["HD"], d["FC"], d["H"]
    J = d["F"] // FC
    tiles = d["E"] // FC
    mbs = d["T"] // L.MB
    xbs = d["T"] // L.XB
    base = 2 * HD + H * 2 * HD

    def fetch_kv():
        return [L.unit(0, r.wbuf.at[0, 0], r.wsem.at[0, 0]), L.unit(HD, r.wbuf.at[0, 1], r.wsem.at[0, 1])]

    def fetch_q(h):
        s = lax.rem(h, 2)
        return [L.unit(2 * HD + h * 2 * HD, r.wbuf.at[1, s], r.wsem.at[1, s])]

    def fetch_o(h):
        s = lax.rem(h, 3)
        return [L.unit(2 * HD + h * 2 * HD + HD, r.obuf.at[s], r.osem.at[s])]

    def fetch_mlp(j):
        col = base + j * 3 * FC
        s = lax.rem(j, 2)
        o = lax.rem(j + H, 3)
        return [L.unit(col, r.wbuf.at[s, 0], r.wsem.at[s, 0]), L.unit(col + FC, r.wbuf.at[s, 1], r.wsem.at[s, 1]),
                L.unit(col + 2 * FC, r.obuf.at[o], r.osem.at[o])]

    def start(copies):
        for c in copies:
            c.start()

    def wait(copies):
        for c in copies:
            c.wait()

    comm = Comm(d, r.stage, r.w, r.send_sem, r.recv_sem)
    after_heads = FIRST + 2 * H
    last = comm.groups + LAG[5]
    over_mlp = last - after_heads

    def ready(points):
        return comm.end(max(points - LAG[5], comm.done[5]))

    for k in range(6):
        assert comm.done[k] >= min(FIRST - LAG[k], comm.groups)
    assert ready(FIRST) >= 2 * HD + 3 * HD
    for h in range(1, H):
        assert ready(FIRST + 2 * h + 1) >= min(2 * HD + (h + 2) * 2 * HD + HD, base)
    assert ready(FIRST + 2 * H - 1) >= base + 3 * FC
    for j in range(J - 1):
        assert ready(after_heads + (j + 1) * over_mlp // (J - 1)) >= base + (j + 2) * 3 * FC

    mine = r.w.at[comm.y, comm.x, comm.core]
    early, late = pl.ds(0, base), pl.ds(base, d["COLS"] - base)
    own = [pltpu.make_async_copy(r.stage.at[:, part], mine.at[:, part], r.local_sem.at[2 + i])
           for i, part in enumerate((early, late))]
    rest = r.stage.at[:, late]
    order_copies(d, r.win, r.wot, r.stage, r.local_sem, 0)
    arrive(d)
    for i in range(xbs):
        L.x_copy(i).start()
    pltpu.make_async_copy(r.stage.at[:, early], r.stage.at[:, early], r.local_sem.at[0]).wait()
    own[0].start()
    meet(d)
    reached = set()

    def late_begun():
        if "begun" not in reached:
            reached.add("begun")
            order_copies(d, r.win, r.wot, r.stage, r.local_sem, 1)

    def late_ready():
        late_begun()
        if "late" not in reached:
            reached.add("late")
            pltpu.make_async_copy(rest, rest, r.local_sem.at[1]).wait()
            own[1].start()

    def late_placed():
        late_ready()
        if "placed" not in reached:
            reached.add("placed")
            own[1].wait()

    normed = keyed = queried = 0
    next_group = [0] * 6
    for what in OPENING:
        if what <= 5:
            g = next_group[what]
            next_group[what] += 1
            if (what, g) == (2, 0):
                own[0].wait()
            if what == 0 and comm.end(g + 1) > base:
                late_ready()
            if what == 2 and comm.end(g + 1) > base:
                late_placed()
            with jax.named_scope(f"stage{what}"):
                comm.stage_fn(what, g, g < SMALL)
            if (what, g) == (0, 1):
                spread_scale(d, r.ln_own, r.ln_all, r.ln_send, r.ln_recv)
            if what == 1:
                late_begun()
            if what == 5 and comm.end(g) < 3 * HD <= comm.end(g + 1):
                start(fetch_kv())
                start(fetch_q(0))
            if what == 5 and comm.end(g) < 5 * HD <= comm.end(g + 1):
                start(fetch_q(1))
                start(fetch_o(0))
        elif what == KEYS:
            if keyed == 0:
                assert normed == xbs
                with jax.named_scope("wait_kv"):
                    wait(fetch_kv())
            if keyed < mbs:
                with jax.named_scope("keys"):
                    L.keys(keyed, r.wbuf.at[0, 0], r.wbuf.at[0, 1])
            keyed += 1
            if keyed == mbs:
                pltpu.make_async_copy(r.k, r.kc.at[0], r.csem.at[0]).start()
                pltpu.make_async_copy(r.v, r.vc.at[0], r.csem.at[1]).start()
        elif what == QUERY:
            if queried == 0:
                wait(fetch_q(0))
            if queried < mbs:
                with jax.named_scope("query"):
                    L.query(queried, r.wbuf.at[1, 0], r.q.at[0])
            queried += 1
        else:
            if normed == 0:
                late_ready()
                with jax.named_scope("tables"):
                    L.tables()
                    L.bias()
                with jax.named_scope("wait_scale"):
                    spread_scale_wait(d, r.ln_all, r.ln_send, r.ln_recv)
                    scale_row(d, r.ln_all, r.ln)
            many = min(what - NORM, xbs - normed)
            if many > 0:
                with jax.named_scope("norm"):
                    @pl.loop(normed, normed + many)
                    def _(i):
                        L.norm(i)
            normed += many
    late_ready()
    late_placed()
    r.a[1] = jnp.zeros((d["T"], FC), jnp.bfloat16)
    r.obuf[2] = jnp.zeros(r.obuf.shape[1:], jnp.bfloat16)

    @pl.loop(0, H)
    def _(h):
        with jax.named_scope("point_head"):
            comm.point(FIRST + 2 * h, FIRST, after_heads)

        @pl.when(h == 1)
        def _():
            start(fetch_o(h))
            start(fetch_q(h + 1))

        @pl.when(jnp.logical_and(h > 0, h + 1 < H))
        def _():
            start(fetch_o(h + 1))

        @pl.when(jnp.logical_and(h > 0, h + 2 < H))
        def _():
            start(fetch_q(h + 2))

        @pl.when(h + 1 < H)
        def _():
            wait(fetch_q(h + 1))

        @pl.when(h > 0)
        def _():
            wait(fetch_o(h - 1))

        @pl.when(h + 1 == H)
        def _():
            start(fetch_mlp(0))

        s = lax.rem(h, 2)

        def midway():
            with jax.named_scope("point_mid"):
                comm.point(FIRST + 2 * h + 1, FIRST, after_heads)

        with jax.named_scope("head"):
            L.head(r.q.at[s], r.a.at[s], r.q.at[1 - s], r.wbuf.at[1, 1 - s], r.a.at[1 - s], r.obuf.at[lax.rem(h + 2, 3)], midway)

    wait(fetch_o(H - 1))

    @pl.loop(0, J)
    def _(j):
        @pl.when(j + 1 < J)
        def _():
            @pl.loop(after_heads + lax.div(j * over_mlp, J - 1), after_heads + lax.div((j + 1) * over_mlp, J - 1))
            def _(p):
                with jax.named_scope("point_mlp"):
                    comm.point(p, after_heads, last)

            start(fetch_mlp(j + 1))

        with jax.named_scope("wait_mlp"):
            wait(fetch_mlp(j))
        s = lax.rem(j, 2)
        prev = r.obuf.at[lax.rem(j - 1 + H, 3)]
        per = tiles // mbs
        with jax.named_scope("mlp"):
            for m in range(mbs):
                L.gated(m, r.wbuf.at[s, 0], r.wbuf.at[s, 1], r.a.at[s])
                for t in range(m * per, (m + 1) * per):
                    L.add_out(r.a.at[1 - s], prev, t)

    with jax.named_scope("finish"):
        L.finish(r.a.at[(J - 1) % 2], r.obuf.at[(J - 1 + H) % 3])
    pltpu.make_async_copy(r.k, r.kc.at[0], r.csem.at[0]).wait()
    pltpu.make_async_copy(r.v, r.vc.at[0], r.csem.at[1]).wait()
    comm.drain()


def layer(d, x, prompt_len, ln, w_in, wot):
    T, E, HD = d["T"], d["E"], d["HD"]
    half = HD // 2
    inv_freq = np.float64(ROPE_BASE) ** (-2.0 * np.arange(half) / HD)
    steps = np.concatenate([np.arange(Layer.QB), np.arange(T // Layer.QB) * Layer.QB])
    angles = steps[:, None] * inv_freq[None, :]
    rc = jnp.asarray(np.cos(angles), jnp.float32)
    rs = jnp.asarray(np.sin(angles), jnp.float32)
    w_shape = (d["SIDE"], d["SIDE"], d["CORES"], d["R"], d["COLS"])
    hbm, vmem = pl.BlockSpec(memory_space=HBM), pl.BlockSpec(memory_space=pltpu.VMEM)
    flops = 2 * T * E * d["COLS"] + 2 * T * T * HD * d["H"]
    cache = jax.ShapeDtypeStruct((1, T, HD), jnp.bfloat16)
    y, kc, vc, _ = pl.pallas_call(
        functools.partial(kernel, d),
        out_shape=(jax.ShapeDtypeStruct(x.shape, jnp.bfloat16), cache, cache,
                   jax.ShapeDtypeStruct(w_shape, jnp.bfloat16)),
        in_specs=[vmem, hbm, hbm, hbm, pl.BlockSpec(memory_space=pltpu.SMEM), vmem, vmem],
        out_specs=(hbm, hbm, hbm, hbm),
        scratch_shapes=scratch(d),
        compiler_params=pltpu.CompilerParams(collective_id=0, has_side_effects=True, vmem_limit_bytes=VMEM_LIMIT),
        cost_estimate=pl.CostEstimate(flops=flops, bytes_accessed=4 * T * E + 2 * E * d["COLS"], transcendentals=0),
        name="layer",
    )(ln[None], w_in, wot, x, prompt_len, rc, rs)
    return hand_on(y, kc, vc)


def hand_on_kernel(parts, *refs):
    n = len(parts)
    src, dst, buf, sem_in, sem_out = refs[:n], refs[n:2 * n], refs[2 * n:3 * n], refs[3 * n], refs[3 * n + 1]
    moves = []
    for i, blocks in enumerate(parts):
        rows = src[i].shape[1] // blocks
        for k in range(blocks):
            at = pl.ds(k * rows, rows)
            moves.append((src[i].at[0, at, :], buf[i].at[at, :], dst[i].at[0, at, :]))
    for k, (a, b, _) in enumerate(moves):
        pltpu.make_async_copy(a, b, sem_in.at[k]).start()
    for k, (a, b, c) in enumerate(moves):
        pltpu.make_async_copy(a, b, sem_in.at[k]).wait()
        pltpu.make_async_copy(b, c, sem_out.at[k]).start()
    for k, (_, b, c) in enumerate(moves):
        pltpu.make_async_copy(b, c, sem_out.at[k]).wait()


def hand_on(y, kc, vc):
    arrays, parts = (y, kc, vc), (8, 1, 1)
    hbm = pl.BlockSpec(memory_space=HBM)
    return pl.pallas_call(
        functools.partial(hand_on_kernel, parts),
        out_shape=tuple(jax.ShapeDtypeStruct(a.shape, a.dtype) for a in arrays),
        in_specs=[hbm] * 3,
        out_specs=(hbm,) * 3,
        scratch_shapes=[pltpu.VMEM(a.shape[1:], a.dtype) for a in arrays]
        + [pltpu.SemaphoreType.DMA((sum(parts),)), pltpu.SemaphoreType.DMA((sum(parts),))],
        compiler_params=pltpu.CompilerParams(vmem_limit_bytes=VMEM_LIMIT),
        name="hand_on",
    )(*arrays)


def solution(mesh):
    batch_spec = P(("pod", "d"))

    def local_layer(x, prompt_len, ln_shard, w_in_shard, w_out_shard):
        d = dims(mesh, x, w_in_shard, w_out_shard)
        return layer(d, x, prompt_len, ln_shard, w_in_shard, w_out_shard.T)

    return jax.shard_map(local_layer, mesh=mesh,
                         in_specs=(batch_spec, batch_spec, P("d"), P("d", None), P(None, "d")),
                         out_specs=(batch_spec, batch_spec, batch_spec), check_vma=False)
```

```python
import functools
import math

import jax
import jax.numpy as jnp
import numpy as np
from jax import lax
from jax.experimental import pallas as pl
from jax.experimental.pallas import tpu as pltpu
from jax.sharding import PartitionSpec as P

EPS = 1e-6
ROPE_BASE = 10000.0
MASKED = -1e30
MESH = pl.DeviceIdType.MESH
HBM = pltpu.HBM
VMEM_LIMIT = 67043328

SMALL, SMALL_WIDTH, WIDTH = 10, 384, 768
LAG = (0, 2, 4, 6, 8, 9)
FIRST = 12
EARLY = 3
KEYS, QUERY, NORM = 6, 7, 8
OPENING = (0, 0, 0, 0, 0, 0, 0, 0, 1, 1, 0, 1, 1, 0, 1, NORM + 1, 1, 0, NORM + 3, 1, NORM + 1, 2, 2, NORM + 11, 1, 1, 1, 1,
           3, 2, 3, 2, 4, 0, 3, 2, 4, 5, 3, 2, 5, KEYS, 4, KEYS, 3, 2, KEYS, 4, KEYS, 5, 1, QUERY, 3, 2, QUERY, QUERY, 4,
           QUERY, 5)


def dims(mesh, x, w_in, w_out):
    devices = mesh.shape["d"]
    cores = 2
    side = math.isqrt(devices // cores)
    model = x.shape[2]
    ffn = 4 * model
    attn = w_out.shape[0] - ffn
    head = (w_in.shape[1] - 2 * ffn - attn) // 2
    return dict(D=devices, CORES=cores, SIDE=side, T=x.shape[1], E=model, F=ffn, H=attn // head, HD=head,
                R=model // devices, COLS=w_in.shape[1] + w_out.shape[0], FC=head)


def place():
    return lax.axis_index("d")


def order_copies(d, win_ref, wot_ref, stage_ref, sem, part):
    F, H, HD, FC = d["F"], d["H"], d["HD"], d["FC"]
    qs = 2 * F
    ks = qs + H * HD
    base = 2 * HD + H * 2 * HD

    def move(src_ref, col, at, width, which):
        pltpu.make_async_copy(src_ref.at[:, pl.ds(pl.multiple_of(col, HD), width)],
                              stage_ref.at[:, pl.ds(pl.multiple_of(at, HD), width)], sem.at[which]).start()

    if part == 0:
        move(win_ref, ks, 0, 2 * HD, 0)

        @pl.loop(0, H)
        def _(h):
            move(win_ref, qs + h * HD, 2 * HD + h * 2 * HD, HD, 0)
            move(wot_ref, F + h * HD, 3 * HD + h * 2 * HD, HD, 0)

        return

    @pl.loop(0, F // FC)
    def _(j):
        at = base + j * 3 * FC
        move(win_ref, j * FC, at, FC, 1)
        move(win_ref, F + j * FC, at + FC, FC, 1)
        move(wot_ref, j * FC, at + 2 * FC, FC, 1)


class Comm:
    def __init__(self, d, stage_ref, w_ref, send_sem, recv_sem):
        self.d = d
        self.stage, self.w, self.send, self.recv = stage_ref, w_ref, send_sem, recv_sem
        self.groups = SMALL + (d["COLS"] - SMALL * SMALL_WIDTH) // WIDTH
        self.done = [OPENING.count(k) for k in range(6)]
        side, cores = d["SIDE"], d["CORES"]
        me = place()
        self.core = lax.rem(me, cores)
        self.x = lax.rem(lax.div(me, cores), side)
        self.y = lax.div(me, cores * side)

    @staticmethod
    def end(groups):
        return min(groups, SMALL) * SMALL_WIDTH + max(groups - SMALL, 0) * WIDTH

    def dev(self, y, x, core):
        d = self.d
        return {"d": (y * d["SIDE"] + x) * d["CORES"] + core}

    def wrap(self, v):
        side = self.d["SIDE"]
        return lax.rem(v + side, side)

    def put(self, src, dst, stage, g, device):
        return pltpu.make_async_remote_copy(src_ref=src, dst_ref=dst, send_sem=self.send.at[stage],
                                            recv_sem=self.recv.at[stage, g], device_id=device, device_id_type=MESH)

    def landed(self, ref, stage, g):
        pltpu.make_async_copy(ref, ref, self.recv.at[stage, g]).wait()

    def stage_fn(self, stage, g, small):
        w, x, y, c = self.w, self.x, self.y, self.core
        half = self.d["R"] // 2
        if small:
            cols = pl.ds(pl.multiple_of(g * SMALL_WIDTH, 128), SMALL_WIDTH)
        else:
            cols = pl.ds(pl.multiple_of(SMALL * SMALL_WIDTH + (g - SMALL) * WIDTH, 128), WIDTH)
        ra, rb = pl.ds(0, half), pl.ds(half, half)
        turn = 1 - 2 * lax.rem(g, 2)
        if stage == 0:
            for s in (1, -1):
                self.put(self.stage.at[ra, cols], w.at[y, x, c, ra, cols], 0, g,
                         self.dev(y, self.wrap(x + s), c)).start()
                self.put(self.stage.at[rb, cols], w.at[y, x, c, rb, cols], 0, g,
                         self.dev(self.wrap(y + s), x, c)).start()
        elif stage == 1:
            self.landed(w.at[0, 0:2, :, ra, cols], 0, g)
            xs, ys = self.wrap(x - turn), self.wrap(y + turn)
            a = w.at[y, xs, c, ra, cols]
            self.put(a, a, 1, g, self.dev(y, self.wrap(x + turn), c)).start()
            b = w.at[ys, x, c, rb, cols]
            self.put(b, b, 1, g, self.dev(self.wrap(y - turn), x, c)).start()
        elif stage == 2:
            self.landed(w.at[0, 0, :, ra, cols], 1, g)
            a = w.at[y, :, c, ra, cols]
            b = w.at[:, x, c, rb, cols]
            for s in (1, -1):
                self.put(a, a, 2, g, self.dev(self.wrap(y + s), x, c)).start()
                self.put(b, b, 2, g, self.dev(y, self.wrap(x + s), c)).start()
        elif stage == 3:
            self.landed(w.at[0:2, :, :, ra, cols], 2, g)
            quarter = half // 2
            for i, s in enumerate((1, -1)):
                a = w.at[self.wrap(y - s), :, c, pl.ds(i * quarter, quarter), cols]
                self.put(a, a, 3, g, self.dev(self.wrap(y + s), x, c)).start()
                b = w.at[:, self.wrap(x - s), c, pl.ds(half + i * quarter, quarter), cols]
                self.put(b, b, 3, g, self.dev(y, self.wrap(x + s), c)).start()
        elif stage == 4:
            self.landed(w.at[0, :, :, ra, cols], 3, g)
            a = w.at[:, :, c, :, cols]
            self.put(a, a, 4, g, self.dev(y, x, 1 - c)).start()
        else:
            self.landed(w.at[:, :, 0, :, cols], 4, g)

    def point(self, p, lo, hi):
        for stage in (4, 3, 2, 1, 0, 5):
            g = p - LAG[stage]
            for small, start, stop in ((True, 0, SMALL), (False, SMALL, self.groups)):
                start = max(start, self.done[stage])
                if hi - 1 - LAG[stage] < start or lo - LAG[stage] >= stop:
                    continue

                @pl.when(jnp.logical_and(g >= start, g < stop))
                def _(stage=stage, g=g, small=small):
                    self.stage_fn(stage, g, small)

    def drain(self):
        side, w = self.d["SIDE"], self.w
        for stage, ref in ((0, w.at[0, 0]), (1, w.at[0, 0, 0]), (2, w.at[0]), (3, w.at[0, 0:side // 2]),
                           (4, w.at[0:side // 2])):
            pltpu.make_async_copy(ref, ref, self.send.at[stage]).wait()


def arrive(d):
    barrier = pltpu.get_barrier_semaphore()
    me = place()

    @pl.loop(1, d["D"])
    def _(i):
        pl.semaphore_signal(barrier, inc=1, device_id={"d": lax.rem(me + i, d["D"])}, device_id_type=MESH)


def meet(d):
    pl.semaphore_wait(pltpu.get_barrier_semaphore(), d["D"] - 1)


def spread_scale(d, ln_ref, ln_all, ln_send, ln_recv):
    me = place()

    @pl.loop(1, d["D"])
    def _(i):
        pltpu.make_async_remote_copy(src_ref=ln_ref, dst_ref=ln_all.at[me], send_sem=ln_send, recv_sem=ln_recv,
                                     device_id={"d": lax.rem(me + i, d["D"])}, device_id_type=MESH).start()

    ln_all[me] = ln_ref[...]


def spread_scale_wait(d, ln_all, ln_send, ln_recv):
    rest = ln_all.at[pl.ds(0, d["D"] - 1)]
    pltpu.make_async_copy(rest, rest, ln_recv).wait()
    pltpu.make_async_copy(rest, rest, ln_send).wait()


def scale_row(d, ln_all, row_ref):
    per = 128 // d["R"]
    for i in range(d["E"] // 128):
        row_ref[0:1, i * 128:(i + 1) * 128] = jnp.concatenate([ln_all[per * i + k] for k in range(per)], axis=1)


def nn(a, b):
    return lax.dot_general(a, b, (((1,), (0,)), ((), ())), preferred_element_type=jnp.float32)


def nt(a, b):
    return lax.dot_general(a, b, (((1,), (1,)), ((), ())), preferred_element_type=jnp.float32)


def rope(u, cos, sin):
    half = u.shape[1] // 2
    u1, u2 = u[:, :half], u[:, half:]
    return jnp.concatenate([u1 * cos - u2 * sin, u2 * cos + u1 * sin], axis=1)


class Layer:
    XB = 128
    MB = 512
    QB = 256

    def __init__(self, d, r):
        self.d, self.r = d, r

    def x_copy(self, i):
        rows = pl.ds(pl.multiple_of(i * self.XB, self.XB), self.XB)
        return pltpu.make_async_copy(self.r.x.at[0, rows, :], self.r.h.at[rows, :], self.r.xsem.at[i])

    def y_copy(self, t):
        cols = pl.ds(t * self.d["FC"], self.d["FC"])
        return pltpu.make_async_copy(self.r.h.at[:, cols], self.r.y.at[0, :, cols], self.r.xsem.at[t])

    def unit(self, col, buf, sem):
        return pltpu.make_async_copy(self.r.w.at[:, :, :, :, pl.ds(pl.multiple_of(col, 128), self.d["FC"])], buf, sem)

    def wval(self, buf):
        return buf[...].reshape(self.d["E"], self.d["FC"])

    def norm(self, i):
        r = self.r
        self.x_copy(i).wait()
        rows = pl.ds(pl.multiple_of(i * self.XB, self.XB), self.XB)
        xf = r.h[rows, :].astype(jnp.float32)
        centered = xf - jnp.mean(xf, axis=-1, keepdims=True)
        var = jnp.mean(centered * centered, axis=-1, keepdims=True)
        r.h[rows, :] = (centered * lax.rsqrt(var + EPS) * r.ln[...]).astype(jnp.bfloat16)
        r.yacc[rows, :] = xf

    def tables(self):
        d, r = self.d, self.r
        lo = r.rc.shape[0] - d["T"] // self.QB
        cl, sl = r.rc[0:self.QB, :], r.rs[0:self.QB, :]
        for b in range(d["T"] // self.QB):
            cb, sb = r.rc[self.QB + b:self.QB + b + 1, :], r.rs[self.QB + b:self.QB + b + 1, :]
            rows = slice(b * self.QB, (b + 1) * self.QB)
            r.cos[rows, :] = cl * cb - sl * sb
            r.sin[rows, :] = sl * cb + cl * sb

    def bias(self):
        r, d = self.r, self.d
        col = lax.broadcasted_iota(jnp.int32, (8, d["T"]), 1)
        r.bias[...] = jnp.where(col < r.plen[0], 0.0, MASKED)

    def keys(self, m, kbuf, vbuf):
        r = self.r
        rows = slice(m * self.MB, (m + 1) * self.MB)
        hb = r.h[rows, :]
        kf = rope(nn(hb, self.wval(kbuf)), r.cos[rows, :], r.sin[rows, :])
        r.k[rows, :] = kf.astype(jnp.bfloat16)
        r.kt[:, rows] = kf.T.astype(jnp.bfloat16)
        r.v[rows, :] = nn(hb, self.wval(vbuf)).astype(jnp.bfloat16)

    def query(self, m, qbuf, q_ref):
        r = self.r
        rows = slice(m * self.MB, (m + 1) * self.MB)
        q_ref[rows, :] = rope(nn(r.h[rows, :], self.wval(qbuf)), r.cos[rows, :], r.sin[rows, :]).astype(jnp.bfloat16)

    def scores(self, b, q_ref, z_ref):
        d, r = self.d, self.r
        qb, half = self.QB, self.QB // 2
        unit = math.log2(math.e) / math.sqrt(d["HD"])
        q = q_ref[b * qb:(b + 1) * qb, :]
        top = [None, None]
        for c in range(b + 1):
            cols = slice(c * qb, (c + 1) * qb)
            s = nn(q, r.kt[:, cols])
            for i in range(2):
                part = slice(i * half, (i + 1) * half)
                z = s[part, :] * unit + r.bias[0:1, cols]
                if c == b:
                    row = lax.broadcasted_iota(jnp.int32, (half, qb), 0) + i * half
                    col = lax.broadcasted_iota(jnp.int32, (half, qb), 1)
                    z = jnp.where(col <= row, z, MASKED)
                z_ref[part, cols] = z
                for k in range(qb // 128):
                    zk = z[:, k * 128:(k + 1) * 128]
                    top[i] = zk if top[i] is None else jnp.maximum(top[i], zk)
        return [jnp.max(t, axis=-1, keepdims=True) for t in top]

    def softmax(self, b, z_ref, p_ref, top):
        qb, half = self.QB, self.QB // 2
        for i in range(2):
            part = slice(i * half, (i + 1) * half)
            total = None
            for c in range(b + 1):
                cols = slice(c * qb, (c + 1) * qb)
                e = jnp.exp2(z_ref[part, cols] - top[i])
                z_ref[part, cols] = e
                for k in range(qb // 128):
                    ek = e[:, k * 128:(k + 1) * 128]
                    total = ek if total is None else total + ek
            inv = 1.0 / jnp.sum(total, axis=-1, keepdims=True)
            for c in range(b + 1):
                cols = slice(c * qb, (c + 1) * qb)
                p_ref[part, cols] = (z_ref[part, cols] * inv).astype(jnp.bfloat16)

    def values(self, b, p_ref, o_ref):
        r, qb = self.r, self.QB
        n = (b + 1) * qb
        o_ref[b * qb:n, :] = nn(p_ref[:, 0:n], r.v[0:n, :]).astype(jnp.bfloat16)

    def head(self, q_ref, o_ref, q_next, qbuf_next, o_prev, obuf_prev, midway):
        d, r = self.d, self.r
        nb = d["T"] // self.QB
        mbs, tiles = d["T"] // self.MB, d["E"] // d["FC"]
        work = [functools.partial(self.add_out, o_prev, obuf_prev, t) for t in range(tiles)]
        per = tiles // mbs
        steps = []
        for m in range(mbs):
            steps += [work[m * per:(m + 1) * per], [functools.partial(self.query, m, qbuf_next, q_next)]]
        last = None
        for n, b in enumerate(reversed(range(nb))):
            if n == nb // 2:
                midway()
            z_ref, p_ref = r.z.at[n % 2], r.p.at[n % 2]
            top = self.scores(b, q_ref, z_ref)
            for f in steps[n]:
                f()
            self.softmax(b, z_ref, p_ref, top)
            if last is not None:
                self.values(*last)
            last = (b, p_ref, o_ref)
        self.values(*last)

    def add_out(self, a_ref, obuf, tile):
        r, d = self.r, self.d
        fc = d["FC"]
        per = fc // d["R"]
        cols = slice(tile * fc, (tile + 1) * fc)
        w = self.wval(obuf)[cols, :]
        r.yacc[:, cols] += nt(a_ref[...], w)

    def gated(self, m, gbuf, ubuf, a_ref):
        r = self.r
        rows = slice(m * self.MB, (m + 1) * self.MB)
        hb = r.h[rows, :]
        g = nn(hb, self.wval(gbuf))
        u = nn(hb, self.wval(ubuf))
        hg = g * 0.5
        a_ref[rows, :] = ((hg + hg * jnp.tanh(hg)) * u).astype(jnp.bfloat16)

    def finish(self, a_ref, obuf):
        d, r = self.d, self.r
        fc = d["FC"]
        for t in range(d["E"] // fc):
            cols = slice(t * fc, (t + 1) * fc)
            total = r.yacc[:, cols] + nt(a_ref[...], self.wval(obuf)[cols, :])
            r.h[:, cols] = total.astype(jnp.bfloat16)
            self.y_copy(t).start()
        for t in range(d["E"] // fc):
            self.y_copy(t).wait()


class Refs:
    pass


NAMES = ("ln_own", "win", "wot", "x", "plen", "rc", "rs",
         "y", "kc", "vc", "w",
         "stage", "ln_all", "ln", "h", "yacc", "cos", "sin", "bias", "k", "kt", "v", "q", "z", "p", "a", "wbuf", "obuf",
         "local_sem", "ln_send", "ln_recv", "send_sem", "recv_sem", "xsem", "wsem", "osem", "csem")


def scratch(d):
    T, E, HD, FC = d["T"], d["E"], d["HD"], d["FC"]
    unit = (d["SIDE"], d["SIDE"], d["CORES"], d["R"], FC)
    bf16, f32, dma = jnp.bfloat16, jnp.float32, pltpu.SemaphoreType.DMA
    return [
        pltpu.VMEM((d["R"], d["COLS"]), bf16),
        pltpu.VMEM((d["D"], 1, d["R"]), f32),
        pltpu.VMEM((1, E), f32),
        pltpu.VMEM((T, E), bf16),
        pltpu.VMEM((T, E), f32),
        pltpu.VMEM((T, HD // 2), f32),
        pltpu.VMEM((T, HD // 2), f32),
        pltpu.VMEM((8, T), f32),
        pltpu.VMEM((T, HD), bf16),
        pltpu.VMEM((HD, T), bf16),
        pltpu.VMEM((T, HD), bf16),
        pltpu.VMEM((2, T, HD), bf16),
        pltpu.VMEM((2, Layer.QB, T), f32),
        pltpu.VMEM((2, Layer.QB, T), bf16),
        pltpu.VMEM((2, T, FC), bf16),
        pltpu.VMEM((2, 2) + unit, bf16),
        pltpu.VMEM((3,) + unit, bf16),
        dma((4,)), dma, dma, dma((5,)), dma((5, SMALL + (d["COLS"] - SMALL * SMALL_WIDTH) // WIDTH)),
        dma((max(T // Layer.XB, E // FC),)), dma((2, 2)), dma((3,)), dma((2,)),
    ]


def kernel(d, *refs):
    r = Refs()
    for name, ref in zip(NAMES, refs, strict=True):
        setattr(r, name, ref)
    L = Layer(d, r)
    HD, FC, H = d["HD"], d["FC"], d["H"]
    J = d["F"] // FC
    tiles = d["E"] // FC
    mbs = d["T"] // L.MB
    xbs = d["T"] // L.XB
    base = 2 * HD + H * 2 * HD

    def fetch_kv():
        return [L.unit(0, r.wbuf.at[0, 0], r.wsem.at[0, 0]), L.unit(HD, r.wbuf.at[0, 1], r.wsem.at[0, 1])]

    def fetch_q(h):
        s = lax.rem(h, 2)
        return [L.unit(2 * HD + h * 2 * HD, r.wbuf.at[1, s], r.wsem.at[1, s])]

    def fetch_o(h):
        s = lax.rem(h, 3)
        return [L.unit(2 * HD + h * 2 * HD + HD, r.obuf.at[s], r.osem.at[s])]

    def fetch_mlp(j):
        col = base + j * 3 * FC
        s = lax.rem(j, 2)
        o = lax.rem(j + H, 3)
        return [L.unit(col, r.wbuf.at[s, 0], r.wsem.at[s, 0]), L.unit(col + FC, r.wbuf.at[s, 1], r.wsem.at[s, 1]),
                L.unit(col + 2 * FC, r.obuf.at[o], r.osem.at[o])]

    def start(copies):
        for c in copies:
            c.start()

    def wait(copies):
        for c in copies:
            c.wait()

    comm = Comm(d, r.stage, r.w, r.send_sem, r.recv_sem)
    after_early = FIRST + 2 * EARLY
    last = comm.groups + LAG[5]
    rest_points, rest_steps = last - after_early, H - EARLY + J - 1

    def ready(points):
        return comm.end(max(points - LAG[5], comm.done[5]))

    def points_before(step):
        return after_early + (lax.div(step * rest_points, rest_steps) if not isinstance(step, int) else step * rest_points // rest_steps)

    for k in range(6):
        assert comm.done[k] >= min(FIRST - LAG[k], comm.groups)
    assert ready(FIRST) >= 2 * HD + 3 * HD
    for h in range(1, H):
        had = FIRST + 2 * h + 1 if h < EARLY else points_before(h - EARLY + 1)
        assert ready(had) >= (min(2 * HD + (h + 2) * 2 * HD + HD, base) if h + 1 < H else base + 3 * FC)
    for j in range(J - 1):
        assert ready(points_before(H - EARLY + j + 1)) >= base + (j + 2) * 3 * FC

    mine = r.w.at[comm.y, comm.x, comm.core]
    early, late = pl.ds(0, base), pl.ds(base, d["COLS"] - base)
    own = [pltpu.make_async_copy(r.stage.at[:, part], mine.at[:, part], r.local_sem.at[2 + i])
           for i, part in enumerate((early, late))]
    rest = r.stage.at[:, late]
    order_copies(d, r.win, r.wot, r.stage, r.local_sem, 0)
    arrive(d)
    for i in range(xbs):
        L.x_copy(i).start()
    pltpu.make_async_copy(r.stage.at[:, early], r.stage.at[:, early], r.local_sem.at[0]).wait()
    own[0].start()
    meet(d)
    reached = set()

    def late_begun():
        if "begun" not in reached:
            reached.add("begun")
            order_copies(d, r.win, r.wot, r.stage, r.local_sem, 1)

    def late_ready():
        late_begun()
        if "late" not in reached:
            reached.add("late")
            pltpu.make_async_copy(rest, rest, r.local_sem.at[1]).wait()
            own[1].start()

    def late_placed():
        late_ready()
        if "placed" not in reached:
            reached.add("placed")
            own[1].wait()

    normed = keyed = queried = 0
    next_group = [0] * 6
    for what in OPENING:
        if what <= 5:
            g = next_group[what]
            next_group[what] += 1
            if (what, g) == (2, 0):
                own[0].wait()
            if what == 0 and comm.end(g + 1) > base:
                late_ready()
            if what == 2 and comm.end(g + 1) > base:
                late_placed()
            with jax.named_scope(f"stage{what}"):
                comm.stage_fn(what, g, g < SMALL)
            if (what, g) == (0, 1):
                spread_scale(d, r.ln_own, r.ln_all, r.ln_send, r.ln_recv)
            if what == 1:
                late_begun()
            if what == 5 and comm.end(g) < 3 * HD <= comm.end(g + 1):
                start(fetch_kv())
                start(fetch_q(0))
            if what == 5 and comm.end(g) < 5 * HD <= comm.end(g + 1):
                start(fetch_q(1))
                start(fetch_o(0))
        elif what == KEYS:
            if keyed == 0:
                assert normed == xbs
                with jax.named_scope("wait_kv"):
                    wait(fetch_kv())
            if keyed < mbs:
                with jax.named_scope("keys"):
                    L.keys(keyed, r.wbuf.at[0, 0], r.wbuf.at[0, 1])
            keyed += 1
            if keyed == mbs:
                pltpu.make_async_copy(r.k, r.kc.at[0], r.csem.at[0]).start()
                pltpu.make_async_copy(r.v, r.vc.at[0], r.csem.at[1]).start()
        elif what == QUERY:
            if queried == 0:
                wait(fetch_q(0))
            if queried < mbs:
                with jax.named_scope("query"):
                    L.query(queried, r.wbuf.at[1, 0], r.q.at[0])
            queried += 1
        else:
            if normed == 0:
                late_ready()
                with jax.named_scope("tables"):
                    L.tables()
                    L.bias()
                with jax.named_scope("wait_scale"):
                    spread_scale_wait(d, r.ln_all, r.ln_send, r.ln_recv)
                    scale_row(d, r.ln_all, r.ln)
            many = min(what - NORM, xbs - normed)
            if many > 0:
                with jax.named_scope("norm"):
                    @pl.loop(normed, normed + many)
                    def _(i):
                        L.norm(i)
            normed += many
    late_ready()
    late_placed()
    r.a[1] = jnp.zeros((d["T"], FC), jnp.bfloat16)
    r.obuf[2] = jnp.zeros(r.obuf.shape[1:], jnp.bfloat16)

    @pl.loop(0, H)
    def _(h):
        @pl.when(h < EARLY)
        def _():
            with jax.named_scope("point_head"):
                comm.point(FIRST + 2 * h, FIRST, after_early)

        @pl.when(h >= EARLY)
        def _():
            @pl.loop(points_before(h - EARLY), points_before(h - EARLY + 1))
            def _(p):
                with jax.named_scope("point_head"):
                    comm.point(p, after_early, points_before(H - EARLY) + 1)

        @pl.when(h == 1)
        def _():
            start(fetch_o(h))
            start(fetch_q(h + 1))

        @pl.when(jnp.logical_and(h > 0, h + 1 < H))
        def _():
            start(fetch_o(h + 1))

        @pl.when(jnp.logical_and(h > 0, h + 2 < H))
        def _():
            start(fetch_q(h + 2))

        @pl.when(h + 1 < H)
        def _():
            wait(fetch_q(h + 1))

        @pl.when(h > 0)
        def _():
            wait(fetch_o(h - 1))

        @pl.when(h + 1 == H)
        def _():
            start(fetch_mlp(0))

        s = lax.rem(h, 2)

        def midway():
            @pl.when(h < EARLY)
            def _():
                with jax.named_scope("point_mid"):
                    comm.point(FIRST + 2 * h + 1, FIRST + 1, after_early)

        with jax.named_scope("head"):
            L.head(r.q.at[s], r.a.at[s], r.q.at[1 - s], r.wbuf.at[1, 1 - s], r.a.at[1 - s], r.obuf.at[lax.rem(h + 2, 3)], midway)

    wait(fetch_o(H - 1))

    @pl.loop(0, J)
    def _(j):
        @pl.when(j + 1 < J)
        def _():
            @pl.loop(points_before(H - EARLY + j), points_before(H - EARLY + j + 1))
            def _(p):
                with jax.named_scope("point_mlp"):
                    comm.point(p, points_before(H - EARLY), last)

            start(fetch_mlp(j + 1))

        with jax.named_scope("wait_mlp"):
            wait(fetch_mlp(j))
        s = lax.rem(j, 2)
        prev = r.obuf.at[lax.rem(j - 1 + H, 3)]
        per = tiles // mbs
        with jax.named_scope("mlp"):
            for m in range(mbs):
                L.gated(m, r.wbuf.at[s, 0], r.wbuf.at[s, 1], r.a.at[s])
                for t in range(m * per, (m + 1) * per):
                    L.add_out(r.a.at[1 - s], prev, t)

    with jax.named_scope("finish"):
        L.finish(r.a.at[(J - 1) % 2], r.obuf.at[(J - 1 + H) % 3])
    pltpu.make_async_copy(r.k, r.kc.at[0], r.csem.at[0]).wait()
    pltpu.make_async_copy(r.v, r.vc.at[0], r.csem.at[1]).wait()
    comm.drain()


def layer(d, x, prompt_len, ln, w_in, wot):
    T, E, HD = d["T"], d["E"], d["HD"]
    half = HD // 2
    inv_freq = np.float64(ROPE_BASE) ** (-2.0 * np.arange(half) / HD)
    steps = np.concatenate([np.arange(Layer.QB), np.arange(T // Layer.QB) * Layer.QB])
    angles = steps[:, None] * inv_freq[None, :]
    rc = jnp.asarray(np.cos(angles), jnp.float32)
    rs = jnp.asarray(np.sin(angles), jnp.float32)
    w_shape = (d["SIDE"], d["SIDE"], d["CORES"], d["R"], d["COLS"])
    hbm, vmem = pl.BlockSpec(memory_space=HBM), pl.BlockSpec(memory_space=pltpu.VMEM)
    flops = 2 * T * E * d["COLS"] + 2 * T * T * HD * d["H"]
    cache = jax.ShapeDtypeStruct((1, T, HD), jnp.bfloat16)
    y, kc, vc, _ = pl.pallas_call(
        functools.partial(kernel, d),
        out_shape=(jax.ShapeDtypeStruct(x.shape, jnp.bfloat16), cache, cache,
                   jax.ShapeDtypeStruct(w_shape, jnp.bfloat16)),
        in_specs=[vmem, hbm, hbm, hbm, pl.BlockSpec(memory_space=pltpu.SMEM), vmem, vmem],
        out_specs=(hbm, hbm, hbm, hbm),
        scratch_shapes=scratch(d),
        compiler_params=pltpu.CompilerParams(collective_id=0, has_side_effects=True, vmem_limit_bytes=VMEM_LIMIT),
        cost_estimate=pl.CostEstimate(flops=flops, bytes_accessed=4 * T * E + 2 * E * d["COLS"], transcendentals=0),
        name="layer",
    )(ln[None], w_in, wot, x, prompt_len, rc, rs)
    return hand_on(y, kc, vc)


def hand_on_kernel(parts, *refs):
    n = len(parts)
    src, dst, buf, sem_in, sem_out = refs[:n], refs[n:2 * n], refs[2 * n:3 * n], refs[3 * n], refs[3 * n + 1]
    moves = []
    for i, blocks in enumerate(parts):
        rows = src[i].shape[1] // blocks
        for k in range(blocks):
            at = pl.ds(k * rows, rows)
            moves.append((src[i].at[0, at, :], buf[i].at[at, :], dst[i].at[0, at, :]))
    for k, (a, b, _) in enumerate(moves):
        pltpu.make_async_copy(a, b, sem_in.at[k]).start()
    for k, (a, b, c) in enumerate(moves):
        pltpu.make_async_copy(a, b, sem_in.at[k]).wait()
        pltpu.make_async_copy(b, c, sem_out.at[k]).start()
    for k, (_, b, c) in enumerate(moves):
        pltpu.make_async_copy(b, c, sem_out.at[k]).wait()


def hand_on(y, kc, vc):
    arrays, parts = (y, kc, vc), (8, 1, 1)
    hbm = pl.BlockSpec(memory_space=HBM)
    return pl.pallas_call(
        functools.partial(hand_on_kernel, parts),
        out_shape=tuple(jax.ShapeDtypeStruct(a.shape, a.dtype) for a in arrays),
        in_specs=[hbm] * 3,
        out_specs=(hbm,) * 3,
        scratch_shapes=[pltpu.VMEM(a.shape[1:], a.dtype) for a in arrays]
        + [pltpu.SemaphoreType.DMA((sum(parts),)), pltpu.SemaphoreType.DMA((sum(parts),))],
        compiler_params=pltpu.CompilerParams(vmem_limit_bytes=VMEM_LIMIT),
        name="hand_on",
    )(*arrays)


def solution(mesh):
    batch_spec = P(("pod", "d"))

    def local_layer(x, prompt_len, ln_shard, w_in_shard, w_out_shard):
        d = dims(mesh, x, w_in_shard, w_out_shard)
        return layer(d, x, prompt_len, ln_shard, w_in_shard, w_out_shard.T)

    return jax.shard_map(local_layer, mesh=mesh,
                         in_specs=(batch_spec, batch_spec, P("d"), P("d", None), P(None, "d")),
                         out_specs=(batch_spec, batch_spec, batch_spec), check_vma=False)
```

```python
import functools
import math

import jax
import jax.numpy as jnp
import numpy as np
from jax import lax
from jax.experimental import pallas as pl
from jax.experimental.pallas import tpu as pltpu
from jax.sharding import PartitionSpec as P

EPS = 1e-6
ROPE_BASE = 10000.0
MASKED = -1e30
MESH = pl.DeviceIdType.MESH
HBM = pltpu.HBM
VMEM_LIMIT = 67043328

SMALL, SMALL_WIDTH, WIDTH = 10, 384, 768
LAG = (0, 2, 4, 6, 8, 9)
FIRST = 12
EARLY = 3
KEYS, QUERY, SCALE, NORM = 6, 7, 8, 9
OPENING = (SCALE, 0, 0, 0, 0, 0, 0, 0, 0, SCALE, 1, 1, SCALE, 0, 1, 1, SCALE, 0, 1, 1, SCALE, 0, 1, 2, 2, NORM + 12, 1, 1,
           NORM + 1, 1, 1, NORM + 3, 3, 2, 3, 2, 4, 0, 3, 2, 4, 5, 3, 2, 5, KEYS, 4, KEYS, 3, 2, KEYS, 4, KEYS, 5, 1, QUERY,
           3, 2, QUERY, QUERY, 4, QUERY, 5)


def dims(mesh, x, w_in, w_out):
    devices = mesh.shape["d"]
    cores = 2
    side = math.isqrt(devices // cores)
    model = x.shape[2]
    ffn = 4 * model
    attn = w_out.shape[0] - ffn
    head = (w_in.shape[1] - 2 * ffn - attn) // 2
    return dict(D=devices, CORES=cores, SIDE=side, T=x.shape[1], E=model, F=ffn, H=attn // head, HD=head,
                R=model // devices, COLS=w_in.shape[1] + w_out.shape[0], FC=head)


def place():
    return lax.axis_index("d")


def order_copies(d, win_ref, wot_ref, stage_ref, sem, part):
    F, H, HD, FC = d["F"], d["H"], d["HD"], d["FC"]
    qs = 2 * F
    ks = qs + H * HD
    base = 2 * HD + H * 2 * HD

    def move(src_ref, col, at, width, which):
        pltpu.make_async_copy(src_ref.at[:, pl.ds(pl.multiple_of(col, HD), width)],
                              stage_ref.at[:, pl.ds(pl.multiple_of(at, HD), width)], sem.at[which]).start()

    if part == 0:
        move(win_ref, ks, 0, 2 * HD, 0)

        @pl.loop(0, H)
        def _(h):
            move(win_ref, qs + h * HD, 2 * HD + h * 2 * HD, HD, 0)
            move(wot_ref, F + h * HD, 3 * HD + h * 2 * HD, HD, 0)

        return

    @pl.loop(0, F // FC)
    def _(j):
        at = base + j * 3 * FC
        move(win_ref, j * FC, at, FC, 1)
        move(win_ref, F + j * FC, at + FC, FC, 1)
        move(wot_ref, j * FC, at + 2 * FC, FC, 1)


class Comm:
    def __init__(self, d, stage_ref, w_ref, send_sem, recv_sem):
        self.d = d
        self.stage, self.w, self.send, self.recv = stage_ref, w_ref, send_sem, recv_sem
        self.groups = SMALL + (d["COLS"] - SMALL * SMALL_WIDTH) // WIDTH
        self.done = [OPENING.count(k) for k in range(6)]
        side, cores = d["SIDE"], d["CORES"]
        me = place()
        self.core = lax.rem(me, cores)
        self.x = lax.rem(lax.div(me, cores), side)
        self.y = lax.div(me, cores * side)

    @staticmethod
    def end(groups):
        return min(groups, SMALL) * SMALL_WIDTH + max(groups - SMALL, 0) * WIDTH

    def dev(self, y, x, core):
        d = self.d
        return {"d": (y * d["SIDE"] + x) * d["CORES"] + core}

    def near(self):
        ways = [self.dev(self.y, self.wrap(self.x + s), self.core) for s in (1, -1)]
        ways += [self.dev(self.wrap(self.y + s), self.x, self.core) for s in (1, -1)]
        return ways + [self.dev(self.y, self.x, 1 - self.core)]

    def wrap(self, v):
        side = self.d["SIDE"]
        return lax.rem(v + side, side)

    def put(self, src, dst, stage, g, device):
        return pltpu.make_async_remote_copy(src_ref=src, dst_ref=dst, send_sem=self.send.at[stage],
                                            recv_sem=self.recv.at[stage, g], device_id=device, device_id_type=MESH)

    def landed(self, ref, stage, g):
        pltpu.make_async_copy(ref, ref, self.recv.at[stage, g]).wait()

    def stage_fn(self, stage, g, small):
        w, x, y, c = self.w, self.x, self.y, self.core
        half = self.d["R"] // 2
        if small:
            cols = pl.ds(pl.multiple_of(g * SMALL_WIDTH, 128), SMALL_WIDTH)
        else:
            cols = pl.ds(pl.multiple_of(SMALL * SMALL_WIDTH + (g - SMALL) * WIDTH, 128), WIDTH)
        ra, rb = pl.ds(0, half), pl.ds(half, half)
        turn = 1 - 2 * lax.rem(g, 2)
        if stage == 0:
            for s in (1, -1):
                self.put(self.stage.at[ra, cols], w.at[y, x, c, ra, cols], 0, g,
                         self.dev(y, self.wrap(x + s), c)).start()
                self.put(self.stage.at[rb, cols], w.at[y, x, c, rb, cols], 0, g,
                         self.dev(self.wrap(y + s), x, c)).start()
        elif stage == 1:
            self.landed(w.at[0, 0:2, :, ra, cols], 0, g)
            xs, ys = self.wrap(x - turn), self.wrap(y + turn)
            a = w.at[y, xs, c, ra, cols]
            self.put(a, a, 1, g, self.dev(y, self.wrap(x + turn), c)).start()
            b = w.at[ys, x, c, rb, cols]
            self.put(b, b, 1, g, self.dev(self.wrap(y - turn), x, c)).start()
        elif stage == 2:
            self.landed(w.at[0, 0, :, ra, cols], 1, g)
            a = w.at[y, :, c, ra, cols]
            b = w.at[:, x, c, rb, cols]
            for s in (1, -1):
                self.put(a, a, 2, g, self.dev(self.wrap(y + s), x, c)).start()
                self.put(b, b, 2, g, self.dev(y, self.wrap(x + s), c)).start()
        elif stage == 3:
            self.landed(w.at[0:2, :, :, ra, cols], 2, g)
            quarter = half // 2
            for i, s in enumerate((1, -1)):
                a = w.at[self.wrap(y - s), :, c, pl.ds(i * quarter, quarter), cols]
                self.put(a, a, 3, g, self.dev(self.wrap(y + s), x, c)).start()
                b = w.at[:, self.wrap(x - s), c, pl.ds(half + i * quarter, quarter), cols]
                self.put(b, b, 3, g, self.dev(y, self.wrap(x + s), c)).start()
        elif stage == 4:
            self.landed(w.at[0, :, :, ra, cols], 3, g)
            a = w.at[:, :, c, :, cols]
            self.put(a, a, 4, g, self.dev(y, x, 1 - c)).start()
        else:
            self.landed(w.at[:, :, 0, :, cols], 4, g)

    def point(self, p, lo, hi):
        for stage in (4, 3, 2, 1, 0, 5):
            g = p - LAG[stage]
            for small, start, stop in ((True, 0, SMALL), (False, SMALL, self.groups)):
                start = max(start, self.done[stage])
                if hi - 1 - LAG[stage] < start or lo - LAG[stage] >= stop:
                    continue

                @pl.when(jnp.logical_and(g >= start, g < stop))
                def _(stage=stage, g=g, small=small):
                    self.stage_fn(stage, g, small)

    def drain(self):
        side, w = self.d["SIDE"], self.w
        for stage, ref in ((0, w.at[0, 0]), (1, w.at[0, 0, 0]), (2, w.at[0]), (3, w.at[0, 0:side // 2]),
                           (4, w.at[0:side // 2])):
            pltpu.make_async_copy(ref, ref, self.send.at[stage]).wait()


def arrive(comm):
    barrier = pltpu.get_barrier_semaphore()
    for device in comm.near():
        pl.semaphore_signal(barrier, inc=1, device_id=device, device_id_type=MESH)


def meet(comm):
    pl.semaphore_wait(pltpu.get_barrier_semaphore(), len(comm.near()))


def scale_stage(comm, stage, ln_all, send, recv):
    x, y, c = comm.x, comm.y, comm.core

    def put(ref, device):
        pltpu.make_async_remote_copy(src_ref=ref, dst_ref=ref, send_sem=send.at[stage], recv_sem=recv.at[stage],
                                     device_id=device, device_id_type=MESH).start()

    arrived = (None, ln_all.at[0, 0], ln_all.at[0, 0, 0], ln_all.at[0], ln_all.at[0, :, 0])[stage]
    if stage:
        pltpu.make_async_copy(arrived, arrived, recv.at[stage - 1]).wait()
    if stage == 0:
        for s in (1, -1):
            put(ln_all.at[y, x, c], comm.dev(y, comm.wrap(x + s), c))
    elif stage == 1:
        put(ln_all.at[y, comm.wrap(x - 1), c], comm.dev(y, comm.wrap(x + 1), c))
    elif stage == 2:
        for s in (1, -1):
            put(ln_all.at[y, :, c], comm.dev(comm.wrap(y + s), x, c))
    elif stage == 3:
        put(ln_all.at[comm.wrap(y - 1), :, c], comm.dev(comm.wrap(y + 1), x, c))
    else:
        put(ln_all.at[:, :, c], comm.dev(y, x, 1 - c))


def scale_wait(ln_all, send, recv):
    half = ln_all.at[:, :, 0]
    pltpu.make_async_copy(half, half, recv.at[4]).wait()
    for stage, ref in enumerate((ln_all.at[0, 0], ln_all.at[0, 0, 0], ln_all.at[0], ln_all.at[0, :, 0], half)):
        pltpu.make_async_copy(ref, ref, send.at[stage]).wait()


def scale_row(d, ln_all, row_ref):
    per = 128 // d["R"]
    side, cores = d["SIDE"], d["CORES"]
    for i in range(d["E"] // 128):
        parts = [ln_all[n // (side * cores), n // cores % side, n % cores] for n in range(per * i, per * (i + 1))]
        row_ref[0:1, i * 128:(i + 1) * 128] = jnp.concatenate(parts, axis=1)


def nn(a, b):
    return lax.dot_general(a, b, (((1,), (0,)), ((), ())), preferred_element_type=jnp.float32)


def nt(a, b):
    return lax.dot_general(a, b, (((1,), (1,)), ((), ())), preferred_element_type=jnp.float32)


def rope(u, cos, sin):
    half = u.shape[1] // 2
    u1, u2 = u[:, :half], u[:, half:]
    return jnp.concatenate([u1 * cos - u2 * sin, u2 * cos + u1 * sin], axis=1)


class Layer:
    XB = 128
    MB = 512
    QB = 256

    def __init__(self, d, r):
        self.d, self.r = d, r

    def x_copy(self, i):
        rows = pl.ds(pl.multiple_of(i * self.XB, self.XB), self.XB)
        return pltpu.make_async_copy(self.r.x.at[0, rows, :], self.r.h.at[rows, :], self.r.xsem.at[i])

    def y_copy(self, t):
        cols = pl.ds(t * self.d["FC"], self.d["FC"])
        return pltpu.make_async_copy(self.r.h.at[:, cols], self.r.y.at[0, :, cols], self.r.xsem.at[t])

    def unit(self, col, buf, sem):
        return pltpu.make_async_copy(self.r.w.at[:, :, :, :, pl.ds(pl.multiple_of(col, 128), self.d["FC"])], buf, sem)

    def wval(self, buf):
        return buf[...].reshape(self.d["E"], self.d["FC"])

    def norm(self, i):
        r = self.r
        self.x_copy(i).wait()
        rows = pl.ds(pl.multiple_of(i * self.XB, self.XB), self.XB)
        xf = r.h[rows, :].astype(jnp.float32)
        centered = xf - jnp.mean(xf, axis=-1, keepdims=True)
        var = jnp.mean(centered * centered, axis=-1, keepdims=True)
        r.h[rows, :] = (centered * lax.rsqrt(var + EPS) * r.ln[...]).astype(jnp.bfloat16)
        r.yacc[rows, :] = xf

    def tables(self):
        d, r = self.d, self.r
        lo = r.rc.shape[0] - d["T"] // self.QB
        cl, sl = r.rc[0:self.QB, :], r.rs[0:self.QB, :]
        for b in range(d["T"] // self.QB):
            cb, sb = r.rc[self.QB + b:self.QB + b + 1, :], r.rs[self.QB + b:self.QB + b + 1, :]
            rows = slice(b * self.QB, (b + 1) * self.QB)
            r.cos[rows, :] = cl * cb - sl * sb
            r.sin[rows, :] = sl * cb + cl * sb

    def bias(self):
        r, d = self.r, self.d
        col = lax.broadcasted_iota(jnp.int32, (8, d["T"]), 1)
        r.bias[...] = jnp.where(col < r.plen[0], 0.0, MASKED)

    def keys(self, m, kbuf, vbuf):
        r = self.r
        rows = slice(m * self.MB, (m + 1) * self.MB)
        hb = r.h[rows, :]
        kf = rope(nn(hb, self.wval(kbuf)), r.cos[rows, :], r.sin[rows, :])
        r.k[rows, :] = kf.astype(jnp.bfloat16)
        r.kt[:, rows] = kf.T.astype(jnp.bfloat16)
        r.v[rows, :] = nn(hb, self.wval(vbuf)).astype(jnp.bfloat16)

    def query(self, m, qbuf, q_ref):
        r = self.r
        rows = slice(m * self.MB, (m + 1) * self.MB)
        q_ref[rows, :] = rope(nn(r.h[rows, :], self.wval(qbuf)), r.cos[rows, :], r.sin[rows, :]).astype(jnp.bfloat16)

    def scores(self, b, q_ref, z_ref):
        d, r = self.d, self.r
        qb, half = self.QB, self.QB // 2
        unit = math.log2(math.e) / math.sqrt(d["HD"])
        q = q_ref[b * qb:(b + 1) * qb, :]
        top = [None, None]
        for c in range(b + 1):
            cols = slice(c * qb, (c + 1) * qb)
            s = nn(q, r.kt[:, cols])
            for i in range(2):
                part = slice(i * half, (i + 1) * half)
                z = s[part, :] * unit + r.bias[0:1, cols]
                if c == b:
                    row = lax.broadcasted_iota(jnp.int32, (half, qb), 0) + i * half
                    col = lax.broadcasted_iota(jnp.int32, (half, qb), 1)
                    z = jnp.where(col <= row, z, MASKED)
                z_ref[part, cols] = z
                for k in range(qb // 128):
                    zk = z[:, k * 128:(k + 1) * 128]
                    top[i] = zk if top[i] is None else jnp.maximum(top[i], zk)
        return [jnp.max(t, axis=-1, keepdims=True) for t in top]

    def softmax(self, b, z_ref, p_ref, top):
        qb, half = self.QB, self.QB // 2
        for i in range(2):
            part = slice(i * half, (i + 1) * half)
            total = None
            for c in range(b + 1):
                cols = slice(c * qb, (c + 1) * qb)
                e = jnp.exp2(z_ref[part, cols] - top[i])
                z_ref[part, cols] = e
                for k in range(qb // 128):
                    ek = e[:, k * 128:(k + 1) * 128]
                    total = ek if total is None else total + ek
            inv = 1.0 / jnp.sum(total, axis=-1, keepdims=True)
            for c in range(b + 1):
                cols = slice(c * qb, (c + 1) * qb)
                p_ref[part, cols] = (z_ref[part, cols] * inv).astype(jnp.bfloat16)

    def values(self, b, p_ref, o_ref):
        r, qb = self.r, self.QB
        n = (b + 1) * qb
        o_ref[b * qb:n, :] = nn(p_ref[:, 0:n], r.v[0:n, :]).astype(jnp.bfloat16)

    def head(self, q_ref, o_ref, q_next, qbuf_next, o_prev, obuf_prev, midway):
        d, r = self.d, self.r
        nb = d["T"] // self.QB
        mbs, tiles = d["T"] // self.MB, d["E"] // d["FC"]
        work = [functools.partial(self.add_out, o_prev, obuf_prev, t) for t in range(tiles)]
        per = tiles // mbs
        steps = []
        for m in range(mbs):
            steps += [work[m * per:(m + 1) * per], [functools.partial(self.query, m, qbuf_next, q_next)]]
        last = None
        for n, b in enumerate(reversed(range(nb))):
            if n == nb // 2:
                midway()
            z_ref, p_ref = r.z.at[n % 2], r.p.at[n % 2]
            top = self.scores(b, q_ref, z_ref)
            for f in steps[n]:
                f()
            self.softmax(b, z_ref, p_ref, top)
            if last is not None:
                self.values(*last)
            last = (b, p_ref, o_ref)
        self.values(*last)

    def add_out(self, a_ref, obuf, tile):
        r, d = self.r, self.d
        fc = d["FC"]
        per = fc // d["R"]
        cols = slice(tile * fc, (tile + 1) * fc)
        w = self.wval(obuf)[cols, :]
        r.yacc[:, cols] += nt(a_ref[...], w)

    def gated(self, m, gbuf, ubuf, a_ref):
        r = self.r
        rows = slice(m * self.MB, (m + 1) * self.MB)
        hb = r.h[rows, :]
        g = nn(hb, self.wval(gbuf))
        u = nn(hb, self.wval(ubuf))
        hg = g * 0.5
        a_ref[rows, :] = ((hg + hg * jnp.tanh(hg)) * u).astype(jnp.bfloat16)

    def finish(self, a_ref, obuf):
        d, r = self.d, self.r
        fc = d["FC"]
        for t in range(d["E"] // fc):
            cols = slice(t * fc, (t + 1) * fc)
            total = r.yacc[:, cols] + nt(a_ref[...], self.wval(obuf)[cols, :])
            r.h[:, cols] = total.astype(jnp.bfloat16)
            self.y_copy(t).start()
        for t in range(d["E"] // fc):
            self.y_copy(t).wait()


class Refs:
    pass


NAMES = ("ln_own", "win", "wot", "x", "plen", "rc", "rs",
         "y", "kc", "vc", "w",
         "stage", "ln_all", "ln", "h", "yacc", "cos", "sin", "bias", "k", "kt", "v", "q", "z", "p", "a", "wbuf", "obuf",
         "local_sem", "ln_send", "ln_recv", "send_sem", "recv_sem", "xsem", "wsem", "osem", "csem")


def scratch(d):
    T, E, HD, FC = d["T"], d["E"], d["HD"], d["FC"]
    unit = (d["SIDE"], d["SIDE"], d["CORES"], d["R"], FC)
    bf16, f32, dma = jnp.bfloat16, jnp.float32, pltpu.SemaphoreType.DMA
    return [
        pltpu.VMEM((d["R"], d["COLS"]), bf16),
        pltpu.VMEM((d["SIDE"], d["SIDE"], d["CORES"], 1, d["R"]), f32),
        pltpu.VMEM((1, E), f32),
        pltpu.VMEM((T, E), bf16),
        pltpu.VMEM((T, E), f32),
        pltpu.VMEM((T, HD // 2), f32),
        pltpu.VMEM((T, HD // 2), f32),
        pltpu.VMEM((8, T), f32),
        pltpu.VMEM((T, HD), bf16),
        pltpu.VMEM((HD, T), bf16),
        pltpu.VMEM((T, HD), bf16),
        pltpu.VMEM((2, T, HD), bf16),
        pltpu.VMEM((2, Layer.QB, T), f32),
        pltpu.VMEM((2, Layer.QB, T), bf16),
        pltpu.VMEM((2, T, FC), bf16),
        pltpu.VMEM((2, 2) + unit, bf16),
        pltpu.VMEM((3,) + unit, bf16),
        dma((5,)), dma((5,)), dma((5,)), dma((5,)), dma((5, SMALL + (d["COLS"] - SMALL * SMALL_WIDTH) // WIDTH)),
        dma((max(T // Layer.XB, E // FC),)), dma((2, 2)), dma((3,)), dma((2,)),
    ]


def kernel(d, *refs):
    r = Refs()
    for name, ref in zip(NAMES, refs, strict=True):
        setattr(r, name, ref)
    L = Layer(d, r)
    HD, FC, H = d["HD"], d["FC"], d["H"]
    J = d["F"] // FC
    tiles = d["E"] // FC
    mbs = d["T"] // L.MB
    xbs = d["T"] // L.XB
    base = 2 * HD + H * 2 * HD

    def fetch_kv():
        return [L.unit(0, r.wbuf.at[0, 0], r.wsem.at[0, 0]), L.unit(HD, r.wbuf.at[0, 1], r.wsem.at[0, 1])]

    def fetch_q(h):
        s = lax.rem(h, 2)
        return [L.unit(2 * HD + h * 2 * HD, r.wbuf.at[1, s], r.wsem.at[1, s])]

    def fetch_o(h):
        s = lax.rem(h, 3)
        return [L.unit(2 * HD + h * 2 * HD + HD, r.obuf.at[s], r.osem.at[s])]

    def fetch_mlp(j):
        col = base + j * 3 * FC
        s = lax.rem(j, 2)
        o = lax.rem(j + H, 3)
        return [L.unit(col, r.wbuf.at[s, 0], r.wsem.at[s, 0]), L.unit(col + FC, r.wbuf.at[s, 1], r.wsem.at[s, 1]),
                L.unit(col + 2 * FC, r.obuf.at[o], r.osem.at[o])]

    def start(copies):
        for c in copies:
            c.start()

    def wait(copies):
        for c in copies:
            c.wait()

    comm = Comm(d, r.stage, r.w, r.send_sem, r.recv_sem)
    after_early = FIRST + 2 * EARLY
    last = comm.groups + LAG[5]
    rest_points, rest_steps = last - after_early, H - EARLY + J - 1

    def ready(points):
        return comm.end(max(points - LAG[5], comm.done[5]))

    def points_before(step):
        return after_early + (lax.div(step * rest_points, rest_steps) if not isinstance(step, int) else step * rest_points // rest_steps)

    for k in range(6):
        assert comm.done[k] >= min(FIRST - LAG[k], comm.groups)
    assert ready(FIRST) >= 2 * HD + 3 * HD
    for h in range(1, H):
        had = FIRST + 2 * h + 1 if h < EARLY else points_before(h - EARLY + 1)
        assert ready(had) >= (min(2 * HD + (h + 2) * 2 * HD + HD, base) if h + 1 < H else base + 3 * FC)
    for j in range(J - 1):
        assert ready(points_before(H - EARLY + j + 1)) >= base + (j + 2) * 3 * FC

    mine = r.w.at[comm.y, comm.x, comm.core]
    early, late = pl.ds(0, base), pl.ds(base, d["COLS"] - base)
    own = [pltpu.make_async_copy(r.stage.at[:, part], mine.at[:, part], r.local_sem.at[2 + i])
           for i, part in enumerate((early, late))]
    rest = r.stage.at[:, late]
    own_scale = pltpu.make_async_copy(r.ln_own, r.ln_all.at[comm.y, comm.x, comm.core], r.local_sem.at[4])
    arrive(comm)
    own_scale.start()
    order_copies(d, r.win, r.wot, r.stage, r.local_sem, 0)
    for i in range(xbs):
        L.x_copy(i).start()
    pltpu.make_async_copy(r.stage.at[:, early], r.stage.at[:, early], r.local_sem.at[0]).wait()
    own[0].start()
    own_scale.wait()
    meet(comm)
    reached = set()

    def late_begun():
        if "begun" not in reached:
            reached.add("begun")
            order_copies(d, r.win, r.wot, r.stage, r.local_sem, 1)

    def late_ready():
        late_begun()
        if "late" not in reached:
            reached.add("late")
            pltpu.make_async_copy(rest, rest, r.local_sem.at[1]).wait()
            own[1].start()

    def late_placed():
        late_ready()
        if "placed" not in reached:
            reached.add("placed")
            own[1].wait()

    normed = keyed = queried = scaled = 0
    next_group = [0] * 6
    for what in OPENING:
        if what <= 5:
            g = next_group[what]
            next_group[what] += 1
            if (what, g) == (2, 0):
                own[0].wait()
            if what == 0 and comm.end(g + 1) > base:
                late_ready()
            if what == 2 and comm.end(g + 1) > base:
                late_placed()
            with jax.named_scope(f"stage{what}"):
                comm.stage_fn(what, g, g < SMALL)
            if what == 1:
                late_begun()
            if what == 5 and comm.end(g) < 3 * HD <= comm.end(g + 1):
                start(fetch_kv())
                start(fetch_q(0))
            if what == 5 and comm.end(g) < 5 * HD <= comm.end(g + 1):
                start(fetch_q(1))
                start(fetch_o(0))
        elif what == SCALE:
            with jax.named_scope("scale"):
                scale_stage(comm, scaled, r.ln_all, r.ln_send, r.ln_recv)
            scaled += 1
        elif what == KEYS:
            if keyed == 0:
                assert normed == xbs
                with jax.named_scope("wait_kv"):
                    wait(fetch_kv())
            if keyed < mbs:
                with jax.named_scope("keys"):
                    L.keys(keyed, r.wbuf.at[0, 0], r.wbuf.at[0, 1])
            keyed += 1
            if keyed == mbs:
                pltpu.make_async_copy(r.k, r.kc.at[0], r.csem.at[0]).start()
                pltpu.make_async_copy(r.v, r.vc.at[0], r.csem.at[1]).start()
        elif what == QUERY:
            if queried == 0:
                wait(fetch_q(0))
            if queried < mbs:
                with jax.named_scope("query"):
                    L.query(queried, r.wbuf.at[1, 0], r.q.at[0])
            queried += 1
        else:
            if normed == 0:
                late_ready()
                with jax.named_scope("tables"):
                    L.tables()
                    L.bias()
                with jax.named_scope("wait_scale"):
                    scale_wait(r.ln_all, r.ln_send, r.ln_recv)
                    scale_row(d, r.ln_all, r.ln)
            many = min(what - NORM, xbs - normed)
            if many > 0:
                with jax.named_scope("norm"):
                    @pl.loop(normed, normed + many)
                    def _(i):
                        L.norm(i)
            normed += many
    late_ready()
    late_placed()
    r.a[1] = jnp.zeros((d["T"], FC), jnp.bfloat16)
    r.obuf[2] = jnp.zeros(r.obuf.shape[1:], jnp.bfloat16)

    @pl.loop(0, H)
    def _(h):
        @pl.when(h < EARLY)
        def _():
            with jax.named_scope("point_head"):
                comm.point(FIRST + 2 * h, FIRST, after_early)

        @pl.when(h >= EARLY)
        def _():
            @pl.loop(points_before(h - EARLY), points_before(h - EARLY + 1))
            def _(p):
                with jax.named_scope("point_head"):
                    comm.point(p, after_early, points_before(H - EARLY) + 1)

        @pl.when(h == 1)
        def _():
            start(fetch_o(h))
            start(fetch_q(h + 1))

        @pl.when(jnp.logical_and(h > 0, h + 1 < H))
        def _():
            start(fetch_o(h + 1))

        @pl.when(jnp.logical_and(h > 0, h + 2 < H))
        def _():
            start(fetch_q(h + 2))

        @pl.when(h + 1 < H)
        def _():
            wait(fetch_q(h + 1))

        @pl.when(h > 0)
        def _():
            wait(fetch_o(h - 1))

        @pl.when(h + 1 == H)
        def _():
            start(fetch_mlp(0))

        s = lax.rem(h, 2)

        def midway():
            @pl.when(h < EARLY)
            def _():
                with jax.named_scope("point_mid"):
                    comm.point(FIRST + 2 * h + 1, FIRST + 1, after_early)

        with jax.named_scope("head"):
            L.head(r.q.at[s], r.a.at[s], r.q.at[1 - s], r.wbuf.at[1, 1 - s], r.a.at[1 - s], r.obuf.at[lax.rem(h + 2, 3)], midway)

    wait(fetch_o(H - 1))

    @pl.loop(0, J)
    def _(j):
        @pl.when(j + 1 < J)
        def _():
            @pl.loop(points_before(H - EARLY + j), points_before(H - EARLY + j + 1))
            def _(p):
                with jax.named_scope("point_mlp"):
                    comm.point(p, points_before(H - EARLY), last)

            start(fetch_mlp(j + 1))

        with jax.named_scope("wait_mlp"):
            wait(fetch_mlp(j))
        s = lax.rem(j, 2)
        prev = r.obuf.at[lax.rem(j - 1 + H, 3)]
        per = tiles // mbs
        with jax.named_scope("mlp"):
            for m in range(mbs):
                L.gated(m, r.wbuf.at[s, 0], r.wbuf.at[s, 1], r.a.at[s])
                for t in range(m * per, (m + 1) * per):
                    L.add_out(r.a.at[1 - s], prev, t)

    with jax.named_scope("finish"):
        L.finish(r.a.at[(J - 1) % 2], r.obuf.at[(J - 1 + H) % 3])
    pltpu.make_async_copy(r.k, r.kc.at[0], r.csem.at[0]).wait()
    pltpu.make_async_copy(r.v, r.vc.at[0], r.csem.at[1]).wait()
    comm.drain()


def layer(d, x, prompt_len, ln, w_in, wot):
    T, E, HD = d["T"], d["E"], d["HD"]
    half = HD // 2
    inv_freq = np.float64(ROPE_BASE) ** (-2.0 * np.arange(half) / HD)
    steps = np.concatenate([np.arange(Layer.QB), np.arange(T // Layer.QB) * Layer.QB])
    angles = steps[:, None] * inv_freq[None, :]
    rc = jnp.asarray(np.cos(angles), jnp.float32)
    rs = jnp.asarray(np.sin(angles), jnp.float32)
    w_shape = (d["SIDE"], d["SIDE"], d["CORES"], d["R"], d["COLS"])
    hbm, vmem = pl.BlockSpec(memory_space=HBM), pl.BlockSpec(memory_space=pltpu.VMEM)
    flops = 2 * T * E * d["COLS"] + 2 * T * T * HD * d["H"]
    cache = jax.ShapeDtypeStruct((1, T, HD), jnp.bfloat16)
    y, kc, vc, _ = pl.pallas_call(
        functools.partial(kernel, d),
        out_shape=(jax.ShapeDtypeStruct(x.shape, jnp.bfloat16), cache, cache,
                   jax.ShapeDtypeStruct(w_shape, jnp.bfloat16)),
        in_specs=[hbm, hbm, hbm, hbm, pl.BlockSpec(memory_space=pltpu.SMEM), vmem, vmem],
        out_specs=(hbm, hbm, hbm, hbm),
        scratch_shapes=scratch(d),
        compiler_params=pltpu.CompilerParams(collective_id=0, has_side_effects=True, vmem_limit_bytes=VMEM_LIMIT),
        cost_estimate=pl.CostEstimate(flops=flops, bytes_accessed=4 * T * E + 2 * E * d["COLS"], transcendentals=0),
        name="layer",
    )(ln[None], w_in, wot, x, prompt_len, rc, rs)
    return hand_on(y, kc, vc)


def hand_on_kernel(parts, *refs):
    n = len(parts)
    src, dst, buf, sem_in, sem_out = refs[:n], refs[n:2 * n], refs[2 * n:3 * n], refs[3 * n], refs[3 * n + 1]
    moves = []
    for i, blocks in enumerate(parts):
        rows = src[i].shape[1] // blocks
        for k in range(blocks):
            at = pl.ds(k * rows, rows)
            moves.append((src[i].at[0, at, :], buf[i].at[at, :], dst[i].at[0, at, :]))
    for k, (a, b, _) in enumerate(moves):
        pltpu.make_async_copy(a, b, sem_in.at[k]).start()
    for k, (a, b, c) in enumerate(moves):
        pltpu.make_async_copy(a, b, sem_in.at[k]).wait()
        pltpu.make_async_copy(b, c, sem_out.at[k]).start()
    for k, (_, b, c) in enumerate(moves):
        pltpu.make_async_copy(b, c, sem_out.at[k]).wait()


def hand_on(y, kc, vc):
    arrays, parts = (y, kc, vc), (8, 1, 1)
    hbm = pl.BlockSpec(memory_space=HBM)
    return pl.pallas_call(
        functools.partial(hand_on_kernel, parts),
        out_shape=tuple(jax.ShapeDtypeStruct(a.shape, a.dtype) for a in arrays),
        in_specs=[hbm] * 3,
        out_specs=(hbm,) * 3,
        scratch_shapes=[pltpu.VMEM(a.shape[1:], a.dtype) for a in arrays]
        + [pltpu.SemaphoreType.DMA((sum(parts),)), pltpu.SemaphoreType.DMA((sum(parts),))],
        compiler_params=pltpu.CompilerParams(vmem_limit_bytes=VMEM_LIMIT),
        name="hand_on",
    )(*arrays)


def solution(mesh):
    batch_spec = P(("pod", "d"))

    def local_layer(x, prompt_len, ln_shard, w_in_shard, w_out_shard):
        d = dims(mesh, x, w_in_shard, w_out_shard)
        return layer(d, x, prompt_len, ln_shard, w_in_shard, w_out_shard.T)

    return jax.shard_map(local_layer, mesh=mesh,
                         in_specs=(batch_spec, batch_spec, P("d"), P("d", None), P(None, "d")),
                         out_specs=(batch_spec, batch_spec, batch_spec), check_vma=False)
```
